1024 devices in a mesh: gx: 8 (over z_lo), gy: 16 (over y, z_hi), gz: 8 (over x, core).
Axes of the slice: x: 4, y: 4, z: 32 (z_hi: 4, z_lo: 8; z = z_hi * 8 + z_lo), core: 2. Of those that a mesh axis runs over, the one named last changes fastest.
Arguments:
- cell_index: int32 [8, 16, 8, 8192], P('gx', 'gy', 'gz'), may hold values from 2471 to 301728, as said below
- offsets: float32 [8, 16, 8, 3, 8192], P('gx', 'gy', 'gz'), may hold values from -0.5 to 0.5
- mass: float32 [8, 16, 8, 8192], P('gx', 'gy', 'gz'), may hold values from 0.5 to 2
- counts: int32 [8, 16, 8], P('gx', 'gy', 'gz'), may hold values from 2048 to 8192, as said below
Outputs:
- density: float32 [1024, 8, 32, 1024], P(None, 'gx', 'gy', 'gz')
- spectrum: float32 [2, 512, 8, 32, 1024], P(None, None, 'gx', 'gy', 'gz')
The draws below stay inside these ranges and needn't reach their ends.
Inputs may be any that keep to these rules, and one draw needn't show every extreme that they name: `cell_index`: each entry is (i + 1) * 18 * 130 + (j + 1) * 130 + k + 1 for a cell (i, j, k) with 0 <= i < 128, 0 <= j < 16, 0 <= k < 128; slots past a block's count hold such indices too. `counts`: some block is full in every draw.
All inputs are finite; a program needn't handle non-finite values.
Results may differ from the reference program's by a relative error of at most 0.0003.
Values sent between devices are 32-bit elements; how exact they have to be, the bound alone decides.
No kernel may reach another device: no remote copies, remote signals or barrier semaphores. Data moves between devices by JAX's collectives and lax.ppermute only.
A program may use at most 32 MiB of HBM per device.

```python
import math
import jax
import jax.numpy as jnp
from jax import lax

CX = 128
YP = 2
CZ = 128
PCAP = 8192
CY = 16
NX = 1024
NY = 256
NZ = 1024
N_GX = 8
N_GY = 16
N_GZ = 8


def edge_biased(key, extent, full_shape):
    pick_key, place_key = jax.random.split(key)
    selector = jax.random.randint(pick_key, full_shape, 0, 8)
    spread = jax.random.randint(place_key, full_shape, 0, extent)
    return jnp.where(selector == 0, 0, jnp.where(selector == 1, extent - 1, spread)).astype(jnp.int32)


def draw_cell_index(key, part):
    full_shape = (N_GX, N_GY, N_GZ, PCAP)
    key_list = jax.random.split(jax.random.fold_in(key, 11), 3)
    coord_x = edge_biased(key_list[0], CX, full_shape)
    coord_y = edge_biased(key_list[1], CY, full_shape)
    coord_z = edge_biased(key_list[2], CZ, full_shape)
    return (((coord_x + 1) * (CY + 2) + coord_y + 1) * (CZ + 2) + coord_z + 1).astype(jnp.int32)


def draw_counts(key, part):
    full_shape = (N_GX, N_GY, N_GZ)
    key_list = jax.random.split(jax.random.fold_in(key, 23), 3)
    base_load = jax.random.randint(key_list[0], full_shape, PCAP // 4, PCAP // 2 + 1)
    heavy = jax.random.randint(key_list[1], full_shape, 0, 16) == 0
    loads = jnp.where(heavy, PCAP, base_load).reshape(-1)
    fullest = jax.random.randint(key_list[2], (), 0, N_GX * N_GY * N_GZ)
    loads = loads.at[fullest].set(PCAP)
    return loads.reshape(full_shape).astype(jnp.int32)


def shard_levels(rng, dims, shards, low, high):
    def one(axis_at, parts):
        steps = jax.random.uniform(jax.random.fold_in(jax.random.fold_in(rng, 6), axis_at), (parts,), jnp.float32, low / len(shards), high / len(shards))
        return jnp.repeat(jnp.exp(steps), dims[axis_at] // parts).reshape((-1,) + (1,) * (len(dims) - axis_at - 1))

    loudness = one(*shards[0])
    for cut in shards[1:]:
        loudness = loudness * one(*cut)
    return loudness


def setup_inputs(seed: int = 0) -> dict:
    keys = jax.random.split(jax.random.key(seed), 5)
    cell_index = draw_cell_index(jax.random.fold_in(keys[4], 71), 0)
    offsets = jnp.clip(jax.random.uniform(keys[1], (N_GX, N_GY, N_GZ, 3, PCAP), jnp.float32, -0.5, 0.5) * shard_levels(keys[1], (N_GX, N_GY, N_GZ, 3, PCAP), ((0, 8), (1, 16), (2, 8)), -0.4, 0.0), -0.5, 0.5)
    mass = jnp.clip(jnp.exp(math.log(2.0) - 1.3862944 * jax.random.uniform(keys[2], (N_GX, N_GY, N_GZ, PCAP), jnp.float32) ** shard_levels(keys[2], (N_GX, N_GY, N_GZ, PCAP), ((0, 8), (1, 16), (2, 8)), -0.2, 0.2)), 0.5, 2.0)
    counts = draw_counts(jax.random.fold_in(keys[4], 71), 0)
    return {"cell_index": cell_index, "offsets": offsets, "mass": mass, "counts": counts}


def to_pencils(field):
    leading = field.shape[:-3]
    split = field.reshape(leading + (field.shape[-3], N_GY, N_GX, YP, NZ))
    moved = jnp.moveaxis(split, -4, -3)
    return moved.reshape(leading + (field.shape[-3], N_GX, N_GY * YP, NZ))

def reference(cell_index, offsets, mass, counts):
    full_shape = (N_GX, N_GY, N_GZ, PCAP)
    plane = (CY + 2) * (CZ + 2)
    block_x = lax.broadcasted_iota(jnp.int32, full_shape, 0)
    block_y = lax.broadcasted_iota(jnp.int32, full_shape, 1)
    block_z = lax.broadcasted_iota(jnp.int32, full_shape, 2)
    slot_ids = lax.broadcasted_iota(jnp.int32, full_shape, 3)
    pos_x = cell_index // plane - 1 + block_x * CX
    pos_y = cell_index // (CZ + 2) % (CY + 2) - 1 + block_y * CY
    pos_z = cell_index % (CZ + 2) - 1 + block_z * CZ
    loaded = jnp.where(slot_ids < counts[..., None], mass, jnp.float32(0.0))
    positions = (pos_x, pos_y, pos_z)
    extents = (NX, NY, NZ)
    shifts = [offsets[:, :, :, axis_pos, :] for axis_pos in range(3)]
    signs = [jnp.where(shifts[axis_pos] >= 0.0, 1, -1).astype(jnp.int32) for axis_pos in range(3)]
    field = jnp.zeros((NX * NY * NZ,), jnp.float32)
    for corner in range(8):
        factor = None
        targets = []
        for axis_pos in range(3):
            upper_bit = corner >> 2 - axis_pos & 1
            magnitude = jnp.abs(shifts[axis_pos])
            if upper_bit:
                target = (positions[axis_pos] + signs[axis_pos]) % extents[axis_pos]
                factor_one = magnitude
            else:
                target = positions[axis_pos] % extents[axis_pos]
                factor_one = 1.0 - magnitude
            targets.append(target.astype(jnp.int32))
            factor = factor_one if factor is None else factor * factor_one
        weight = factor * loaded
        flat_cell = ((targets[0] * NY + targets[1]) * NZ + targets[2]).astype(jnp.int32)
        field = field.at[flat_cell.reshape(-1)].add(weight.reshape(-1))
    field = field.reshape(NX, NY, NZ)
    modes = jnp.fft.rfft(field, axis=0)[:NX // 2]
    scale = 1.0 / math.sqrt(NX)
    spectrum = jnp.stack([jnp.real(modes), jnp.imag(modes)]).astype(jnp.float32) * scale
    return (to_pencils(field), to_pencils(spectrum))
```

```python
import functools
import math

import jax
import jax.numpy as jnp
from jax import lax
from jax.experimental import pallas as pl
from jax.experimental.pallas import tpu as pltpu
from jax.sharding import PartitionSpec as P

F32, I32, BF = jnp.float32, jnp.int32, jnp.bfloat16
GX = 8
ROWS = 18
FROWS = 8
NROW = 64
PAYROWS = 96
XR = 136
LANE = {6: 64, 7: 1, 8: 2, 9: 4, 10: 8, 11: 16, 12: 32}
SUB = {3: 1, 4: 2, 5: 4}
VM = pl.BlockSpec(memory_space=pltpu.VMEM)
SM = pl.BlockSpec(memory_space=pltpu.SMEM)


def cells_of(flat):
    row = jnp.floor((flat + 0.5) * (1.0 / 130.0))
    xp = jnp.floor((row + 0.5) * (1.0 / 18.0))
    return xp, row - 18.0 * xp, flat - 130.0 * row


def halves(value):
    high = value.astype(BF).astype(F32)
    return high, value - high


def index_bit(bit, lane, sub, reg):
    if bit < 3:
        return bool((reg >> bit) & 1)
    if bit in SUB:
        return (sub & SUB[bit]) != 0
    return (lane & LANE[bit]) != 0


def sort_network(ops, lane, sub):
    for size in range(1, 14):
        for bit in range(size - 1, -1, -1):
            new = [[None] * 8 for _ in ops]
            if bit < 3:
                for v in range(8):
                    w = v | (1 << bit)
                    if v == w:
                        continue
                    down = False if size == 13 else index_bit(size, lane, sub, v)
                    a, c = ops[0][v], ops[0][w]
                    if down is True:
                        move = a < c
                    elif down is False:
                        move = a > c
                    else:
                        move = ((a > c) ^ down) & (a != c)
                    for o in range(len(ops)):
                        a, c = ops[o][v], ops[o][w]
                        new[o][v] = jnp.where(move, c, a)
                        new[o][w] = jnp.where(move, a, c)
            else:
                axis, step, index = (0, SUB[bit], sub) if bit in SUB else (1, LANE[bit], lane)
                upper = (index & step) != 0
                other = index ^ step

                def partner(x):
                    if 2 * step == x.shape[axis]:
                        return pltpu.roll(x, step, axis)
                    return jnp.take_along_axis(x, other, axis=axis)

                for v in range(8):
                    down = False if size == 13 else index_bit(size, lane, sub, v)
                    mine, theirs = ops[0][v], partner(ops[0][v])
                    if down is True:
                        big = ~upper
                    elif down is False:
                        big = upper
                    else:
                        big = upper ^ down
                    move = ((theirs > mine) & big) | ((theirs < mine) & ~big)
                    new[0][v] = jnp.where(move, theirs, mine)
                    for o in range(1, len(ops)):
                        new[o][v] = jnp.where(move, partner(ops[o][v]), ops[o][v])
            ops = new
    return ops


def sort_kernel(count_ref, cell_ref, off_ref, mass_ref, sorted_ref, pay_ref):
    lane = lax.broadcasted_iota(I32, (8, 128), 1)
    sub = lax.broadcasted_iota(I32, (8, 128), 0)
    count = count_ref[0]
    key, px, py, pz, pm = [], [], [], [], []
    below = [jnp.zeros((8, 128), F32) for _ in range(17)]
    for v in range(8):
        s = slice(8 * v, 8 * v + 8)
        cell = cell_ref[s, :]
        dy = off_ref[1, s, :]
        live = v * 1024 + sub * 128 + lane < count
        _, yp, _ = cells_of(cell.astype(F32))
        k = jnp.where(live, jnp.where(dy >= 0, yp, yp - 1.0), 20.0)
        for t in range(1, 17):
            below[t] = below[t] + jnp.where(k < t, 1.0, 0.0)
        key.append((k.astype(I32) << 19) | cell)
        px.append(off_ref[0, s, :])
        py.append(dy)
        pz.append(off_ref[2, s, :])
        pm.append(jnp.where(live, mass_ref[s, :], 0.0))
    below = [None] + [jnp.sum(b).astype(I32) for b in below[1:]]
    ops = sort_network([key, px, py, pz, pm], lane, sub)
    ops[0] = [(k & ((1 << 19) - 1)).astype(F32) for k in ops[0]]
    for o in range(5):
        t = jnp.concatenate(ops[o], axis=0).T
        sorted_ref[o] = jnp.concatenate([t[:64], t[64:]], axis=1)
    starts, over = [], below[1] > FROWS * 128
    for p in range(GX):
        if p < GX - 1:
            begin = below[2 * p] if p else jnp.int32(0)
            w = jnp.minimum(begin // 128, NROW - ROWS)
            over = over | (below[2 * p + 3] > 128 * (w + ROWS))
        else:
            w = jnp.clip((count + 127) // 128 - ROWS, 0, NROW - ROWS)
            over = over | (below[2 * p] < 128 * w) | (below[2 * p + 2] < 128 * (w + ROWS - FROWS))
        starts.append(w)
    flag = jnp.where(over, 1.0, 0.0)
    for p in range(GX):
        for o in range(5):
            pay_ref[p, o * ROWS : (o + 1) * ROWS, :] = sorted_ref[o, pl.ds(starts[p], ROWS), :]
        pay_ref[p, 5 * ROWS : PAYROWS, :] = jnp.full((PAYROWS - 5 * ROWS, 128), flag, F32)


def sort_and_pack(count, cell, off, mass):
    return pl.pallas_call(
        sort_kernel,
        out_shape=(
            jax.ShapeDtypeStruct((5, NROW, 128), F32),
            jax.ShapeDtypeStruct((GX, PAYROWS, 128), F32),
        ),
        in_specs=[SM, VM, VM, VM],
        out_specs=(VM, VM),
        name="sort_pack",
        cost_estimate=pl.CostEstimate(flops=30000000, bytes_accessed=800000, transcendentals=0),
    )(count, cell, off, mass)


def x_cells():
    i = lax.broadcasted_iota(I32, (XR, 128), 0)
    i = jnp.where(i == 128, 0, jnp.where(i == 129, 129, jnp.where(i > 129, 200, i + 1)))
    return i.astype(F32).astype(BF)


def spread(grid, first, second, one, two):
    zero = jnp.zeros((), BF)
    return jnp.where(first, one, jnp.where(second, two, zero))


def paint_kernel(rows, add, skip, where_ref, *refs):
    if add:
        recv_ref, acc_ref, out_ref, val_ref, a_ref, z_ref = refs
    else:
        recv_ref, out_ref, val_ref, a_ref, z_ref = refs
    ybase = where_ref[0].astype(F32)

    def source(i, carry):
        def op(k):
            return recv_ref[i, k * rows : (k + 1) * rows, :]

        dx, dy, dz, m = op(1), op(2), op(3), op(4)
        xp, yp, zp = cells_of(op(0))
        y = yp - 1.0 - ybase
        y1 = y + jnp.where(dy >= 0, 1.0, -1.0)
        ax, ay, az = jnp.abs(dx), jnp.abs(dy), jnp.abs(dz)
        coarse = jnp.floor(az * 256.0) * (1.0 / 256.0)
        fine = az - coarse
        vals = [xp, xp + jnp.where(dx >= 0, 1.0, -1.0), zp - 1.0, zp - 1.0 + jnp.where(dz >= 0, 1.0, -1.0)]
        vals += [1.0 - coarse, coarse, -fine, fine]
        for j in range(2):
            mj = m * (jnp.where(y == j, 1.0 - ay, 0.0) + jnp.where(y1 == j, ay, 0.0))
            for w in (1.0 - ax, ax):
                vals += list(halves(mj * w))
        for n, v in enumerate(vals):
            val_ref[n] = v
        xi = x_cells()
        zi = lax.broadcasted_iota(I32, (128, 128), 0).astype(F32).astype(BF)
        for r in range(rows):

            def row(n, height):
                return jnp.broadcast_to(val_ref[n, r : r + 1, :].astype(BF), (height, 128))

            cols = slice(r * 128, (r + 1) * 128)
            first, second = xi == row(0, XR), xi == row(1, XR)
            for j in range(2):
                for h in range(2):
                    n = 8 + 4 * j + h
                    a_ref[(2 * j + h) * XR : (2 * j + h + 1) * XR, cols] = spread(xi, first, second, row(n, XR), row(n + 2, XR))
            first, second = zi == row(2, 128), zi == row(3, 128)
            z_ref[0:128, cols] = spread(zi, first, second, row(4, 128), row(5, 128))
            z_ref[128:256, cols] = spread(zi, first, second, row(6, 128), row(7, 128))
        o = lax.dot_general(a_ref[...], z_ref[...], (((1,), (1,)), ((), ())), preferred_element_type=F32)
        for j in range(2):
            high, low = o[2 * j * XR : (2 * j + 1) * XR], o[(2 * j + 1) * XR : (2 * j + 2) * XR]
            total = high[:, :128] + high[:, 128:] + low[:, :128]
            if add:
                total = total + acc_ref[i, j]
            out_ref[i, j] = total
        return carry

    if skip:

        @pl.when((where_ref[1] == 0) | (where_ref[1] == GX - 1))
        def _():
            lax.fori_loop(0, GX, source, 0)
    else:
        lax.fori_loop(0, GX, source, 0)


def paint(where, recv, acc=None, rows=ROWS, skip=False):
    add = acc is not None
    shape = jax.ShapeDtypeStruct((GX, 2, XR, 128), F32)
    return pl.pallas_call(
        functools.partial(paint_kernel, rows, add, skip),
        out_shape=shape,
        in_specs=[SM, VM] + ([VM] if add else []),
        out_specs=VM,
        scratch_shapes=[
            pltpu.VMEM((16, rows, 128), F32),
            pltpu.VMEM((4 * XR, rows * 128), BF),
            pltpu.VMEM((256, rows * 128), BF),
        ],
        input_output_aliases={2: 0} if add else {},
        name="paint",
        cost_estimate=pl.CostEstimate(flops=rows * 3000000, bytes_accessed=2000000, transcendentals=0),
    )(where, recv, *([acc] if add else []))


def face_kernel(count_ref, cell_ref, off_ref, mass_ref, low_ref, high_ref, val_ref, x_ref, v_ref):
    count = count_ref[0]
    slot = lax.broadcasted_iota(I32, (NROW, 128), 0) * 128 + lax.broadcasted_iota(I32, (NROW, 128), 1)
    m = jnp.where(slot < count, mass_ref[...], 0.0)
    dx, dy, dz = off_ref[0], off_ref[1], off_ref[2]
    xp, yp, zp = cells_of(cell_ref[...].astype(F32))
    up = (zp == 128.0) & (dz >= 0)
    down = (zp == 1.0) & (dz < 0)
    ax, ay = jnp.abs(dx), jnp.abs(dy)
    w = jnp.where(up | down, m * jnp.abs(dz), 0.0)
    coarse = jnp.floor(ax * 256.0) * (1.0 / 256.0)
    fine = ax - coarse
    y = yp + jnp.where(up, 24.0, 0.0)
    vals = [xp, xp + jnp.where(dx >= 0, 1.0, -1.0), 1.0 - coarse, coarse, -fine, fine]
    vals += [y, y + jnp.where(dy >= 0, 1.0, -1.0)]
    vals += [*halves(w * (1.0 - ay)), *halves(w * ay)]
    for n, v in enumerate(vals):
        val_ref[n] = v
    xi = x_cells()
    yi = lax.broadcasted_iota(I32, (48, 128), 0).astype(F32).astype(BF)

    def chunk(b, total):
        for r in range(16):

            def row(n, height):
                return jnp.broadcast_to(val_ref[n, pl.ds(b * 16 + r, 1), :].astype(BF), (height, 128))

            cols = slice(r * 128, (r + 1) * 128)
            first, second = xi == row(0, XR), xi == row(1, XR)
            x_ref[0:XR, cols] = spread(xi, first, second, row(2, XR), row(3, XR))
            x_ref[XR : 2 * XR, cols] = spread(xi, first, second, row(4, XR), row(5, XR))
            first, second = yi == row(6, 48), yi == row(7, 48)
            v_ref[0:48, cols] = spread(yi, first, second, row(8, 48), row(10, 48))
            v_ref[64:112, cols] = spread(yi, first, second, row(9, 48), row(11, 48))
        return total + lax.dot_general(x_ref[...], v_ref[...], (((1,), (1,)), ((), ())), preferred_element_type=F32)

    v_ref[...] = jnp.zeros(v_ref.shape, BF)
    o = lax.fori_loop(0, 4, chunk, jnp.zeros((2 * XR, 128), F32))
    g = o[0:XR] + pltpu.roll(o[0:XR], 64, 1) + o[XR : 2 * XR]
    t = g.T
    low_ref[0:24] = t[0:24, 0:128]
    high_ref[0:24] = t[24:48, 0:128]
    low_ref[24:32] = g[128:136]
    high_ref[24:32] = g[128:136]


def faces(count, cell, off, mass):
    shape = jax.ShapeDtypeStruct((32, 128), F32)
    return pl.pallas_call(
        face_kernel,
        out_shape=(shape, shape),
        in_specs=[SM, VM, VM, VM],
        out_specs=(VM, VM),
        scratch_shapes=[
            pltpu.VMEM((12, NROW, 128), F32),
            pltpu.VMEM((2 * XR, 2048), BF),
            pltpu.VMEM((128, 2048), BF),
        ],
        name="faces",
        cost_estimate=pl.CostEstimate(flops=8000000, bytes_accessed=200000, transcendentals=0),
    )(count, cell, off, mass)


def face_pack_kernel(low_ref, high_ref, out_ref):
    for p in range(GX):
        out_ref[p, 0:4] = low_ref[2 * p : 2 * p + 4]
        out_ref[p, 4:8] = high_ref[2 * p : 2 * p + 4]
        out_ref[p, 8:10] = low_ref[24:26]
        out_ref[p, 10:12] = high_ref[24:26]
        out_ref[p, 12:16] = jnp.zeros((4, 128), F32)


def face_pack(low, high):
    return pl.pallas_call(
        face_pack_kernel,
        out_shape=jax.ShapeDtypeStruct((GX, 16, 128), F32),
        in_specs=[VM, VM],
        out_specs=VM,
        name="face_pack",
        cost_estimate=pl.CostEstimate(flops=500000, bytes_accessed=100000, transcendentals=0),
    )(low, high)


def forward_kernel(where_ref, recv_ref, face_ref, out_ref):
    first = jnp.where(where_ref[1] == GX - 1, ROWS - FROWS, 0)
    flag = jnp.zeros((1, 128), F32)
    for i in range(GX):
        for o in range(5):
            out_ref[i, o * FROWS : (o + 1) * FROWS, :] = recv_ref[i, pl.ds(o * ROWS + first, FROWS), :]
        flag = jnp.maximum(flag, recv_ref[i, 5 * ROWS : 5 * ROWS + 1, :])
    for i in range(GX):
        out_ref[i, 40:52, :] = face_ref[i, 0:12, :]
        out_ref[i, 52:56, :] = jnp.broadcast_to(flag, (4, 128))


def forward_pack(where, recv, face):
    return pl.pallas_call(
        forward_kernel,
        out_shape=jax.ShapeDtypeStruct((GX, 56, 128), F32),
        in_specs=[SM, VM, VM],
        out_specs=VM,
        name="forward_pack",
        cost_estimate=pl.CostEstimate(flops=500000, bytes_accessed=600000, transcendentals=0),
    )(where, recv, face)


def table_kernel(high_ref, low_ref, base_ref):
    step = 2.0 * math.pi / 1024.0
    x = lax.broadcasted_iota(I32, (64, 1024), 1)
    k = lax.broadcasted_iota(I32, (64, 1024), 0)
    angle = ((k * x) & 1023).astype(F32) * step
    base_ref[0] = jnp.cos(angle)
    base_ref[1] = jnp.sin(angle)
    x = lax.broadcasted_iota(I32, (8, 1024), 1)
    k = lax.broadcasted_iota(I32, (8, 1024), 0)
    angle = ((64 * k * x) & 1023).astype(F32) * step
    scale = 1.0 / 32.0
    turn_c, turn_s = jnp.cos(angle) * scale, jnp.sin(angle) * scale
    for b in range(8):
        c, s = turn_c[b : b + 1], turn_s[b : b + 1]
        real = base_ref[0] * c - base_ref[1] * s
        imag = -(base_ref[0] * s + base_ref[1] * c)
        for part, value in ((0, real), (512, imag)):
            high = value.astype(BF)
            high_ref[part + 64 * b : part + 64 * b + 64] = high
            low_ref[part + 64 * b : part + 64 * b + 64] = (value - high.astype(F32)).astype(BF)


def tables():
    shape = jax.ShapeDtypeStruct((1024, 1024), BF)
    return pl.pallas_call(
        table_kernel,
        out_shape=(shape, shape),
        out_specs=(VM, VM),
        scratch_shapes=[pltpu.VMEM((2, 64, 1024), F32)],
        name="tables",
        cost_estimate=pl.CostEstimate(flops=8000000, bytes_accessed=4000000, transcendentals=0),
    )()


def final_kernel(where_ref, acc_ref, face_ref, in_ref, th_ref, tl_ref, dens_ref, spec_ref, dh_ref, dl_ref):
    p = where_ref[1]
    first, last = p == 0, p == GX - 1
    lane = lax.broadcasted_iota(I32, (8, 128), 1)
    lane1 = lax.broadcasted_iota(I32, (1, 128), 1)

    def face_rows(i, j):
        got = []
        for side in range(2):
            v = face_ref[i, 4 * side + 1 + j : 4 * side + 2 + j, :]
            if j == 0:
                v = v + jnp.where(first, in_ref[i, 40 + 4 * side + 3 : 40 + 4 * side + 4, :], 0.0)
            else:
                v = v + jnp.where(last, in_ref[i, 40 + 4 * side : 40 + 4 * side + 1, :], 0.0)
            got.append(v)
        return got

    def ghost(i, j, side, end):
        n = 8 + 2 * side + end
        base = 24 if side == 0 else 0
        v = jnp.sum(jnp.where(lane1 == base + 2 * p + 1 + j, face_ref[i, n : n + 1, :], 0.0), axis=1, keepdims=True)
        pick, on = (17, first) if j == 0 else (0, last)
        u = jnp.sum(jnp.where(lane1 == base + pick, in_ref[i, 40 + n : 41 + n, :], 0.0), axis=1, keepdims=True)
        return v + jnp.where(on, u, 0.0)

    wide = lax.broadcasted_iota(I32, (128, 128), 1)
    tall = lax.broadcasted_iota(I32, (128, 128), 0)
    for i in range(GX):
        before, after = (i - 1) % GX, (i + 1) % GX
        rows = []
        for j in range(2):
            for side, v in enumerate(face_rows(i, j)):
                v = v + jnp.where(lane1 == 127, ghost(after, j, side, 0), 0.0)
                v = v + jnp.where(lane1 == 0, ghost(before, j, side, 1), 0.0)
                rows.append(v)
        cols = jnp.concatenate(rows + [jnp.zeros((124, 128), F32)], axis=0).T
        for j in range(2):
            v = acc_ref[i, j, 0:128, :]
            v = v + jnp.where(tall == 127, acc_ref[after, j, 128:129, :], 0.0)
            v = v + jnp.where(tall == 0, acc_ref[before, j, 129:130, :], 0.0)
            v = v + jnp.where(wide == 0, cols[:, 2 * j : 2 * j + 1], 0.0)
            v = v + jnp.where(wide == 127, cols[:, 2 * j + 1 : 2 * j + 2], 0.0)
            dens_ref[pl.ds(i * 256 + j, 128, stride=2), :] = v
            high = v.astype(BF)
            dh_ref[i * 128 : (i + 1) * 128, j * 128 : (j + 1) * 128] = high
            dl_ref[i * 128 : (i + 1) * 128, j * 128 : (j + 1) * 128] = (v - high.astype(F32)).astype(BF)
    for b in range(4):
        rows = slice(b * 256, (b + 1) * 256)
        o = jnp.dot(th_ref[rows], dh_ref[...], preferred_element_type=F32)
        o = o + jnp.dot(th_ref[rows], dl_ref[...], preferred_element_type=F32)
        o = o + jnp.dot(tl_ref[rows], dh_ref[...], preferred_element_type=F32)
        for j in range(2):
            spec_ref[pl.ds(b * 512 + j, 256, stride=2), :] = o[:, j * 128 : (j + 1) * 128]


def finish(where, acc, face, received, th, tl):
    shape = jax.ShapeDtypeStruct((2048, 128), F32)
    return pl.pallas_call(
        final_kernel,
        out_shape=(shape, shape),
        in_specs=[SM] + [VM] * 5,
        out_specs=(VM, VM),
        scratch_shapes=[pltpu.VMEM((1024, 256), BF), pltpu.VMEM((1024, 256), BF)],
        name="finish",
        cost_estimate=pl.CostEstimate(flops=1600000000, bytes_accessed=8000000, transcendentals=0),
    )(where, acc, face, received, th, tl)


def y_pairs(blocks):
    pairs = []
    for q in range(blocks):
        pairs.append(((GX - 1) * blocks + q, (q + 1) % blocks))
        pairs.append((q, (GX - 1) * blocks + (q - 1) % blocks))
    return pairs


def exchange(x):
    return lax.all_to_all(x, "gx", split_axis=0, concat_axis=0, tiled=False)


def hand_on(x):
    return lax.ppermute(x, ("gx", "gy"), y_pairs(lax.axis_size("gy")))


def later_window(ordered, count, turn):
    xp, yp, zp = cells_of(ordered[0])
    live = ordered[4] != 0.0
    key = jnp.where(live, jnp.where(ordered[2] >= 0, yp, yp - 1.0), 20.0)
    space = jnp.zeros((5, NROW + 3 * ROWS, 128), F32)
    padded = jnp.concatenate([space, ordered, space], axis=1)
    base = NROW + 3 * ROWS
    blocks = []
    for p in range(GX):
        if p < GX - 1:
            begin = jnp.sum(jnp.where(key < 2 * p, 1, 0))
            w = jnp.minimum(begin // 128, NROW - ROWS) + turn * ROWS
        else:
            w = jnp.clip((count + 127) // 128 - ROWS, 0, NROW - ROWS) - turn * ROWS
        part = lax.dynamic_slice_in_dim(padded, base + w, ROWS, axis=1).reshape(5 * ROWS, 128)
        blocks.append(jnp.concatenate([part, jnp.zeros((PAYROWS - 5 * ROWS, 128), F32)], axis=0))
    return jnp.stack(blocks)


def body(cell_index, offsets, mass, counts):
    p = lax.axis_index("gx")
    blocks = lax.axis_size("gz")
    cell, off, m, count = cell_index.reshape(NROW, 128), offsets.reshape(3, NROW, 128), mass.reshape(NROW, 128), counts.reshape(1)
    here = jnp.stack([2 * p, p]).astype(I32)
    there = jnp.stack([jnp.where(p == 0, 16, -2), p]).astype(I32)

    ordered, pay = sort_and_pack(count, cell, off, m)
    recv = exchange(pay)

    low, high = faces(count, cell, off, m)
    from_below = lax.ppermute(high, "gz", [(i, (i + 1) % blocks) for i in range(blocks)])
    from_above = lax.ppermute(low, "gz", [((i + 1) % blocks, i) for i in range(blocks)])
    face = exchange(face_pack(from_below, from_above))
    th, tl = tables()

    passed = hand_on(forward_pack(here, recv, face))
    acc = paint(here, recv)
    acc = paint(there, passed[:, :40], acc, rows=FROWS, skip=True)

    mine = jnp.max(recv[:, 5 * ROWS, 0]) > 0
    theirs = passed[0, 52, 0] > 0

    def slow(acc):
        later = lax.cond(
            mine,
            lambda: jnp.stack([exchange(later_window(ordered, count[0], t)) for t in (1, 2, 3)]),
            lambda: jnp.zeros((3,) + recv.shape, F32),
        )
        first = jnp.where(p == GX - 1, ROWS - FROWS, 0)
        row = lax.broadcasted_iota(I32, (PAYROWS, 128), 0) - 4 * ROWS
        sent = (row >= first) & (row < first + FROWS)
        rest = jnp.where(sent, 0.0, recv)
        for t in range(3):
            acc = paint(here, later[t], acc)
        for x in [rest] + [later[t] for t in range(3)]:
            acc = paint(there, hand_on(x), acc, skip=True)
        return acc

    acc = lax.cond(mine | theirs, slow, lambda a: a, acc)
    density, spectrum = finish(here, acc, face, passed, th, tl)
    return density.reshape(1024, 1, 2, 128), spectrum.reshape(2, 512, 1, 2, 128)


def solution(mesh):
    placed = (
        P("gx", "gy", "gz", None),
        P("gx", "gy", "gz", None, None),
        P("gx", "gy", "gz", None),
        P("gx", "gy", "gz"),
    )
    return jax.shard_map(
        body,
        mesh=mesh,
        in_specs=placed,
        out_specs=(P(None, "gx", "gy", "gz"), P(None, None, "gx", "gy", "gz")),
        check_vma=False,
    )
```

```python
import functools
import math

import jax
import jax.numpy as jnp
from jax import lax
from jax.experimental import pallas as pl
from jax.experimental.pallas import tpu as pltpu
from jax.sharding import PartitionSpec as P

F32, I32, BF = jnp.float32, jnp.int32, jnp.bfloat16
GX = 8
ROWS = 17
FROWS = 8
NROW = 64
PAYROWS = 96
FACE = 5 * ROWS
XR = 136
LANE = {6: 64, 7: 1, 8: 2, 9: 4, 10: 8, 11: 16, 12: 32}
SUB = {3: 1, 4: 2, 5: 4}
ROOM = pltpu.CompilerParams(vmem_limit_bytes=12 * 1024 * 1024)
VM = pl.BlockSpec(memory_space=pltpu.VMEM)
SM = pl.BlockSpec(memory_space=pltpu.SMEM)


def cells_of(flat):
    row = jnp.floor((flat + 0.5) * (1.0 / 130.0))
    xp = jnp.floor((row + 0.5) * (1.0 / 18.0))
    return xp, row - 18.0 * xp, flat - 130.0 * row


def halves(value):
    high = value.astype(BF).astype(F32)
    return high, value - high


def index_bit(bit, lane, sub, reg):
    if bit < 3:
        return bool((reg >> bit) & 1)
    if bit in SUB:
        return (sub & SUB[bit]) != 0
    return (lane & LANE[bit]) != 0


def sort_network(ops, lane, sub):
    for size in range(1, 14):
        for bit in range(size - 1, -1, -1):
            new = [[None] * 8 for _ in ops]
            if bit < 3:
                for v in range(8):
                    w = v | (1 << bit)
                    if v == w:
                        continue
                    down = False if size == 13 else index_bit(size, lane, sub, v)
                    a, c = ops[0][v], ops[0][w]
                    if down is True:
                        move = a < c
                    elif down is False:
                        move = a > c
                    else:
                        move = ((a > c) ^ down) & (a != c)
                    for o in range(len(ops)):
                        a, c = ops[o][v], ops[o][w]
                        new[o][v] = jnp.where(move, c, a)
                        new[o][w] = jnp.where(move, a, c)
            else:
                axis, step, index = (0, SUB[bit], sub) if bit in SUB else (1, LANE[bit], lane)
                upper = (index & step) != 0
                other = index ^ step

                def partner(x):
                    if 2 * step == x.shape[axis]:
                        return pltpu.roll(x, step, axis)
                    if axis == 0:
                        return jnp.where(upper, pltpu.roll(x, step, 0), pltpu.roll(x, 8 - step, 0))
                    return jnp.take_along_axis(x, other, axis=axis)

                for v in range(8):
                    down = False if size == 13 else index_bit(size, lane, sub, v)
                    mine, theirs = ops[0][v], partner(ops[0][v])
                    if down is True:
                        big = ~upper
                    elif down is False:
                        big = upper
                    else:
                        big = upper ^ down
                    move = ((theirs > mine) & big) | ((theirs < mine) & ~big)
                    new[0][v] = jnp.where(move, theirs, mine)
                    for o in range(1, len(ops)):
                        new[o][v] = jnp.where(move, partner(ops[o][v]), ops[o][v])
            ops = new
    return ops


def sort_kernel(count_ref, cell_ref, off_ref, mass_ref, sorted_ref, start_ref):
    lane = lax.broadcasted_iota(I32, (8, 128), 1)
    sub = lax.broadcasted_iota(I32, (8, 128), 0)
    count = count_ref[0]
    key, px, py, pz, pm = [], [], [], [], []
    below = [jnp.zeros((8, 128), F32) for _ in range(17)]
    for v in range(8):
        s = slice(8 * v, 8 * v + 8)
        cell = cell_ref[s, :]
        dy = off_ref[1, s, :]
        live = v * 1024 + sub * 128 + lane < count
        _, yp, _ = cells_of(cell.astype(F32))
        k = jnp.where(live, jnp.where(dy >= 0, yp, yp - 1.0), 20.0)
        for t in range(1, 17):
            below[t] = below[t] + jnp.where(k < t, 1.0, 0.0)
        key.append((k.astype(I32) << 19) | cell)
        px.append(off_ref[0, s, :])
        py.append(dy)
        pz.append(off_ref[2, s, :])
        pm.append(jnp.where(live, mass_ref[s, :], 0.0))
    below = [None] + [jnp.sum(b).astype(I32) for b in below[1:]]
    ops = sort_network([key, px, py, pz, pm], lane, sub)
    ops[0] = [(k & ((1 << 19) - 1)).astype(F32) for k in ops[0]]
    for o in range(5):
        t = jnp.concatenate(ops[o], axis=0).T
        sorted_ref[o] = jnp.concatenate([t[:64], t[64:]], axis=1)
    over = below[1] > FROWS * 128
    for p in range(GX):
        if p < GX - 1:
            begin = below[2 * p] if p else jnp.int32(0)
            w = jnp.minimum(begin >> 7, NROW - ROWS)
            over = over | (below[2 * p + 3] > 128 * (w + ROWS))
        else:
            w = jnp.clip(((count + 127) >> 7) - ROWS, 0, NROW - ROWS)
            over = over | (below[2 * p] < 128 * w) | (below[2 * p + 2] < 128 * (w + ROWS - FROWS))
        start_ref[p] = w
    start_ref[GX] = over.astype(I32)


def sort_particles(count, cell, off, mass):
    return pl.pallas_call(
        sort_kernel,
        out_shape=(jax.ShapeDtypeStruct((5, NROW, 128), F32), jax.ShapeDtypeStruct((GX + 1,), I32)),
        in_specs=[SM, VM, VM, VM],
        out_specs=(VM, SM),
        name="sort_particles",
        compiler_params=ROOM,
        cost_estimate=pl.CostEstimate(flops=30000000, bytes_accessed=800000, transcendentals=0),
    )(count, cell, off, mass)


def pack_kernel(start_ref, part_ref, below_ref, above_ref, pay_ref):
    lane = lax.broadcasted_iota(I32, (2, 128), 1)
    ghosts = jnp.where(lane < 24, above_ref[24:26], below_ref[24:26])
    ghosts = jnp.where(lane < 64, ghosts, start_ref[GX].astype(F32))
    for p in range(GX):
        for o in range(5):
            pay_ref[p, o * ROWS : (o + 1) * ROWS, :] = part_ref[o, pl.ds(start_ref[p], ROWS), :]
        past = 17 if p == GX - 1 else 0
        for n, ref in enumerate((below_ref, above_ref)):
            pay_ref[p, FACE + 3 * n : FACE + 3 * n + 2, :] = ref[2 * p + 1 : 2 * p + 3]
            pay_ref[p, FACE + 3 * n + 2 : FACE + 3 * n + 3, :] = ref[past : past + 1]
        pay_ref[p, FACE + 6 : FACE + 8, :] = ghosts


def pack(start, ordered, below, above):
    return pl.pallas_call(
        pack_kernel,
        out_shape=jax.ShapeDtypeStruct((GX, PAYROWS, 128), F32),
        in_specs=[SM, VM, VM, VM],
        out_specs=VM,
        name="pack",
        compiler_params=ROOM,
        cost_estimate=pl.CostEstimate(flops=3000000, bytes_accessed=600000, transcendentals=0),
    )(start, ordered, below, above)


def spread(first, second, one, two):
    return jnp.where(first, one, jnp.where(second, two, jnp.zeros((), BF)))


def counting(height, start=0):
    return (lax.broadcasted_iota(I32, (height, 128), 0) + start).astype(F32).astype(BF)


def paint_sources(rows, together, acc_ref, where_ref, recv_ref, out_ref, val_ref):
    ybase = where_ref[0].astype(F32)
    grid = counting(16)
    ghost = lax.broadcasted_iota(I32, (16, 128), 0)
    ghost_cell = jnp.where(ghost >= 8, 200, jnp.where((ghost & 1) == 0, 0, 129)).astype(F32).astype(BF)
    ghost_row = (ghost >> 1).astype(F32).astype(BF)

    def prepare(i, slot):
        def op(k):
            return recv_ref[i, k * rows : (k + 1) * rows, :]

        dx, dy, dz, m = op(1), op(2), op(3), op(4)
        xp, yp, zp = cells_of(op(0))
        y = yp - 1.0 - ybase
        y1 = y + jnp.where(dy >= 0, 1.0, -1.0)
        ax, ay, az = jnp.abs(dx), jnp.abs(dy), jnp.abs(dz)
        coarse = jnp.floor(az * 256.0) * (1.0 / 256.0)
        fine = az - coarse
        vals = [xp, xp + jnp.where(dx >= 0, 1.0, -1.0), zp - 1.0, zp - 1.0 + jnp.where(dz >= 0, 1.0, -1.0)]
        vals += [1.0 - coarse, coarse, -fine, fine]
        for j in range(2):
            mj = m * (jnp.where(y == j, 1.0 - ay, 0.0) + jnp.where(y1 == j, ay, 0.0))
            for w in (1.0 - ax, ax):
                vals += list(halves(mj * w))
        for n, v in enumerate(vals):
            val_ref[slot, n, 0:rows] = v

    def operands(slot, r):
        def row(n):
            return jnp.broadcast_to(val_ref[slot, n, r : r + 1, :].astype(BF), (16, 128))

        x0, x1, z0, z1 = (row(n) for n in range(4))
        near = [row(8 + 4 * (c // 2) + c % 2) for c in range(4)]
        far = [row(10 + 4 * (c // 2) + c % 2) for c in range(4)]
        a = [[] for _ in range(4)]
        for g in range(8):
            cell = grid + float(16 * g + 1)
            first, second = cell == x0, cell == x1
            for c in range(4):
                a[c].append(spread(first, second, near[c], far[c]))
        w = far[3]
        for c in range(3):
            w = jnp.where(ghost_row == float(c), far[c], w)
        a = a[0] + a[1] + a[2] + a[3] + [jnp.where(ghost_cell == x1, w, jnp.zeros((), BF))]
        zc, zf = [], []
        weights = [row(n) for n in range(4, 8)]
        for g in range(8):
            cell = grid + float(16 * g)
            first, second = cell == z0, cell == z1
            zc.append(spread(first, second, weights[0], weights[1]))
            zf.append(spread(first, second, weights[2], weights[3]))
        return jnp.concatenate(a, axis=0), jnp.concatenate(zc + zf, axis=0)

    def source(i, slot):
        prepare(i, slot)
        o = None
        for t in range((rows + 1) // 2):
            pairs = [operands(slot, r) for r in range(2 * t, min(2 * t + 2, rows))]
            a = jnp.concatenate([pair[0] for pair in pairs], axis=1)
            z = jnp.concatenate([pair[1] for pair in pairs], axis=1)
            d = lax.dot_general(a, z, (((1,), (1,)), ((), ())), preferred_element_type=F32)
            o = d if o is None else o + d
        ends = o[512:520, :128] + o[512:520, 128:]
        ends = ends + pltpu.roll(ends, 6, 0)
        for j in range(2):
            high, low = o[256 * j : 256 * j + 128], o[256 * j + 128 : 256 * j + 256]
            total = high[:, :128] + high[:, 128:] + low[:, :128]
            end = ends if j == 0 else pltpu.roll(ends, 4, 0)
            if acc_ref is not None:
                total = total + acc_ref[i, j, 0:128]
                end = end + acc_ref[i, j, 128:136]
            out_ref[i, j, 0:128] = total
            out_ref[i, j, 128:136] = end

    def step(b, carry):
        for u in range(together):
            source(b * together + u, u)
        return carry

    lax.fori_loop(0, GX // together, step, 0)


def paint_kernel(where_ref, recv_ref, out_ref, val_ref):
    paint_sources(ROWS, 2, None, where_ref, recv_ref, out_ref, val_ref)


def paint_more_kernel(where_ref, recv_ref, acc_ref, out_ref, val_ref):
    paint_sources(ROWS, 1, acc_ref, where_ref, recv_ref, out_ref, val_ref)


def paint_handed_kernel(where_ref, over_ref, recv_ref, acc_ref, out_ref, flag_ref, val_ref):
    flag_ref[0] = over_ref[0]

    @pl.when((where_ref[1] == 0) | (where_ref[1] == GX - 1))
    def _():
        flag_ref[0] = jnp.maximum(over_ref[0], flagged(recv_ref, 5 * FROWS + 6))
        paint_sources(FROWS, 4, acc_ref, where_ref, recv_ref, out_ref, val_ref)


def flagged(ref, row):
    flag = ref[0, row : row + 1, :]
    for i in range(1, GX):
        flag = jnp.maximum(flag, ref[i, row : row + 1, :])
    return jnp.max(jnp.where(lax.broadcasted_iota(I32, (1, 128), 1) >= 64, flag, 0.0)).astype(I32)


def paint_scratch(together):
    return [pltpu.VMEM((together, 16, 24, 128), F32)]


PAINTED = jax.ShapeDtypeStruct((GX, 2, XR, 128), F32)


def paint(where, recv):
    return pl.pallas_call(
        paint_kernel,
        out_shape=PAINTED,
        in_specs=[SM, VM],
        out_specs=VM,
        scratch_shapes=paint_scratch(2),
        name="paint",
        compiler_params=ROOM,
        cost_estimate=pl.CostEstimate(flops=60000000, bytes_accessed=2000000, transcendentals=0),
    )(where, recv)


def paint_more(where, recv, acc):
    return pl.pallas_call(
        paint_more_kernel,
        out_shape=PAINTED,
        in_specs=[SM, VM, VM],
        out_specs=VM,
        scratch_shapes=paint_scratch(1),
        input_output_aliases={2: 0},
        name="paint_more",
        compiler_params=ROOM,
    )(where, recv, acc)


def paint_handed(where, over, recv, acc):
    return pl.pallas_call(
        paint_handed_kernel,
        out_shape=(PAINTED, jax.ShapeDtypeStruct((1,), I32)),
        in_specs=[SM, SM, VM, VM],
        out_specs=(VM, SM),
        scratch_shapes=paint_scratch(4),
        input_output_aliases={3: 0},
        name="paint_handed",
        compiler_params=ROOM,
        cost_estimate=pl.CostEstimate(flops=30000000, bytes_accessed=2000000, transcendentals=0),
    )(where, over, recv, acc)


def face_kernel(count_ref, cell_ref, off_ref, mass_ref, low_ref, high_ref, val_ref):
    slot = lax.broadcasted_iota(I32, (NROW, 128), 0) * 128 + lax.broadcasted_iota(I32, (NROW, 128), 1)
    m = jnp.where(slot < count_ref[0], mass_ref[...], 0.0)
    dx, dy, dz = off_ref[0], off_ref[1], off_ref[2]
    xp, yp, zp = cells_of(cell_ref[...].astype(F32))
    up = (zp == 128.0) & (dz >= 0)
    down = (zp == 1.0) & (dz < 0)
    ax, ay = jnp.abs(dx), jnp.abs(dy)
    w = jnp.where(up | down, m * jnp.abs(dz), 0.0)
    coarse = jnp.floor(ax * 256.0) * (1.0 / 256.0)
    fine = ax - coarse
    y = yp + jnp.where(up, 24.0, 0.0)
    vals = [xp, xp + jnp.where(dx >= 0, 1.0, -1.0), 1.0 - coarse, coarse, -fine, fine]
    vals += [y, y + jnp.where(dy >= 0, 1.0, -1.0)]
    vals += [*halves(w * (1.0 - ay)), *halves(w * ay)]
    for n, v in enumerate(vals):
        val_ref[n] = v
    grid = counting(16)
    ghost = lax.broadcasted_iota(I32, (16, 128), 0)
    ghost_cell = jnp.where(ghost >= 4, 200, jnp.where((ghost & 1) == 0, 0, 129)).astype(F32).astype(BF)
    ghost_fine = (ghost >> 1).astype(F32).astype(BF) == 1.0

    def operands(r):
        def row(n):
            return jnp.broadcast_to(val_ref[n, pl.ds(r, 1), :].astype(BF), (16, 128))

        x0, x1, y0, y1 = row(0), row(1), row(6), row(7)
        weights = [row(n) for n in (2, 3, 4, 5, 8, 10, 9, 11)]
        xc, xf, high, low = [], [], [], []
        for g in range(8):
            cell = grid + float(16 * g + 1)
            first, second = cell == x0, cell == x1
            xc.append(spread(first, second, weights[0], weights[1]))
            xf.append(spread(first, second, weights[2], weights[3]))
        ends = jnp.where(ghost_cell == x1, jnp.where(ghost_fine, weights[3], weights[1]), jnp.zeros((), BF))
        for g in range(3):
            cell = grid + float(16 * g)
            first, second = cell == y0, cell == y1
            high.append(spread(first, second, weights[4], weights[5]))
            low.append(spread(first, second, weights[6], weights[7]))
        gap = [jnp.zeros((16, 128), BF)]
        return jnp.concatenate(xc + xf + [ends], axis=0), jnp.concatenate(high + gap + low + gap, axis=0)

    def step(b, total):
        for t in range(8):
            pairs = [operands(16 * b + 2 * t + u) for u in range(2)]
            x = jnp.concatenate([pair[0] for pair in pairs], axis=1)
            v = jnp.concatenate([pair[1] for pair in pairs], axis=1)
            total = total + lax.dot_general(x, v, (((1,), (1,)), ((), ())), preferred_element_type=F32)
        return total

    o = lax.fori_loop(0, NROW // 16, step, jnp.zeros((272, 128), F32))
    o = o + pltpu.roll(o, 64, 1)
    t = (o[0:128] + o[128:256]).T
    ends = o[256:264] + pltpu.roll(o[256:264], 6, 0)
    low_ref[0:24] = t[0:24]
    high_ref[0:24] = t[24:48]
    low_ref[24:32] = ends
    high_ref[24:32] = ends


def faces(count, cell, off, mass):
    shape = jax.ShapeDtypeStruct((32, 128), F32)
    return pl.pallas_call(
        face_kernel,
        out_shape=(shape, shape),
        in_specs=[SM, VM, VM, VM],
        out_specs=(VM, VM),
        scratch_shapes=[pltpu.VMEM((12, NROW, 128), F32)],
        name="faces",
        compiler_params=ROOM,
        cost_estimate=pl.CostEstimate(flops=8000000, bytes_accessed=200000, transcendentals=0),
    )(count, cell, off, mass)


def forward_kernel(where_ref, recv_ref, table_ref, out_ref, over_ref):
    first = jnp.where(where_ref[1] == GX - 1, ROWS - FROWS, 0)
    for i in range(GX):
        for o in range(5):
            out_ref[i, o * FROWS : (o + 1) * FROWS, :] = recv_ref[i, pl.ds(o * ROWS + first, FROWS), :]
        out_ref[i, 5 * FROWS : 5 * FROWS + 8, :] = recv_ref[i, FACE : FACE + 8, :]
    over_ref[0] = flagged(recv_ref, FACE + 6)


def forward_pack(where, recv, table):
    return pl.pallas_call(
        forward_kernel,
        out_shape=(jax.ShapeDtypeStruct((GX, 5 * FROWS + 8, 128), F32), jax.ShapeDtypeStruct((1,), I32)),
        in_specs=[SM, VM, pl.BlockSpec(memory_space=pl.ANY)],
        out_specs=(VM, SM),
        name="forward_pack",
        compiler_params=ROOM,
        cost_estimate=pl.CostEstimate(flops=500000, bytes_accessed=600000, transcendentals=0),
    )(where, recv, table)


def table_kernel(high_ref, low_ref):
    scale = 1.0 / 32.0
    j = lax.broadcasted_iota(I32, (64, 128), 1)
    k8 = 8 * lax.broadcasted_iota(I32, (64, 128), 0)
    none = jnp.zeros((64, 128), F32)

    def turns(m):
        angle = (((k8 + m) * j) & 1023).astype(F32) * (2.0 * math.pi / 1024.0)
        return jnp.cos(angle) * scale, jnp.sin(angle) * scale

    for g, (m, w) in enumerate(((1, 7), (3, 5), (2, 6), (0, 4))):
        (c, s), (e, t) = turns(m), turns(w)
        if g < 3:
            parts = ((c, s), (-s, c), (e, -t), (-t, -e))
        else:
            parts = ((c, none), (-s, none), (none, e), (none, -t))
        for n, pair in enumerate(parts):
            for h, value in enumerate(pair):
                high = value.astype(BF)
                high_ref[g, 64 * n : 64 * n + 64, 128 * h : 128 * h + 128] = high
                low_ref[g, 64 * n : 64 * n + 64, 128 * h : 128 * h + 128] = (value - high.astype(F32)).astype(BF)


def tables():
    shape = jax.ShapeDtypeStruct((4, 256, 256), BF)
    return pl.pallas_call(
        table_kernel,
        out_shape=(shape, shape),
        out_specs=(VM, VM),
        name="tables",
        compiler_params=ROOM,
        cost_estimate=pl.CostEstimate(flops=8000000, bytes_accessed=1000000, transcendentals=0),
    )()


def final_kernel(where_ref, acc_ref, face_ref, in_ref, th_ref, tl_ref, dens_ref, spec_ref, x_ref):
    p = where_ref[1]
    first, last = p == 0, p == GX - 1
    lane1 = lax.broadcasted_iota(I32, (1, 128), 1)
    lane2 = lax.broadcasted_iota(I32, (2, 128), 1)

    def face_row(i, side, j):
        v = face_ref[i, FACE + 3 * side + j : FACE + 3 * side + j + 1, :]
        u = in_ref[i, 5 * FROWS + 3 * side + 2 : 5 * FROWS + 3 * side + 3, :]
        return v + jnp.where(first if j == 0 else last, u, 0.0)

    def ghosts(i):
        got = {}
        v, u = face_ref[i, FACE + 6 : FACE + 8, :], in_ref[i, 5 * FROWS + 6 : 5 * FROWS + 8, :]
        for side in range(2):
            base = 24 if side == 0 else 0
            for j in range(2):
                mine = jnp.where(lane2 == base + 2 * p + 1 + j, v, 0.0)
                handed = jnp.where((lane2 == base + (17 if j == 0 else 0)) & (first if j == 0 else last), u, 0.0)
                got[side, j] = jnp.sum(mine + handed, axis=1, keepdims=True)
        return got

    past = [ghosts(i) for i in range(GX)]
    wide = lax.broadcasted_iota(I32, (128, 128), 1)
    for i in range(GX):
        before, after = (i - 1) % GX, (i + 1) % GX
        rows = {}
        for side in range(2):
            for j in range(2):
                v = face_row(i, side, j)
                v = v + jnp.where(lane1 == 127, past[after][side, j][0:1], 0.0)
                rows[side, j] = v + jnp.where(lane1 == 0, past[before][side, j][1:2], 0.0)
        gap = jnp.zeros((4, 128), F32)
        cols = jnp.concatenate(
            [rows[0, 0], rows[0, 1], gap[:2], jnp.zeros((120, 128), F32), gap[:2], rows[1, 0], rows[1, 1]], axis=0
        ).T
        for j in range(2):
            shifted = pltpu.roll(cols, 1 if j == 0 else 127, 1)
            v = acc_ref[i, j, 0:128, :]
            if j == 0:
                v = v + jnp.where(wide == 0, cols, jnp.where(wide == 127, shifted, 0.0))
            else:
                v = v + jnp.where(wide == 127, cols, jnp.where(wide == 0, shifted, 0.0))
            x_ref[i, :, j * 128 : (j + 1) * 128] = v
            x_ref[i, 127:128, j * 128 : (j + 1) * 128] = v[127:128] + acc_ref[after, j, 128:129, :]
            x_ref[i, 0:1, j * 128 : (j + 1) * 128] = v[0:1] + acc_ref[before, j, 129:130, :]
            dens_ref[pl.ds(i * 256 + j, 128, stride=2), :] = x_ref[i, :, j * 128 : (j + 1) * 128]

    def even(b):
        return x_ref[b] + x_ref[b + 4]

    def odd(b):
        return x_ref[b] - x_ref[b + 4]

    root = math.sqrt(0.5)
    for g, (m, w) in enumerate(((1, 7), (3, 5), (2, 6), (0, 4))):
        if g < 2:
            d1, d3 = odd(1), odd(3)
            s, t = (d1 - d3) * root, (d1 + d3) * root
            pair = (odd(0) + s, -odd(2) - t) if g == 0 else (odd(0) - s, odd(2) - t)
        elif g == 2:
            pair = (even(0) - even(2), even(3) - even(1))
        else:
            s, t = even(0) + even(2), even(1) + even(3)
            pair = (s + t, s - t)
        value = jnp.concatenate(pair, axis=0)
        high = value.astype(BF)
        low = (value - high.astype(F32)).astype(BF)
        o = jnp.dot(th_ref[g], high, preferred_element_type=F32)
        o = o + jnp.dot(tl_ref[g], high, preferred_element_type=F32)
        o = o + jnp.dot(th_ref[g], low, preferred_element_type=F32)
        for n, (k, part) in enumerate(((m, 0), (m, 1), (w, 0), (w, 1))):
            for j in range(2):
                spec_ref[pl.ds(part * 1024 + 2 * k + j, 64, stride=16), :] = o[64 * n : 64 * n + 64, j * 128 : (j + 1) * 128]


def finish(where, acc, face, received, th, tl):
    shape = jax.ShapeDtypeStruct((2048, 128), F32)
    return pl.pallas_call(
        final_kernel,
        out_shape=(shape, shape),
        in_specs=[SM] + [VM] * 5,
        out_specs=(VM, VM),
        scratch_shapes=[pltpu.VMEM((GX, 128, 256), F32)],
        name="finish",
        compiler_params=ROOM,
        cost_estimate=pl.CostEstimate(flops=400000000, bytes_accessed=4000000, transcendentals=0),
    )(where, acc, face, received, th, tl)


def y_pairs(blocks):
    pairs = []
    for q in range(blocks):
        pairs.append(((GX - 1) * blocks + q, (q + 1) % blocks))
        pairs.append((q, (GX - 1) * blocks + (q - 1) % blocks))
    return pairs


def exchange(x):
    return lax.all_to_all(x, "gx", split_axis=0, concat_axis=0, tiled=False)


def hand_on(x):
    return lax.ppermute(x, ("gx", "gy"), y_pairs(lax.axis_size("gy")))


def later_window(ordered, count, turn):
    xp, yp, zp = cells_of(ordered[0])
    live = ordered[4] != 0.0
    key = jnp.where(live, jnp.where(ordered[2] >= 0, yp, yp - 1.0), 20.0)
    space = jnp.zeros((5, NROW + 3 * ROWS, 128), F32)
    padded = jnp.concatenate([space, ordered, space], axis=1)
    base = NROW + 3 * ROWS
    blocks = []
    for p in range(GX):
        if p < GX - 1:
            begin = jnp.sum(jnp.where(key < 2 * p, 1, 0))
            w = jnp.minimum(begin // 128, NROW - ROWS) + turn * ROWS
        else:
            w = jnp.clip((count + 127) // 128 - ROWS, 0, NROW - ROWS) - turn * ROWS
        part = lax.dynamic_slice_in_dim(padded, base + w, ROWS, axis=1).reshape(5 * ROWS, 128)
        blocks.append(jnp.concatenate([part, jnp.zeros((PAYROWS - 5 * ROWS, 128), F32)], axis=0))
    return jnp.stack(blocks)


def body(cell_index, offsets, mass, counts):
    p = lax.axis_index("gx")
    blocks = lax.axis_size("gz")
    cell, off, m, count = cell_index.reshape(NROW, 128), offsets.reshape(3, NROW, 128), mass.reshape(NROW, 128), counts.reshape(1)
    here = jnp.stack([2 * p, p]).astype(I32)
    there = jnp.stack([jnp.where(p == 0, 16, -2), p]).astype(I32)

    low, high = faces(count, cell, off, m)
    from_below = lax.ppermute(high, "gz", [(i, (i + 1) % blocks) for i in range(blocks)])
    from_above = lax.ppermute(low, "gz", [((i + 1) % blocks, i) for i in range(blocks)])
    ordered, start = sort_particles(count, cell, off, m)
    recv = exchange(pack(start, ordered, from_below, from_above))
    th, tl = tables()

    packed, mine = forward_pack(here, recv, th)
    passed = hand_on(packed)
    acc = paint(here, recv)
    acc, over = paint_handed(there, mine, passed, acc)

    def slow(acc):
        later = lax.cond(
            mine[0] > 0,
            lambda: jnp.stack([exchange(later_window(ordered, count[0], t)) for t in (1, 2, 3)]),
            lambda: jnp.zeros((3,) + recv.shape, F32),
        )
        first = jnp.where(p == GX - 1, ROWS - FROWS, 0)
        row = lax.broadcasted_iota(I32, (PAYROWS, 128), 0) - 4 * ROWS
        sent = (row >= first) & (row < first + FROWS)
        rest = jnp.where(sent, 0.0, recv)
        for t in range(3):
            acc = paint_more(here, later[t], acc)
        for x in [rest] + [later[t] for t in range(3)]:
            acc = paint_more(there, hand_on(x), acc)
        return acc

    acc = lax.cond(over[0] > 0, slow, lambda a: a, acc)
    density, spectrum = finish(here, acc, recv, passed, th, tl)
    return density.reshape(1024, 1, 2, 128), spectrum.reshape(2, 512, 1, 2, 128)


def solution(mesh):
    placed = (
        P("gx", "gy", "gz", None),
        P("gx", "gy", "gz", None, None),
        P("gx", "gy", "gz", None),
        P("gx", "gy", "gz"),
    )
    return jax.shard_map(
        body,
        mesh=mesh,
        in_specs=placed,
        out_specs=(P(None, "gx", "gy", "gz"), P(None, None, "gx", "gy", "gz")),
        check_vma=False,
    )
```

```python
import functools
import math

import jax
import jax.numpy as jnp
from jax import lax
from jax.experimental import pallas as pl
from jax.experimental.pallas import tpu as pltpu
from jax.sharding import PartitionSpec as P

F32, I32, BF = jnp.float32, jnp.int32, jnp.bfloat16
GX = 8
ROWS = 17
FROWS = 8
NROW = 64
PAYROWS = 96
FACE = 5 * ROWS
XR = 136
LANE = {6: 64, 7: 1, 8: 2, 9: 4, 10: 8, 11: 16, 12: 32}
SUB = {3: 1, 4: 2, 5: 4}
CELL = (1 << 19) - 1
FULL = pltpu.CompilerParams(vmem_limit_bytes=60 * 1024 * 1024)
ROOM = pltpu.CompilerParams(vmem_limit_bytes=12 * 1024 * 1024)
VM = pl.BlockSpec(memory_space=pltpu.VMEM)
SM = pl.BlockSpec(memory_space=pltpu.SMEM)
ANY = pl.BlockSpec(memory_space=pl.ANY)


def cells_of(flat):
    row = jnp.floor((flat + 0.5) * (1.0 / 130.0))
    xp = jnp.floor((row + 0.5) * (1.0 / 18.0))
    return xp, row - 18.0 * xp, flat - 130.0 * row


def halves(value):
    high = value.astype(BF).astype(F32)
    return high, value - high


def index_bit(bit, lane, sub, reg):
    if bit < 3:
        return bool((reg >> bit) & 1)
    if bit in SUB:
        return (sub & SUB[bit]) != 0
    return (lane & LANE[bit]) != 0


def sort_network(ops, lane, sub):
    for size in range(1, 14):
        for bit in range(size - 1, -1, -1):
            new = [[None] * 8 for _ in ops]
            if bit < 3:
                for v in range(8):
                    w = v | (1 << bit)
                    if v == w:
                        continue
                    down = False if size == 13 else index_bit(size, lane, sub, v)
                    a, c = ops[0][v], ops[0][w]
                    if down is True:
                        move = a < c
                    elif down is False:
                        move = a > c
                    else:
                        move = ((a > c) ^ down) & (a != c)
                    for o in range(len(ops)):
                        a, c = ops[o][v], ops[o][w]
                        new[o][v] = jnp.where(move, c, a)
                        new[o][w] = jnp.where(move, a, c)
            else:
                axis, step, index = (0, SUB[bit], sub) if bit in SUB else (1, LANE[bit], lane)
                upper = (index & step) != 0
                other = index ^ step

                def partner(x):
                    if 2 * step == x.shape[axis]:
                        return pltpu.roll(x, step, axis)
                    if axis == 0:
                        return jnp.where(upper, pltpu.roll(x, step, 0), pltpu.roll(x, 8 - step, 0))
                    return jnp.take_along_axis(x, other, axis=axis)

                for v in range(8):
                    down = False if size == 13 else index_bit(size, lane, sub, v)
                    mine, theirs = ops[0][v], partner(ops[0][v])
                    if down is True:
                        big = ~upper
                    elif down is False:
                        big = upper
                    else:
                        big = upper ^ down
                    move = ((theirs > mine) & big) | ((theirs < mine) & ~big)
                    new[0][v] = jnp.where(move, theirs, mine)
                    for o in range(1, len(ops)):
                        new[o][v] = jnp.where(move, partner(ops[o][v]), ops[o][v])
            ops = new
    return ops


def sort_and_pack(count, cell_ref, off_ref, mass_ref, low, high, ghosts, sorted_ref, pay_ref):
    lane = lax.broadcasted_iota(I32, (8, 128), 1)
    sub = lax.broadcasted_iota(I32, (8, 128), 0)
    below = [jnp.zeros((8, 128), F32) for _ in range(18)]
    ops = [[] for _ in range(5)]
    for v in range(8):
        s = slice(8 * v, 8 * v + 8)
        cell, dy = cell_ref[s, :], off_ref[1, s, :]
        live = v * 1024 + sub * 128 + lane < count
        _, yp, _ = cells_of(cell.astype(F32))
        row = jnp.where(live, jnp.where(dy >= 0, yp, yp - 1.0), 20.0)
        for t in range(1, 18):
            below[t] = below[t] + jnp.where(row < t, 1.0, 0.0)
        ops[0].append((row.astype(I32) << 19) | cell)
        for o in range(3):
            ops[o + 1].append(off_ref[o, s, :])
        ops[4].append(jnp.where(live, mass_ref[s, :], 0.0))
    below = [None] + [jnp.sum(b).astype(I32) for b in below[1:]]
    ops = sort_network(ops, lane, sub)
    ops[0] = [(k & CELL).astype(F32) for k in ops[0]]
    for o in range(5):
        t = jnp.concatenate(ops[o], axis=0).T
        sorted_ref[o] = jnp.concatenate([t[:64], t[64:]], axis=1)
    over = below[1] > FROWS * 128
    starts = []
    for p in range(GX):
        if p < GX - 1:
            begin = below[2 * p] if p else jnp.int32(0)
            w = jnp.minimum(begin >> 7, NROW - ROWS)
            over = over | (below[2 * p + 3] > 128 * (w + ROWS))
        else:
            w = jnp.clip(((below[17] + 127) >> 7) - ROWS, 0, NROW - ROWS)
            over = over | (below[2 * p] < 128 * w) | (below[2 * p + 2] < 128 * (w + ROWS - FROWS))
        starts.append(w)
    ghosts = jnp.where(lax.broadcasted_iota(I32, (2, 128), 1) < 64, ghosts, jnp.where(over, 1.0, 0.0))
    for p in range(GX):
        for o in range(5):
            pay_ref[p, o * ROWS : (o + 1) * ROWS, :] = sorted_ref[o, pl.ds(starts[p], ROWS), :]
        past = 17 if p == GX - 1 else 0
        rows = []
        for v in (low, high):
            rows += [v[2 * p + 1 : 2 * p + 3], v[past : past + 1]]
        pay_ref[p, FACE : FACE + 8, :] = jnp.concatenate(rows + [ghosts], axis=0)
        pay_ref[p, FACE + 8 : PAYROWS, :] = jnp.zeros((PAYROWS - FACE - 8, 128), F32)


def spread(first, second, one, two):
    return jnp.where(first, one, jnp.where(second, two, jnp.zeros((), BF)))


def counting(height, start=0):
    return (lax.broadcasted_iota(I32, (height, 128), 0) + start).astype(F32).astype(BF)


def paint_sources(rows, together, handed, acc_ref, recv_ref, out_ref, val_ref, begin=0, end=GX):
    p = lax.axis_index("gx")
    count = 1 if handed else 2
    grid = counting(16)
    ghost = lax.broadcasted_iota(I32, (16, 128), 0)
    ghost_cell = jnp.where(ghost >= 4 * count, 200, jnp.where((ghost & 1) == 0, 0, 129)).astype(F32).astype(BF)
    ghost_row = (ghost >> 1).astype(F32).astype(BF)

    def prepare(i, slot):
        def op(k):
            return recv_ref[i, k * rows : (k + 1) * rows, :]

        xp, yp, zp = cells_of(op(0))
        if handed:
            dx, dz, weights = op(1), op(2), [op(3)]
        else:
            dx, dy, dz, m = op(1), op(2), op(3), op(4)
            y = yp - (2 * p + 1).astype(F32)
            y1 = y + jnp.where(dy >= 0, 1.0, -1.0)
            ay = jnp.abs(dy)
            weights = [m * (jnp.where(y == j, 1.0 - ay, 0.0) + jnp.where(y1 == j, ay, 0.0)) for j in range(2)]
        ax, az = jnp.abs(dx), jnp.abs(dz)
        coarse = jnp.floor(az * 256.0) * (1.0 / 256.0)
        fine = az - coarse
        vals = [xp, xp + jnp.where(dx >= 0, 1.0, -1.0), zp - 1.0, zp - 1.0 + jnp.where(dz >= 0, 1.0, -1.0)]
        vals += [1.0 - coarse, coarse, -fine, fine]
        for mj in weights:
            for w in (1.0 - ax, ax):
                vals += list(halves(mj * w))
        for n, v in enumerate(vals):
            val_ref[slot, n, 0:rows] = v

    def operands(slot, r):
        def row(n):
            return jnp.broadcast_to(val_ref[slot, n, r : r + 1, :].astype(BF), (16, 128))

        x0, x1, z0, z1 = (row(n) for n in range(4))
        near = [row(8 + 4 * (c // 2) + c % 2) for c in range(2 * count)]
        far = [row(10 + 4 * (c // 2) + c % 2) for c in range(2 * count)]
        a = [[] for _ in range(2 * count)]
        for g in range(8):
            cell = grid + float(16 * g + 1)
            first, second = cell == x0, cell == x1
            for c in range(2 * count):
                a[c].append(spread(first, second, near[c], far[c]))
        w = far[-1]
        for c in range(2 * count - 1):
            w = jnp.where(ghost_row == float(c), far[c], w)
        a = sum(a, []) + [jnp.where(ghost_cell == x1, w, jnp.zeros((), BF))]
        zc, zf = [], []
        weights = [row(n) for n in range(4, 8)]
        for g in range(8):
            cell = grid + float(16 * g)
            first, second = cell == z0, cell == z1
            zc.append(spread(first, second, weights[0], weights[1]))
            zf.append(spread(first, second, weights[2], weights[3]))
        return jnp.concatenate(a, axis=0), jnp.concatenate(zc + zf, axis=0)

    def source(i, slot):
        prepare(i, slot)
        o = None
        for t in range((rows + 1) // 2):
            pairs = [operands(slot, r) for r in range(2 * t, min(2 * t + 2, rows))]
            a = jnp.concatenate([pair[0] for pair in pairs], axis=1)
            z = jnp.concatenate([pair[1] for pair in pairs], axis=1)
            d = lax.dot_general(a, z, (((1,), (1,)), ((), ())), preferred_element_type=F32)
            o = d if o is None else o + d
        ends = o[256 * count : 256 * count + 8, :128] + o[256 * count : 256 * count + 8, 128:]
        ends = ends + pltpu.roll(ends, 6, 0)
        for j in range(count):
            at = jnp.where(p == 0, 0, 1) if handed else j
            high, low = o[256 * j : 256 * j + 128], o[256 * j + 128 : 256 * j + 256]
            total = high[:, :128] + high[:, 128:] + low[:, :128]
            end = ends if j == 0 else pltpu.roll(ends, 4, 0)
            if acc_ref is not None:
                total = total + acc_ref[i, at, 0:128]
                end = end + acc_ref[i, at, 128:136]
            out_ref[i, at, 0:128] = total
            out_ref[i, at, 128:136] = end

    def step(b, carry):
        for u in range(together):
            source(b * together + u, u)
        return carry

    lax.fori_loop(begin // together, end // together, step, 0)


def waits_long():
    p = lax.axis_index("gx")
    return ((p == 0) | (p == GX - 1)) & (lax.axis_index("gy") % 4 == 0)


def paint_early_kernel(recv_ref, out_ref, val_ref):
    @pl.when(waits_long())
    def _():
        paint_sources(ROWS, 2, False, None, recv_ref, out_ref, val_ref, 0, EARLY)


def paint_late_kernel(recv_ref, after_ref, acc_ref, out_ref, val_ref):
    begin = jnp.where(waits_long(), EARLY, 0)
    paint_sources(ROWS, 2, False, None, recv_ref, out_ref, val_ref, begin)


def paint_more_kernel(handed, recv_ref, acc_ref, out_ref, val_ref):
    if handed:
        out_ref[...] = acc_ref[...]

        @pl.when((lax.axis_index("gx") == 0) | (lax.axis_index("gx") == GX - 1))
        def _():
            paint_sources(ROWS, 1, handed, acc_ref, recv_ref, out_ref, val_ref)
    else:
        paint_sources(ROWS, 1, handed, acc_ref, recv_ref, out_ref, val_ref)


def flagged(ref, row):
    flag = ref[0, row : row + 1, :]
    for i in range(1, GX):
        flag = jnp.maximum(flag, ref[i, row : row + 1, :])
    return jnp.max(jnp.where(lax.broadcasted_iota(I32, (1, 128), 1) >= 64, flag, 0.0)).astype(I32)


def paint_scratch(together):
    return [pltpu.VMEM((together, 16, 24, 128), F32)]


EARLY = 8
PAINTED = jax.ShapeDtypeStruct((GX, 2, XR, 128), F32)
PAINT_COST = pl.CostEstimate(flops=60000000, bytes_accessed=2000000, transcendentals=0)


def paint_early(recv):
    return pl.pallas_call(
        paint_early_kernel,
        out_shape=PAINTED,
        in_specs=[VM],
        out_specs=VM,
        scratch_shapes=paint_scratch(2),
        name="paint_early",
        compiler_params=ROOM,
        cost_estimate=PAINT_COST,
    )(recv)


def paint_late(recv, after, acc):
    return pl.pallas_call(
        paint_late_kernel,
        out_shape=PAINTED,
        in_specs=[VM, ANY, VM],
        out_specs=VM,
        scratch_shapes=paint_scratch(2),
        input_output_aliases={2: 0},
        name="paint_late",
        compiler_params=ROOM,
        cost_estimate=PAINT_COST,
    )(recv, after, acc)


def paint_more(recv, acc, handed=False):
    return pl.pallas_call(
        functools.partial(paint_more_kernel, handed),
        out_shape=PAINTED,
        in_specs=[VM, VM],
        out_specs=VM,
        scratch_shapes=paint_scratch(1),
        input_output_aliases={1: 0},
        name="paint_more",
        compiler_params=ROOM,
    )(recv, acc)


def paint_faces(count, cell_ref, off_ref, mass_ref, val_ref):
    slot = lax.broadcasted_iota(I32, (NROW, 128), 0) * 128 + lax.broadcasted_iota(I32, (NROW, 128), 1)
    m = jnp.where(slot < count, mass_ref[...], 0.0)
    dx, dy, dz = off_ref[0], off_ref[1], off_ref[2]
    xp, yp, zp = cells_of(cell_ref[...].astype(F32))
    up = (zp == 128.0) & (dz >= 0)
    down = (zp == 1.0) & (dz < 0)
    ax, ay = jnp.abs(dx), jnp.abs(dy)
    w = jnp.where(up | down, m * jnp.abs(dz), 0.0)
    coarse = jnp.floor(ax * 256.0) * (1.0 / 256.0)
    fine = ax - coarse
    y = yp + jnp.where(up, 24.0, 0.0)
    vals = [xp, xp + jnp.where(dx >= 0, 1.0, -1.0), 1.0 - coarse, coarse, -fine, fine]
    vals += [y, y + jnp.where(dy >= 0, 1.0, -1.0)]
    vals += [*halves(w * (1.0 - ay)), *halves(w * ay)]
    for n, v in enumerate(vals):
        val_ref[n] = v
    grid = counting(16)
    ghost = lax.broadcasted_iota(I32, (16, 128), 0)
    ghost_cell = jnp.where(ghost >= 4, 200, jnp.where((ghost & 1) == 0, 0, 129)).astype(F32).astype(BF)
    ghost_fine = (ghost >> 1).astype(F32).astype(BF) == 1.0

    def operands(r):
        def row(n):
            return jnp.broadcast_to(val_ref[n, pl.ds(r, 1), :].astype(BF), (16, 128))

        x0, x1, y0, y1 = row(0), row(1), row(6), row(7)
        weights = [row(n) for n in (2, 3, 4, 5, 8, 10, 9, 11)]
        xc, xf, high, low = [], [], [], []
        for g in range(8):
            cell = grid + float(16 * g + 1)
            first, second = cell == x0, cell == x1
            xc.append(spread(first, second, weights[0], weights[1]))
            xf.append(spread(first, second, weights[2], weights[3]))
        ends = jnp.where(ghost_cell == x1, jnp.where(ghost_fine, weights[3], weights[1]), jnp.zeros((), BF))
        for g in range(3):
            cell = grid + float(16 * g)
            first, second = cell == y0, cell == y1
            high.append(spread(first, second, weights[4], weights[5]))
            low.append(spread(first, second, weights[6], weights[7]))
        gap = [jnp.zeros((16, 128), BF)]
        return jnp.concatenate(xc + xf + [ends], axis=0), jnp.concatenate(high + gap + low + gap, axis=0)

    def step(b, total):
        for t in range(8):
            pairs = [operands(16 * b + 2 * t + u) for u in range(2)]
            x = jnp.concatenate([pair[0] for pair in pairs], axis=1)
            v = jnp.concatenate([pair[1] for pair in pairs], axis=1)
            total = total + lax.dot_general(x, v, (((1,), (1,)), ((), ())), preferred_element_type=F32)
        return total

    o = lax.fori_loop(0, NROW // 16, step, jnp.zeros((272, 128), F32))
    o = o + pltpu.roll(o, 64, 1)
    t = (o[0:128] + o[128:256]).T
    ends = o[256:264] + pltpu.roll(o[256:264], 6, 0)
    return t[0:24], t[24:48], ends[0:2]


def front_kernel(count_ref, cell_ref, off_ref, mass_ref, sorted_ref, pay_ref, val_ref):
    count = count_ref[0, 0, 0]
    low, high, ghosts = paint_faces(count, cell_ref, off_ref, mass_ref, val_ref)
    sort_and_pack(count, cell_ref, off_ref, mass_ref, low, high, ghosts, sorted_ref, pay_ref)


def front(count, cell, off, mass):
    return pl.pallas_call(
        front_kernel,
        out_shape=(jax.ShapeDtypeStruct((5, NROW, 128), F32), jax.ShapeDtypeStruct((GX, PAYROWS, 128), F32)),
        in_specs=[SM, VM, VM, VM],
        out_specs=(VM, VM),
        scratch_shapes=[pltpu.VMEM((12, NROW, 128), F32)],
        name="front",
        compiler_params=FULL,
        cost_estimate=pl.CostEstimate(flops=40000000, bytes_accessed=1000000, transcendentals=0),
    )(count, cell, off, mass)


def forward_kernel(recv_ref, table_ref, acc_ref, out_ref):
    last = lax.axis_index("gx") == GX - 1
    first = jnp.where(last, ROWS - FROWS, 0)
    row = jnp.where(last, 17.0, 0.0)
    for i in range(GX):
        cell, dx, dy, dz, m = (recv_ref[i, pl.ds(o * ROWS + first, FROWS), :] for o in range(5))
        _, yp, _ = cells_of(cell)
        ay = jnp.abs(dy)
        near = jnp.where(yp == row, 1.0 - ay, 0.0)
        weight = m * (near + jnp.where(yp + jnp.where(dy >= 0, 1.0, -1.0) == row, ay, 0.0))
        for o, v in enumerate((cell, dx, dz, weight)):
            out_ref[i, o * FROWS : (o + 1) * FROWS, :] = v
        out_ref[i, 4 * FROWS : 4 * FROWS + 8, :] = recv_ref[i, FACE : FACE + 8, :]


def forward_pack(recv, table, acc):
    return pl.pallas_call(
        forward_kernel,
        out_shape=jax.ShapeDtypeStruct((GX, 4 * FROWS + 8, 128), F32),
        in_specs=[VM, ANY, ANY],
        out_specs=VM,
        name="forward_pack",
        compiler_params=ROOM,
        cost_estimate=pl.CostEstimate(flops=500000, bytes_accessed=600000, transcendentals=0),
    )(recv, table, acc)


def table_kernel(high_ref, low_ref):
    scale = 1.0 / 32.0
    j = lax.broadcasted_iota(I32, (64, 128), 1)
    k8 = 8 * lax.broadcasted_iota(I32, (64, 128), 0)
    none = jnp.zeros((64, 128), F32)

    def turns(m):
        angle = (((k8 + m) * j) & 1023).astype(F32) * (2.0 * math.pi / 1024.0)
        return jnp.cos(angle) * scale, jnp.sin(angle) * scale

    for g, (m, w) in enumerate(((1, 7), (3, 5), (2, 6), (0, 4))):
        (c, s), (e, t) = turns(m), turns(w)
        if g < 3:
            parts = ((c, s), (-s, c), (e, -t), (-t, -e))
        else:
            parts = ((c, none), (-s, none), (none, e), (none, -t))
        for n, pair in enumerate(parts):
            for h, value in enumerate(pair):
                high = value.astype(BF)
                high_ref[g, 64 * n : 64 * n + 64, 128 * h : 128 * h + 128] = high
                low_ref[g, 64 * n : 64 * n + 64, 128 * h : 128 * h + 128] = (value - high.astype(F32)).astype(BF)


def tables():
    shape = jax.ShapeDtypeStruct((4, 256, 256), BF)
    return pl.pallas_call(
        table_kernel,
        out_shape=(shape, shape),
        out_specs=(VM, VM),
        name="tables",
        compiler_params=ROOM,
        cost_estimate=pl.CostEstimate(flops=8000000, bytes_accessed=1000000, transcendentals=0),
    )()


GROUPS = ((1, 7), (3, 5), (2, 6), (0, 4))


def transform(field, th_ref, tl_ref, put):
    root = math.sqrt(0.5)

    def even(b):
        return field(b) + field(b + 4)

    def odd(b):
        return field(b) - field(b + 4)

    for g in range(4):
        if g < 2:
            d1, d3 = odd(1), odd(3)
            s, t = (d1 - d3) * root, (d1 + d3) * root
            pair = (odd(0) + s, -odd(2) - t) if g == 0 else (odd(0) - s, odd(2) - t)
        elif g == 2:
            pair = (even(0) - even(2), even(3) - even(1))
        else:
            s, t = even(0) + even(2), even(1) + even(3)
            pair = (s + t, s - t)
        value = jnp.concatenate(pair, axis=0)
        high = value.astype(BF)
        low = (value - high.astype(F32)).astype(BF)
        o = jnp.dot(th_ref[g], high, preferred_element_type=F32)
        o = o + jnp.dot(tl_ref[g], high, preferred_element_type=F32)
        put(g, o + jnp.dot(th_ref[g], low, preferred_element_type=F32))


def face_columns(i, rows, ghosts):
    before, after = (i - 1) % GX, (i + 1) % GX
    lane = lax.broadcasted_iota(I32, (1, 128), 1)
    out = []
    for side in range(2):
        v = rows[i][side] + jnp.where(lane == 127, ghosts[after][side][0:1], 0.0)
        out.append(v + jnp.where(lane == 0, ghosts[before][side][1:2], 0.0))
    return out


def pick(v, lane):
    return jnp.sum(jnp.where(lax.broadcasted_iota(I32, (2, 128), 1) == lane, v, 0.0), axis=1, keepdims=True)


def along_z_kernel(face_ref, in_ref, down_ref, up_ref):
    p = lax.axis_index("gx")
    for j in range(2):
        on = p == (0 if j == 0 else GX - 1)
        rows, ghosts = [], []
        for i in range(GX):
            own, handed = face_ref[i, FACE : FACE + 8, :], in_ref[i, 4 * FROWS : 4 * FROWS + 8, :]
            rows.append([own[3 * n + j : 3 * n + j + 1] + jnp.where(on, handed[3 * n + 2 : 3 * n + 3], 0.0) for n in range(2)])
            past = [pick(own[6:8], base + 2 * p + 1 + j) for base in (0, 24)]
            more = [pick(handed[6:8], base + (17 if j == 0 else 0)) for base in (0, 24)]
            ghosts.append([a + jnp.where(on, b, 0.0) for a, b in zip(past, more)])
        for i in range(GX):
            down, up = face_columns(i, rows, ghosts)
            down_ref[2 * i + j : 2 * i + j + 1] = down
            up_ref[2 * i + j : 2 * i + j + 1] = up


def along_z(recv, passed):
    shape = jax.ShapeDtypeStruct((2 * GX, 128), F32)
    return pl.pallas_call(
        along_z_kernel,
        out_shape=(shape, shape),
        in_specs=[VM, VM],
        out_specs=(VM, VM),
        name="along_z",
        compiler_params=ROOM,
        cost_estimate=pl.CostEstimate(flops=500000, bytes_accessed=100000, transcendentals=0),
    )(recv, passed)


def handed_kernel(in_ref, acc_ref, out_ref, val_ref):
    p = lax.axis_index("gx")

    @pl.when((p == 0) | (p == GX - 1))
    def _():
        paint_sources(FROWS, 4, True, acc_ref, in_ref, out_ref, val_ref)


def paint_handed(passed, acc):
    return pl.pallas_call(
        handed_kernel,
        out_shape=PAINTED,
        in_specs=[VM, VM],
        out_specs=VM,
        scratch_shapes=paint_scratch(4),
        input_output_aliases={1: 0},
        name="paint_handed",
        compiler_params=ROOM,
        cost_estimate=PAINT_COST,
    )(passed, acc)


def finish_kernel(acc_ref, face_ref, in_ref, below_ref, above_ref, th_ref, tl_ref, dens_ref, spec_ref, flag_ref, x_ref):
    p = lax.axis_index("gx")
    flag_ref[0] = flagged(face_ref, FACE + 6)

    @pl.when((p == 0) | (p == GX - 1))
    def _():
        flag_ref[0] = jnp.maximum(flag_ref[0], flagged(in_ref, 4 * FROWS + 6))

    wide = lax.broadcasted_iota(I32, (128, 128), 1)
    for i in range(GX):
        before, after = (i - 1) % GX, (i + 1) % GX
        gap = jnp.zeros((124, 128), F32)
        t = jnp.concatenate([below_ref[2 * i : 2 * i + 2], gap, above_ref[2 * i : 2 * i + 2]], axis=0).T
        for j in range(2):
            shifted = pltpu.roll(t, 1 if j == 0 else 127, 1)
            low, high = (t, shifted) if j == 0 else (shifted, t)
            v = acc_ref[i, j, 0:128, :] + jnp.where(wide == 0, low, jnp.where(wide == 127, high, 0.0))
            cols = slice(j * 128, (j + 1) * 128)
            x_ref[i, :, cols] = v
            x_ref[i, 127:128, cols] = v[127:128] + acc_ref[after, j, 128:129, :]
            x_ref[i, 0:1, cols] = v[0:1] + acc_ref[before, j, 129:130, :]
            dens_ref[pl.ds(i * 256 + j, 128, stride=2), :] = x_ref[i, :, cols]

    def put(g, o):
        m, w = GROUPS[g]
        for n, (k, part) in enumerate(((m, 0), (m, 1), (w, 0), (w, 1))):
            for j in range(2):
                spec_ref[pl.ds(part * 1024 + 2 * k + j, 64, stride=16), :] = o[64 * n : 64 * n + 64, j * 128 : (j + 1) * 128]

    transform(lambda b: x_ref[b], th_ref, tl_ref, put)


def finish(acc, recv, passed, below, above, th, tl):
    shape = jax.ShapeDtypeStruct((2048, 128), F32)
    return pl.pallas_call(
        finish_kernel,
        out_shape=(shape, shape, jax.ShapeDtypeStruct((1,), I32)),
        in_specs=[VM] * 7,
        out_specs=(VM, VM, SM),
        scratch_shapes=[pltpu.VMEM((GX, 128, 256), F32)],
        name="finish",
        compiler_params=ROOM,
        cost_estimate=pl.CostEstimate(flops=400000000, bytes_accessed=4000000, transcendentals=0),
    )(acc, recv, passed, below, above, th, tl)


def y_pairs(blocks):
    pairs = []
    for q in range(blocks):
        pairs.append(((GX - 1) * blocks + q, (q + 1) % blocks))
        pairs.append((q, (GX - 1) * blocks + (q - 1) % blocks))
    return pairs


def exchange(x):
    return lax.all_to_all(x, "gx", split_axis=0, concat_axis=0, tiled=False)


def hand_on(x):
    return lax.ppermute(x, ("gx", "gy"), y_pairs(lax.axis_size("gy")))


def weighted(block):
    cell, dx, dy, dz, m = (block[:, o * ROWS : (o + 1) * ROWS] for o in range(5))
    row = jnp.where(lax.axis_index("gx") == GX - 1, 17.0, 0.0)
    _, yp, _ = cells_of(cell)
    ay = jnp.abs(dy)
    far = yp + jnp.where(dy >= 0, 1.0, -1.0)
    weight = m * (jnp.where(yp == row, 1.0 - ay, 0.0) + jnp.where(far == row, ay, 0.0))
    return jnp.concatenate([cell, dx, dz, weight, jnp.zeros((GX, PAYROWS - 4 * ROWS, 128), F32)], axis=1)


def later_window(ordered, turn):
    xp, yp, zp = cells_of(ordered[0])
    live = ordered[4] != 0.0
    key = jnp.where(live, jnp.where(ordered[2] >= 0, yp, yp - 1.0), 20.0)
    space = jnp.zeros((5, NROW + 3 * ROWS, 128), F32)
    padded = jnp.concatenate([space, ordered, space], axis=1)
    base = NROW + 3 * ROWS
    blocks = []
    for p in range(GX):
        if p < GX - 1:
            begin = jnp.sum(jnp.where(key < 2 * p, 1, 0))
            w = jnp.minimum(begin // 128, NROW - ROWS) + turn * ROWS
        else:
            w = jnp.clip((jnp.sum(jnp.where(live, 1, 0)) + 127) // 128 - ROWS, 0, NROW - ROWS) - turn * ROWS
        part = lax.dynamic_slice_in_dim(padded, base + w, ROWS, axis=1).reshape(5 * ROWS, 128)
        blocks.append(jnp.concatenate([part, jnp.zeros((PAYROWS - 5 * ROWS, 128), F32)], axis=0))
    return jnp.stack(blocks)


def body(cell_index, offsets, mass, counts):
    p = lax.axis_index("gx")
    blocks = lax.axis_size("gz")
    ordered, pay = front(counts, cell_index.reshape(NROW, 128), offsets.reshape(3, NROW, 128), mass.reshape(NROW, 128))
    recv = exchange(pay)
    th, tl = tables()

    acc = paint_early(recv)
    packed = forward_pack(recv, th, acc)
    passed = hand_on(packed)
    acc = paint_late(recv, packed, acc)
    down, up = along_z(recv, passed)
    below = lax.ppermute(up, "gz", [(i, (i + 1) % blocks) for i in range(blocks)])
    above = lax.ppermute(down, "gz", [((i + 1) % blocks, i) for i in range(blocks)])
    acc = paint_handed(passed, acc)
    density, spectrum, over = finish(acc, recv, passed, below, above, th, tl)

    def slow(outputs):
        mine = jnp.max(recv[:, FACE + 6, 64:]) > 0
        later = lax.cond(
            mine,
            lambda: tuple(exchange(later_window(ordered, t)) for t in (1, 2, 3)),
            lambda: (jnp.zeros(recv.shape, F32),) * 3,
        )
        first = jnp.where(p == GX - 1, ROWS - FROWS, 0)
        row = lax.broadcasted_iota(I32, (PAYROWS, 128), 0) - 4 * ROWS
        sent = (row >= first) & (row < first + FROWS)
        rest = jnp.where(sent, 0.0, recv)
        acc = jnp.zeros(PAINTED.shape, F32)
        for x in (recv, *later):
            acc = paint_more(x, acc)
        for x in (rest, *later):
            acc = paint_more(hand_on(weighted(x)), acc, handed=True)
        acc = paint_handed(passed, acc)
        density, spectrum, _ = finish(acc, recv, passed, below, above, th, tl)
        return density, spectrum

    density, spectrum = lax.cond(over[0] > 0, slow, lambda outputs: outputs, (density, spectrum))
    return density.reshape(1024, 1, 2, 128), spectrum.reshape(2, 512, 1, 2, 128)


def solution(mesh):
    placed = (
        P("gx", "gy", "gz", None),
        P("gx", "gy", "gz", None, None),
        P("gx", "gy", "gz", None),
        P("gx", "gy", "gz"),
    )
    return jax.shard_map(
        body,
        mesh=mesh,
        in_specs=placed,
        out_specs=(P(None, "gx", "gy", "gz"), P(None, None, "gx", "gy", "gz")),
        check_vma=False,
    )
```

```python
import functools
import math

import jax
import jax.numpy as jnp
from jax import lax
from jax.experimental import pallas as pl
from jax.experimental.pallas import tpu as pltpu
from jax.sharding import PartitionSpec as P

F32, I32, BF = jnp.float32, jnp.int32, jnp.bfloat16
GX = 8
ROWS = 17
FROWS = 7
NROW = 64
HANDED = 4 * FROWS + 4
PAYROWS = 96
FACE = 5 * ROWS
XR = 136
LANE = {6: 64, 7: 1, 8: 2, 9: 4, 10: 8, 11: 16, 12: 32}
SUB = {3: 1, 4: 2, 5: 4}
CELL = (1 << 19) - 1
FULL = pltpu.CompilerParams(vmem_limit_bytes=60 * 1024 * 1024)
ROOM = pltpu.CompilerParams(vmem_limit_bytes=12 * 1024 * 1024)
VM = pl.BlockSpec(memory_space=pltpu.VMEM)
SM = pl.BlockSpec(memory_space=pltpu.SMEM)
ANY = pl.BlockSpec(memory_space=pl.ANY)


def cells_of(flat):
    row = jnp.floor((flat + 0.5) * (1.0 / 130.0))
    xp = jnp.floor((row + 0.5) * (1.0 / 18.0))
    return xp, row - 18.0 * xp, flat - 130.0 * row


def halves(value):
    high = value.astype(BF).astype(F32)
    return high, value - high


def index_bit(bit, lane, sub, reg):
    if bit < 3:
        return bool((reg >> bit) & 1)
    if bit in SUB:
        return (sub & SUB[bit]) != 0
    return (lane & LANE[bit]) != 0


def sort_network(ops, lane, sub):
    for size in range(1, 14):
        for bit in range(size - 1, -1, -1):
            new = [[None] * 8 for _ in ops]
            if bit < 3:
                for v in range(8):
                    w = v | (1 << bit)
                    if v == w:
                        continue
                    down = False if size == 13 else index_bit(size, lane, sub, v)
                    a, c = ops[0][v], ops[0][w]
                    if down is True:
                        move = a < c
                    elif down is False:
                        move = a > c
                    else:
                        move = jnp.where(down, c, a) > jnp.where(down, a, c)
                    for o in range(len(ops)):
                        a, c = ops[o][v], ops[o][w]
                        new[o][v] = jnp.where(move, c, a)
                        new[o][w] = jnp.where(move, a, c)
            else:
                axis, step, index = (0, SUB[bit], sub) if bit in SUB else (1, LANE[bit], lane)
                upper = (index & step) != 0
                other = index ^ step

                def partner(x):
                    if 2 * step == x.shape[axis]:
                        return pltpu.roll(x, step, axis)
                    if axis == 0:
                        return jnp.where(upper, pltpu.roll(x, step, 0), pltpu.roll(x, 8 - step, 0))
                    return jnp.take_along_axis(x, other, axis=axis)

                for v in range(8):
                    down = False if size == 13 else index_bit(size, lane, sub, v)
                    mine, theirs = ops[0][v], partner(ops[0][v])
                    if down is True:
                        big = ~upper
                    elif down is False:
                        big = upper
                    else:
                        big = upper ^ down
                    move = jnp.where(big, theirs, mine) > jnp.where(big, mine, theirs)
                    new[0][v] = jnp.where(move, theirs, mine)
                    for o in range(1, len(ops)):
                        new[o][v] = jnp.where(move, partner(ops[o][v]), ops[o][v])
            ops = new
    return ops


def sort_and_pack(count, cell_ref, off_ref, mass_ref, low, high, ghosts, sorted_ref, pay_ref):
    lane = lax.broadcasted_iota(I32, (8, 128), 1)
    sub = lax.broadcasted_iota(I32, (8, 128), 0)
    below = [jnp.zeros((8, 128), F32) for _ in range(18)]
    ops = [[] for _ in range(5)]
    for v in range(8):
        s = slice(8 * v, 8 * v + 8)
        cell, dy = cell_ref[s, :], off_ref[1, s, :]
        live = v * 1024 + sub * 128 + lane < count
        _, yp, _ = cells_of(cell.astype(F32))
        row = jnp.where(live, jnp.where(dy >= 0, yp, yp - 1.0), 20.0)
        for t in range(1, 18):
            below[t] = below[t] + jnp.where(row < t, 1.0, 0.0)
        ops[0].append((row.astype(I32) << 19) | cell)
        for o in range(3):
            ops[o + 1].append(off_ref[o, s, :])
        ops[4].append(jnp.where(live, mass_ref[s, :], 0.0))
    below = [None] + [jnp.sum(b).astype(I32) for b in below[1:]]
    ops = sort_network(ops, lane, sub)
    ops[0] = [(k & CELL).astype(F32) for k in ops[0]]
    for o in range(5):
        t = jnp.concatenate(ops[o], axis=0).T
        sorted_ref[o] = jnp.concatenate([t[:64], t[64:]], axis=1)
    over = below[1] > FROWS * 128
    starts = []
    for p in range(GX):
        if p < GX - 1:
            begin = below[2 * p] if p else jnp.int32(0)
            w = jnp.minimum(begin >> 7, NROW - ROWS)
            over = over | (below[2 * p + 3] > 128 * (w + ROWS))
        else:
            w = jnp.clip(((below[17] + 127) >> 7) - ROWS, 0, NROW - ROWS)
            over = over | (below[2 * p] < 128 * w) | (below[2 * p + 2] < 128 * (w + ROWS - FROWS))
        starts.append(w)
    ghosts = jnp.where(lax.broadcasted_iota(I32, (2, 128), 1) < 64, ghosts, jnp.where(over, 1.0, 0.0))
    for p in range(GX):
        for o in range(5):
            pay_ref[p, o * ROWS : (o + 1) * ROWS, :] = sorted_ref[o, pl.ds(starts[p], ROWS), :]
        past = 17 if p == GX - 1 else 0
        rows = []
        for v in (low, high):
            rows += [v[2 * p + 1 : 2 * p + 3], v[past : past + 1]]
        pay_ref[p, FACE : FACE + 8, :] = jnp.concatenate(rows + [ghosts], axis=0)
        pay_ref[p, FACE + 8 : PAYROWS, :] = jnp.zeros((PAYROWS - FACE - 8, 128), F32)


def spread(first, second, one, two):
    return jnp.where(first, one, jnp.where(second, two, jnp.zeros((), BF)))


def counting(height, start=0):
    return (lax.broadcasted_iota(I32, (height, 128), 0) + start).astype(F32).astype(BF)


def paint_sources(rows, together, handed, acc_ref, recv_ref, out_ref, val_ref, begin=0, end=GX):
    p = lax.axis_index("gx")
    count = 1 if handed else 2
    grid = counting(16)
    ghost = lax.broadcasted_iota(I32, (16, 128), 0)
    ghost_cell = jnp.where(ghost >= 4 * count, 200, jnp.where((ghost & 1) == 0, 0, 129)).astype(F32).astype(BF)
    ghost_row = (ghost >> 1).astype(F32).astype(BF)

    def prepare(i, slot):
        def op(k):
            return recv_ref[i, k * rows : (k + 1) * rows, :]

        xp, yp, zp = cells_of(op(0))
        if handed:
            dx, dz, weights = op(1), op(2), [op(3)]
        else:
            dx, dy, dz, m = op(1), op(2), op(3), op(4)
            y = yp - (2 * p + 1).astype(F32)
            y1 = y + jnp.where(dy >= 0, 1.0, -1.0)
            ay = jnp.abs(dy)
            weights = [m * (jnp.where(y == j, 1.0 - ay, 0.0) + jnp.where(y1 == j, ay, 0.0)) for j in range(2)]
        ax, az = jnp.abs(dx), jnp.abs(dz)
        coarse = jnp.floor(az * 256.0) * (1.0 / 256.0)
        fine = az - coarse
        vals = [xp, xp + jnp.where(dx >= 0, 1.0, -1.0), zp - 1.0, zp - 1.0 + jnp.where(dz >= 0, 1.0, -1.0)]
        vals += [1.0 - coarse, coarse, -fine, fine]
        for mj in weights:
            for w in (1.0 - ax, ax):
                vals += list(halves(mj * w))
        for n, v in enumerate(vals):
            val_ref[slot, n, 0:rows] = v

    def operands(slot, r):
        def row(n):
            return jnp.broadcast_to(val_ref[slot, n, r : r + 1, :].astype(BF), (16, 128))

        x0, x1, z0, z1 = (row(n) for n in range(4))
        near = [row(8 + 4 * (c // 2) + c % 2) for c in range(2 * count)]
        far = [row(10 + 4 * (c // 2) + c % 2) for c in range(2 * count)]
        a = [[] for _ in range(2 * count)]
        for g in range(8):
            cell = grid + float(16 * g + 1)
            first, second = cell == x0, cell == x1
            for c in range(2 * count):
                a[c].append(spread(first, second, near[c], far[c]))
        w = far[-1]
        for c in range(2 * count - 1):
            w = jnp.where(ghost_row == float(c), far[c], w)
        a = sum(a, []) + [jnp.where(ghost_cell == x1, w, jnp.zeros((), BF))]
        zc, zf = [], []
        weights = [row(n) for n in range(4, 8)]
        for g in range(8):
            cell = grid + float(16 * g)
            first, second = cell == z0, cell == z1
            zc.append(spread(first, second, weights[0], weights[1]))
            zf.append(spread(first, second, weights[2], weights[3]))
        return jnp.concatenate(a, axis=0), jnp.concatenate(zc + zf, axis=0)

    def source(i, slot):
        prepare(i, slot)
        o = None
        for t in range((rows + 1) // 2):
            pairs = [operands(slot, r) for r in range(2 * t, min(2 * t + 2, rows))]
            a = jnp.concatenate([pair[0] for pair in pairs], axis=1)
            z = jnp.concatenate([pair[1] for pair in pairs], axis=1)
            d = lax.dot_general(a, z, (((1,), (1,)), ((), ())), preferred_element_type=F32)
            o = d if o is None else o + d
        ends = o[256 * count : 256 * count + 8, :128] + o[256 * count : 256 * count + 8, 128:]
        ends = ends + pltpu.roll(ends, 6, 0)
        for j in range(count):
            at = jnp.where(p == 0, 0, 1) if handed else j
            high, low = o[256 * j : 256 * j + 128], o[256 * j + 128 : 256 * j + 256]
            total = high[:, :128] + high[:, 128:] + low[:, :128]
            end = ends if j == 0 else pltpu.roll(ends, 4, 0)
            if acc_ref is not None:
                total = total + acc_ref[i, at, 0:128]
                end = end + acc_ref[i, at, 128:136]
            out_ref[i, at, 0:128] = total
            out_ref[i, at, 128:136] = end

    def step(b, carry):
        for u in range(together):
            source(b * together + u, u)
        return carry

    lax.fori_loop(begin // together, end // together, step, 0)


def waits_long():
    p = lax.axis_index("gx")
    return ((p == 0) | (p == GX - 1)) & (lax.axis_index("gy") % 4 == 0)


def paint_early_kernel(recv_ref, out_ref, val_ref):
    @pl.when(waits_long())
    def _():
        paint_sources(ROWS, 2, False, None, recv_ref, out_ref, val_ref, 0, EARLY)


def paint_late_kernel(recv_ref, after_ref, acc_ref, out_ref, val_ref):
    begin = jnp.where(waits_long(), EARLY, 0)
    paint_sources(ROWS, 2, False, None, recv_ref, out_ref, val_ref, begin)


def paint_more_kernel(handed, recv_ref, acc_ref, out_ref, val_ref):
    if handed:
        out_ref[...] = acc_ref[...]

        @pl.when((lax.axis_index("gx") == 0) | (lax.axis_index("gx") == GX - 1))
        def _():
            paint_sources(ROWS, 1, handed, acc_ref, recv_ref, out_ref, val_ref)
    else:
        paint_sources(ROWS, 1, handed, acc_ref, recv_ref, out_ref, val_ref)


def flagged(ref, row):
    flag = ref[0, row : row + 1, :]
    for i in range(1, GX):
        flag = jnp.maximum(flag, ref[i, row : row + 1, :])
    return jnp.max(jnp.where(lax.broadcasted_iota(I32, (1, 128), 1) >= 64, flag, 0.0)).astype(I32)


def paint_scratch(together):
    return [pltpu.VMEM((together, 16, 24, 128), F32)]


EARLY = 8
PAINTED = jax.ShapeDtypeStruct((GX, 2, XR, 128), F32)
PAINT_COST = pl.CostEstimate(flops=60000000, bytes_accessed=2000000, transcendentals=0)


def paint_early(recv):
    return pl.pallas_call(
        paint_early_kernel,
        out_shape=PAINTED,
        in_specs=[VM],
        out_specs=VM,
        scratch_shapes=paint_scratch(2),
        name="paint_early",
        compiler_params=ROOM,
        cost_estimate=PAINT_COST,
    )(recv)


def paint_late(recv, after, acc):
    return pl.pallas_call(
        paint_late_kernel,
        out_shape=PAINTED,
        in_specs=[VM, ANY, VM],
        out_specs=VM,
        scratch_shapes=paint_scratch(2),
        input_output_aliases={2: 0},
        name="paint_late",
        compiler_params=ROOM,
        cost_estimate=PAINT_COST,
    )(recv, after, acc)


def paint_more(recv, acc, handed=False):
    return pl.pallas_call(
        functools.partial(paint_more_kernel, handed),
        out_shape=PAINTED,
        in_specs=[VM, VM],
        out_specs=VM,
        scratch_shapes=paint_scratch(1),
        input_output_aliases={1: 0},
        name="paint_more",
        compiler_params=ROOM,
    )(recv, acc)


def paint_faces(count, cell_ref, off_ref, mass_ref, val_ref):
    slot = lax.broadcasted_iota(I32, (NROW, 128), 0) * 128 + lax.broadcasted_iota(I32, (NROW, 128), 1)
    m = jnp.where(slot < count, mass_ref[...], 0.0)
    dx, dy, dz = off_ref[0], off_ref[1], off_ref[2]
    xp, yp, zp = cells_of(cell_ref[...].astype(F32))
    up = (zp == 128.0) & (dz >= 0)
    down = (zp == 1.0) & (dz < 0)
    ax, ay = jnp.abs(dx), jnp.abs(dy)
    w = jnp.where(up | down, m * jnp.abs(dz), 0.0)
    coarse = jnp.floor(ax * 256.0) * (1.0 / 256.0)
    fine = ax - coarse
    y = yp + jnp.where(up, 24.0, 0.0)
    vals = [xp, xp + jnp.where(dx >= 0, 1.0, -1.0), 1.0 - coarse, coarse, -fine, fine]
    vals += [y, y + jnp.where(dy >= 0, 1.0, -1.0)]
    vals += [*halves(w * (1.0 - ay)), *halves(w * ay)]
    for n, v in enumerate(vals):
        val_ref[n] = v
    grid = counting(16)
    ghost = lax.broadcasted_iota(I32, (16, 128), 0)
    ghost_cell = jnp.where(ghost >= 4, 200, jnp.where((ghost & 1) == 0, 0, 129)).astype(F32).astype(BF)
    ghost_fine = (ghost >> 1).astype(F32).astype(BF) == 1.0

    def operands(r):
        def row(n):
            return jnp.broadcast_to(val_ref[n, r : r + 1, :].astype(BF), (16, 128))

        x0, x1, y0, y1 = row(0), row(1), row(6), row(7)
        weights = [row(n) for n in (2, 3, 4, 5, 8, 10, 9, 11)]
        xc, xf, high, low = [], [], [], []
        for g in range(8):
            cell = grid + float(16 * g + 1)
            first, second = cell == x0, cell == x1
            xc.append(spread(first, second, weights[0], weights[1]))
            xf.append(spread(first, second, weights[2], weights[3]))
        ends = jnp.where(ghost_cell == x1, jnp.where(ghost_fine, weights[3], weights[1]), jnp.zeros((), BF))
        for g in range(3):
            cell = grid + float(16 * g)
            first, second = cell == y0, cell == y1
            high.append(spread(first, second, weights[4], weights[5]))
            low.append(spread(first, second, weights[6], weights[7]))
        gap = [jnp.zeros((16, 128), BF)]
        return jnp.concatenate(xc + xf + [ends], axis=0), jnp.concatenate(high + gap + low + gap, axis=0)

    def step(b, total):
        for t in range(8):
            pairs = [operands(16 * b + 2 * t + u) for u in range(2)]
            x = jnp.concatenate([pair[0] for pair in pairs], axis=1)
            v = jnp.concatenate([pair[1] for pair in pairs], axis=1)
            total = total + lax.dot_general(x, v, (((1,), (1,)), ((), ())), preferred_element_type=F32)
        return total

    o = jnp.zeros((272, 128), F32)
    for b in range(NROW // 16):
        o = step(b, o)
    o = o + pltpu.roll(o, 64, 1)
    t = (o[0:128] + o[128:256]).T
    ends = o[256:264] + pltpu.roll(o[256:264], 6, 0)
    return t[0:24], t[24:48], ends[0:2]


def front_kernel(count_ref, cell_ref, off_ref, mass_ref, sorted_ref, pay_ref, val_ref):
    count = count_ref[0, 0, 0]
    low, high, ghosts = paint_faces(count, cell_ref, off_ref, mass_ref, val_ref)
    sort_and_pack(count, cell_ref, off_ref, mass_ref, low, high, ghosts, sorted_ref, pay_ref)


def front(count, cell, off, mass):
    return pl.pallas_call(
        front_kernel,
        out_shape=(jax.ShapeDtypeStruct((5, NROW, 128), F32), jax.ShapeDtypeStruct((GX, PAYROWS, 128), F32)),
        in_specs=[SM, VM, VM, VM],
        out_specs=(VM, VM),
        scratch_shapes=[pltpu.VMEM((12, NROW, 128), F32)],
        name="front",
        compiler_params=FULL,
        cost_estimate=pl.CostEstimate(flops=40000000, bytes_accessed=1000000, transcendentals=0),
    )(count, cell, off, mass)


def forward_kernel(recv_ref, table_ref, acc_ref, out_ref):
    last = lax.axis_index("gx") == GX - 1
    first = jnp.where(last, ROWS - FROWS, 0)
    row = jnp.where(last, 17.0, 0.0)
    for i in range(GX):
        cell, dx, dy, dz, m = (recv_ref[i, pl.ds(o * ROWS + first, FROWS), :] for o in range(5))
        _, yp, _ = cells_of(cell)
        ay = jnp.abs(dy)
        near = jnp.where(yp == row, 1.0 - ay, 0.0)
        weight = m * (near + jnp.where(yp + jnp.where(dy >= 0, 1.0, -1.0) == row, ay, 0.0))
        for o, v in enumerate((cell, dx, dz, weight)):
            out_ref[i, o * FROWS : (o + 1) * FROWS, :] = v
        for n, r in enumerate((2, 5, 6, 7)):
            out_ref[i, 4 * FROWS + n : 4 * FROWS + n + 1, :] = recv_ref[i, FACE + r : FACE + r + 1, :]


def forward_pack(recv, table, acc):
    return pl.pallas_call(
        forward_kernel,
        out_shape=jax.ShapeDtypeStruct((GX, HANDED, 128), F32),
        in_specs=[VM, ANY, ANY],
        out_specs=VM,
        name="forward_pack",
        compiler_params=ROOM,
        cost_estimate=pl.CostEstimate(flops=500000, bytes_accessed=600000, transcendentals=0),
    )(recv, table, acc)


def table_kernel(high_ref, low_ref):
    scale = 1.0 / 32.0
    j = lax.broadcasted_iota(I32, (64, 128), 1)
    k8 = 8 * lax.broadcasted_iota(I32, (64, 128), 0)
    none = jnp.zeros((64, 128), F32)

    def turns(m):
        angle = (((k8 + m) * j) & 1023).astype(F32) * (2.0 * math.pi / 1024.0)
        return jnp.cos(angle) * scale, jnp.sin(angle) * scale

    for g, (m, w) in enumerate(((1, 7), (3, 5), (2, 6), (0, 4))):
        (c, s), (e, t) = turns(m), turns(w)
        if g < 3:
            parts = ((c, s), (-s, c), (e, -t), (-t, -e))
        else:
            parts = ((c, none), (-s, none), (none, e), (none, -t))
        for n, pair in enumerate(parts):
            for h, value in enumerate(pair):
                high = value.astype(BF)
                high_ref[g, 64 * n : 64 * n + 64, 128 * h : 128 * h + 128] = high
                low_ref[g, 64 * n : 64 * n + 64, 128 * h : 128 * h + 128] = (value - high.astype(F32)).astype(BF)


def tables():
    shape = jax.ShapeDtypeStruct((4, 256, 256), BF)
    return pl.pallas_call(
        table_kernel,
        out_shape=(shape, shape),
        out_specs=(VM, VM),
        name="tables",
        compiler_params=ROOM,
        cost_estimate=pl.CostEstimate(flops=8000000, bytes_accessed=1000000, transcendentals=0),
    )()


GROUPS = ((1, 7), (3, 5), (2, 6), (0, 4))


def transform(field, th_ref, tl_ref, put):
    root = math.sqrt(0.5)

    def even(b):
        return field(b) + field(b + 4)

    def odd(b):
        return field(b) - field(b + 4)

    for g in range(4):
        if g < 2:
            d1, d3 = odd(1), odd(3)
            s, t = (d1 - d3) * root, (d1 + d3) * root
            pair = (odd(0) + s, -odd(2) - t) if g == 0 else (odd(0) - s, odd(2) - t)
        elif g == 2:
            pair = (even(0) - even(2), even(3) - even(1))
        else:
            s, t = even(0) + even(2), even(1) + even(3)
            pair = (s + t, s - t)
        value = jnp.concatenate(pair, axis=0)
        high = value.astype(BF)
        low = (value - high.astype(F32)).astype(BF)
        o = jnp.dot(th_ref[g], high, preferred_element_type=F32)
        o = o + jnp.dot(tl_ref[g], high, preferred_element_type=F32)
        put(g, o + jnp.dot(th_ref[g], low, preferred_element_type=F32))


def face_columns(i, rows, ghosts):
    before, after = (i - 1) % GX, (i + 1) % GX
    lane = lax.broadcasted_iota(I32, (1, 128), 1)
    out = []
    for side in range(2):
        v = rows[i][side] + jnp.where(lane == 127, ghosts[after][side][0:1], 0.0)
        out.append(v + jnp.where(lane == 0, ghosts[before][side][1:2], 0.0))
    return out


def pick(v, lane):
    return jnp.sum(jnp.where(lax.broadcasted_iota(I32, (2, 128), 1) == lane, v, 0.0), axis=1, keepdims=True)


def along_z_kernel(face_ref, in_ref, after_ref, down_ref, up_ref):
    p = lax.axis_index("gx")
    for j in range(2):
        on = p == (0 if j == 0 else GX - 1)
        rows, ghosts = [], []
        for i in range(GX):
            own, handed = face_ref[i, FACE : FACE + 8, :], in_ref[i, 4 * FROWS : HANDED, :]
            rows.append([own[3 * n + j : 3 * n + j + 1] + jnp.where(on, handed[n : n + 1], 0.0) for n in range(2)])
            past = [pick(own[6:8], base + 2 * p + 1 + j) for base in (0, 24)]
            more = [pick(handed[2:4], base + (17 if j == 0 else 0)) for base in (0, 24)]
            ghosts.append([a + jnp.where(on, b, 0.0) for a, b in zip(past, more)])
        for i in range(GX):
            down, up = face_columns(i, rows, ghosts)
            down_ref[2 * i + j : 2 * i + j + 1] = down
            up_ref[2 * i + j : 2 * i + j + 1] = up


def along_z(recv, passed, after):
    shape = jax.ShapeDtypeStruct((2 * GX, 128), F32)
    return pl.pallas_call(
        along_z_kernel,
        out_shape=(shape, shape),
        in_specs=[VM, VM, ANY],
        out_specs=(VM, VM),
        name="along_z",
        compiler_params=ROOM,
        cost_estimate=pl.CostEstimate(flops=500000, bytes_accessed=100000, transcendentals=0),
    )(recv, passed, after)


def handed_kernel(in_ref, face_ref, acc_ref, out_ref, flag_ref, val_ref):
    p = lax.axis_index("gx")
    flag_ref[0] = flagged(face_ref, FACE + 6)

    @pl.when((p == 0) | (p == GX - 1))
    def _():
        flag_ref[0] = jnp.maximum(flag_ref[0], flagged(in_ref, 4 * FROWS + 2))
        paint_sources(FROWS, 4, True, acc_ref, in_ref, out_ref, val_ref)


def paint_handed(passed, recv, acc):
    return pl.pallas_call(
        handed_kernel,
        out_shape=(PAINTED, pltpu.SMEM((1,), I32)),
        in_specs=[VM, VM, VM],
        out_specs=(VM, SM),
        scratch_shapes=paint_scratch(4),
        input_output_aliases={2: 0},
        name="paint_handed",
        compiler_params=ROOM,
        cost_estimate=PAINT_COST,
    )(passed, recv, acc)


def finish_kernel(acc_ref, below_ref, above_ref, th_ref, tl_ref, dens_ref, spec_ref, x_ref):
    wide = lax.broadcasted_iota(I32, (128, 128), 1)
    for i in range(GX):
        before, after = (i - 1) % GX, (i + 1) % GX
        gap = jnp.zeros((124, 128), F32)
        t = jnp.concatenate([below_ref[2 * i : 2 * i + 2], gap, above_ref[2 * i : 2 * i + 2]], axis=0).T
        for j in range(2):
            shifted = pltpu.roll(t, 1 if j == 0 else 127, 1)
            low, high = (t, shifted) if j == 0 else (shifted, t)
            v = acc_ref[i, j, 0:128, :] + jnp.where(wide == 0, low, jnp.where(wide == 127, high, 0.0))
            cols = slice(j * 128, (j + 1) * 128)
            x_ref[i, :, cols] = v
            x_ref[i, 127:128, cols] = v[127:128] + acc_ref[after, j, 128:129, :]
            x_ref[i, 0:1, cols] = v[0:1] + acc_ref[before, j, 129:130, :]
            dens_ref[pl.ds(i * 256 + j, 128, stride=2), :] = x_ref[i, :, cols]

    def put(g, o):
        m, w = GROUPS[g]
        for n, (k, part) in enumerate(((m, 0), (m, 1), (w, 0), (w, 1))):
            for j in range(2):
                spec_ref[pl.ds(part * 1024 + 2 * k + j, 64, stride=16), :] = o[64 * n : 64 * n + 64, j * 128 : (j + 1) * 128]

    transform(lambda b: x_ref[b], th_ref, tl_ref, put)


def finish(acc, below, above, th, tl):
    shape = jax.ShapeDtypeStruct((2048, 128), F32)
    return pl.pallas_call(
        finish_kernel,
        out_shape=(shape, shape),
        in_specs=[VM] * 5,
        out_specs=(VM, VM),
        scratch_shapes=[pltpu.VMEM((GX, 128, 256), F32)],
        name="finish",
        compiler_params=ROOM,
        cost_estimate=pl.CostEstimate(flops=400000000, bytes_accessed=4000000, transcendentals=0),
    )(acc, below, above, th, tl)


def y_pairs(blocks):
    pairs = []
    for q in range(blocks):
        pairs.append(((GX - 1) * blocks + q, (q + 1) % blocks))
        pairs.append((q, (GX - 1) * blocks + (q - 1) % blocks))
    return pairs


def exchange(x):
    return lax.all_to_all(x, "gx", split_axis=0, concat_axis=0, tiled=False)


def hand_on(x):
    return lax.ppermute(x, ("gx", "gy"), y_pairs(lax.axis_size("gy")))


def weighted(block):
    cell, dx, dy, dz, m = (block[:, o * ROWS : (o + 1) * ROWS] for o in range(5))
    row = jnp.where(lax.axis_index("gx") == GX - 1, 17.0, 0.0)
    _, yp, _ = cells_of(cell)
    ay = jnp.abs(dy)
    far = yp + jnp.where(dy >= 0, 1.0, -1.0)
    weight = m * (jnp.where(yp == row, 1.0 - ay, 0.0) + jnp.where(far == row, ay, 0.0))
    return jnp.concatenate([cell, dx, dz, weight, jnp.zeros((GX, PAYROWS - 4 * ROWS, 128), F32)], axis=1)


def later_window(ordered, turn):
    xp, yp, zp = cells_of(ordered[0])
    live = ordered[4] != 0.0
    key = jnp.where(live, jnp.where(ordered[2] >= 0, yp, yp - 1.0), 20.0)
    space = jnp.zeros((5, NROW + 3 * ROWS, 128), F32)
    padded = jnp.concatenate([space, ordered, space], axis=1)
    base = NROW + 3 * ROWS
    blocks = []
    for p in range(GX):
        if p < GX - 1:
            begin = jnp.sum(jnp.where(key < 2 * p, 1, 0))
            w = jnp.minimum(begin // 128, NROW - ROWS) + turn * ROWS
        else:
            w = jnp.clip((jnp.sum(jnp.where(live, 1, 0)) + 127) // 128 - ROWS, 0, NROW - ROWS) - turn * ROWS
        part = lax.dynamic_slice_in_dim(padded, base + w, ROWS, axis=1).reshape(5 * ROWS, 128)
        blocks.append(jnp.concatenate([part, jnp.zeros((PAYROWS - 5 * ROWS, 128), F32)], axis=0))
    return jnp.stack(blocks)


def body(cell_index, offsets, mass, counts):
    p = lax.axis_index("gx")
    blocks = lax.axis_size("gz")
    ordered, pay = front(counts, cell_index.reshape(NROW, 128), offsets.reshape(3, NROW, 128), mass.reshape(NROW, 128))
    recv = exchange(pay)
    th, tl = tables()

    acc = paint_early(recv)
    packed = forward_pack(recv, th, acc)
    passed = hand_on(packed)
    acc = paint_late(recv, packed, acc)
    down, up = along_z(recv, passed, acc)
    below = lax.ppermute(up, "gz", [(i, (i + 1) % blocks) for i in range(blocks)])
    above = lax.ppermute(down, "gz", [((i + 1) % blocks, i) for i in range(blocks)])
    acc, over = paint_handed(passed, recv, acc)
    density, spectrum = finish(acc, below, above, th, tl)

    def slow(outputs):
        mine = jnp.max(recv[:, FACE + 6, 64:]) > 0
        later = lax.cond(
            mine,
            lambda: tuple(exchange(later_window(ordered, t)) for t in (1, 2, 3)),
            lambda: (jnp.zeros(recv.shape, F32),) * 3,
        )
        first = jnp.where(p == GX - 1, ROWS - FROWS, 0)
        row = lax.broadcasted_iota(I32, (PAYROWS, 128), 0) - 4 * ROWS
        sent = (row >= first) & (row < first + FROWS)
        rest = jnp.where(sent, 0.0, recv)
        acc = jnp.zeros(PAINTED.shape, F32)
        for x in (recv, *later):
            acc = paint_more(x, acc)
        for x in (rest, *later):
            acc = paint_more(hand_on(weighted(x)), acc, handed=True)
        acc, _ = paint_handed(passed, recv, acc)
        return finish(acc, below, above, th, tl)

    density, spectrum = lax.cond(over[0] > 0, slow, lambda outputs: outputs, (density, spectrum))
    return density.reshape(1024, 1, 2, 128), spectrum.reshape(2, 512, 1, 2, 128)


def solution(mesh):
    placed = (
        P("gx", "gy", "gz", None),
        P("gx", "gy", "gz", None, None),
        P("gx", "gy", "gz", None),
        P("gx", "gy", "gz"),
    )
    return jax.shard_map(
        body,
        mesh=mesh,
        in_specs=placed,
        out_specs=(P(None, "gx", "gy", "gz"), P(None, None, "gx", "gy", "gz")),
        check_vma=False,
    )
```

```python
import functools
import math

import jax
import jax.numpy as jnp
from jax import lax
from jax.experimental import pallas as pl
from jax.experimental.pallas import tpu as pltpu
from jax.sharding import PartitionSpec as P


F32, I32, BF = jnp.float32, jnp.int32, jnp.bfloat16
GX = 8
RING = 4
ROWS = 17
FROWS = 7
NROW = 64
HANDED = 4 * FROWS + 4
PAYROWS = 96
FACE = 5 * ROWS
XR = 136
LANE = {6: 64, 7: 1, 8: 2, 9: 4, 10: 8, 11: 16, 12: 32}
SUB = {3: 1, 4: 2, 5: 4}
CELL = (1 << 19) - 1
FULL = pltpu.CompilerParams(vmem_limit_bytes=60 * 1024 * 1024)
ROOM = pltpu.CompilerParams(vmem_limit_bytes=12 * 1024 * 1024)
VM = pl.BlockSpec(memory_space=pltpu.VMEM)
SM = pl.BlockSpec(memory_space=pltpu.SMEM)
ANY = pl.BlockSpec(memory_space=pl.ANY)


def cells_of(flat):
    row = jnp.floor((flat + 0.5) * (1.0 / 130.0))
    xp = jnp.floor((row + 0.5) * (1.0 / 18.0))
    return xp, row - 18.0 * xp, flat - 130.0 * row


def halves(value):
    high = value.astype(BF).astype(F32)
    return high, value - high


def index_bit(bit, lane, sub, reg):
    if bit < 3:
        return bool((reg >> bit) & 1)
    if bit in SUB:
        return (sub & SUB[bit]) != 0
    return (lane & LANE[bit]) != 0


def sort_network(ops, lane, sub):
    for size in range(1, 14):
        for bit in range(size - 1, -1, -1):
            new = [[None] * 8 for _ in ops]
            if bit < 3:
                for v in range(8):
                    w = v | (1 << bit)
                    if v == w:
                        continue
                    down = False if size == 13 else index_bit(size, lane, sub, v)
                    a, c = ops[0][v], ops[0][w]
                    if down is True:
                        move = a < c
                    elif down is False:
                        move = a > c
                    else:
                        move = jnp.where(down, c, a) > jnp.where(down, a, c)
                    for o in range(len(ops)):
                        a, c = ops[o][v], ops[o][w]
                        new[o][v] = jnp.where(move, c, a)
                        new[o][w] = jnp.where(move, a, c)
            else:
                axis, step, index = (0, SUB[bit], sub) if bit in SUB else (1, LANE[bit], lane)
                upper = (index & step) != 0
                other = index ^ step

                def partner(x):
                    if 2 * step == x.shape[axis]:
                        return pltpu.roll(x, step, axis)
                    return jnp.take_along_axis(x, other, axis=axis)

                for v in range(8):
                    down = False if size == 13 else index_bit(size, lane, sub, v)
                    mine, theirs = ops[0][v], partner(ops[0][v])
                    if down is True:
                        big = ~upper
                    elif down is False:
                        big = upper
                    else:
                        big = upper ^ down
                    move = jnp.where(big, theirs, mine) > jnp.where(big, mine, theirs)
                    new[0][v] = jnp.where(move, theirs, mine)
                    for o in range(1, len(ops)):
                        new[o][v] = jnp.where(move, partner(ops[o][v]), ops[o][v])
            ops = new
    return ops


def sort_and_pack(count, cell_ref, off_ref, mass_ref, low, high, ghosts, sorted_ref, pay_ref, hand_ref):
    lane = lax.broadcasted_iota(I32, (8, 128), 1)
    sub = lax.broadcasted_iota(I32, (8, 128), 0)
    below = [jnp.zeros((8, 128), F32) for _ in range(18)]
    ops = [[] for _ in range(5)]
    for v in range(8):
        s = slice(8 * v, 8 * v + 8)
        cell, dy = cell_ref[s, :], off_ref[1, s, :]
        live = v * 1024 + sub * 128 + lane < count
        _, yp, _ = cells_of(cell.astype(F32))
        row = jnp.where(live, jnp.where(dy >= 0, yp, yp - 1.0), 20.0)
        for t in range(1, 18):
            below[t] = below[t] + jnp.where(row < t, 1.0, 0.0)
        ops[0].append((row.astype(I32) << 19) | cell)
        for o in range(3):
            ops[o + 1].append(off_ref[o, s, :])
        ops[4].append(jnp.where(live, mass_ref[s, :], 0.0))
    below = [None] + [jnp.sum(b).astype(I32) for b in below[1:]]
    ops = sort_network(ops, lane, sub)
    ops[0] = [(k & CELL).astype(F32) for k in ops[0]]
    for o in range(5):
        t = jnp.concatenate(ops[o], axis=0).T
        sorted_ref[o] = jnp.concatenate([t[:64], t[64:]], axis=1)
    over = below[1] > FROWS * 128
    starts = []
    for p in range(GX):
        if p < GX - 1:
            begin = below[2 * p] if p else jnp.int32(0)
            w = jnp.minimum(begin >> 7, NROW - ROWS)
            over = over | (below[2 * p + 3] > 128 * (w + ROWS))
        else:
            w = jnp.clip(((below[17] + 127) >> 7) - ROWS, 0, NROW - ROWS)
            over = over | (below[2 * p] < 128 * w) | (below[2 * p + 2] < 128 * (w + ROWS - FROWS))
        starts.append(w)
    ghosts = jnp.where(lax.broadcasted_iota(I32, (2, 128), 1) < 64, ghosts, jnp.where(over, 1.0, 0.0))
    for p in range(GX):
        for o in range(5):
            pay_ref[p, o * ROWS : (o + 1) * ROWS, :] = sorted_ref[o, pl.ds(starts[p], ROWS), :]
        past = 17 if p == GX - 1 else 0
        rows = []
        for v in (low, high):
            rows += [v[2 * p + 1 : 2 * p + 3], v[past : past + 1]]
        pay_ref[p, FACE : FACE + 8, :] = jnp.concatenate(rows + [ghosts], axis=0)
        pay_ref[p, FACE + 8 : PAYROWS, :] = jnp.zeros((PAYROWS - FACE - 8, 128), F32)
    last = lax.axis_index("gy") % RING == RING - 1
    first = jnp.where(last, starts[GX - 1] + ROWS - FROWS, 0)
    row = jnp.where(last, 17.0, 0.0)
    parts = [sorted_ref[o, pl.ds(first, FROWS), :] for o in range(5)]
    for o, v in enumerate(one_row(*parts, row)):
        hand_ref[o * FROWS : (o + 1) * FROWS, :] = v
    ends = [jnp.where(last, v[17:18], v[0:1]) for v in (low, high)]
    hand_ref[4 * FROWS : HANDED, :] = jnp.concatenate(ends + [ghosts], axis=0)


def one_row(cell, dx, dy, dz, m, row):
    _, yp, _ = cells_of(cell)
    ay = jnp.abs(dy)
    far = yp + jnp.where(dy >= 0, 1.0, -1.0)
    return cell, dx, dz, m * (jnp.where(yp == row, 1.0 - ay, 0.0) + jnp.where(far == row, ay, 0.0))


def spread(first, second, one, two):
    return jnp.where(first, one, jnp.where(second, two, jnp.zeros((), BF)))


def counting(height, start=0):
    return (lax.broadcasted_iota(I32, (height, 128), 0) + start).astype(F32).astype(BF)


def paint_sources(rows, together, handed, acc_ref, recv_ref, out_ref, val_ref, begin=0, end=GX):
    p = lax.axis_index("gx")
    count = 1 if handed else 2
    grid = counting(16)
    ghost = lax.broadcasted_iota(I32, (16, 128), 0)
    ghost_cell = jnp.where(ghost >= 4 * count, 200, jnp.where((ghost & 1) == 0, 0, 129)).astype(F32).astype(BF)
    ghost_row = (ghost >> 1).astype(F32).astype(BF)

    def prepare(i, slot):
        def op(k):
            return recv_ref[i, k * rows : (k + 1) * rows, :]

        xp, yp, zp = cells_of(op(0))
        if handed:
            dx, dz, weights = op(1), op(2), [op(3)]
        else:
            dx, dy, dz, m = op(1), op(2), op(3), op(4)
            y = yp - (2 * p + 1).astype(F32)
            y1 = y + jnp.where(dy >= 0, 1.0, -1.0)
            ay = jnp.abs(dy)
            weights = [m * (jnp.where(y == j, 1.0 - ay, 0.0) + jnp.where(y1 == j, ay, 0.0)) for j in range(2)]
        ax, az = jnp.abs(dx), jnp.abs(dz)
        coarse = jnp.floor(az * 256.0) * (1.0 / 256.0)
        fine = az - coarse
        vals = [xp, xp + jnp.where(dx >= 0, 1.0, -1.0), zp - 1.0, zp - 1.0 + jnp.where(dz >= 0, 1.0, -1.0)]
        vals += [1.0 - coarse, coarse, -fine, fine]
        for mj in weights:
            for w in (1.0 - ax, ax):
                vals += list(halves(mj * w))
        for n, v in enumerate(vals):
            val_ref[slot, n, 0:rows] = v

    def operands(slot, r):
        def row(n):
            return jnp.broadcast_to(val_ref[slot, n, r : r + 1, :].astype(BF), (16, 128))

        x0, x1, z0, z1 = (row(n) for n in range(4))
        near = [row(8 + 4 * (c // 2) + c % 2) for c in range(2 * count)]
        far = [row(10 + 4 * (c // 2) + c % 2) for c in range(2 * count)]
        a = [[] for _ in range(2 * count)]
        for g in range(8):
            cell = grid + float(16 * g + 1)
            first, second = cell == x0, cell == x1
            for c in range(2 * count):
                a[c].append(spread(first, second, near[c], far[c]))
        w = far[-1]
        for c in range(2 * count - 1):
            w = jnp.where(ghost_row == float(c), far[c], w)
        a = sum(a, []) + [jnp.where(ghost_cell == x1, w, jnp.zeros((), BF))]
        zc, zf = [], []
        weights = [row(n) for n in range(4, 8)]
        for g in range(8):
            cell = grid + float(16 * g)
            first, second = cell == z0, cell == z1
            zc.append(spread(first, second, weights[0], weights[1]))
            zf.append(spread(first, second, weights[2], weights[3]))
        return jnp.concatenate(a, axis=0), jnp.concatenate(zc + zf, axis=0)

    def source(i, slot):
        prepare(i, slot)
        o = None
        for t in range((rows + 1) // 2):
            pairs = [operands(slot, r) for r in range(2 * t, min(2 * t + 2, rows))]
            a = jnp.concatenate([pair[0] for pair in pairs], axis=1)
            z = jnp.concatenate([pair[1] for pair in pairs], axis=1)
            d = lax.dot_general(a, z, (((1,), (1,)), ((), ())), preferred_element_type=F32)
            o = d if o is None else o + d
        ends = o[256 * count : 256 * count + 8, :128] + o[256 * count : 256 * count + 8, 128:]
        ends = ends + pltpu.roll(ends, 6, 0)
        for j in range(count):
            at = jnp.where(p == 0, 0, 1) if handed else j
            high, low = o[256 * j : 256 * j + 128], o[256 * j + 128 : 256 * j + 256]
            total = high[:, :128] + high[:, 128:] + low[:, :128]
            end = ends if j == 0 else pltpu.roll(ends, 4, 0)
            if acc_ref is not None:
                total = total + acc_ref[i, at, 0:128]
                end = end + acc_ref[i, at, 128:136]
            out_ref[i, at, 0:128] = total
            out_ref[i, at, 128:136] = end

    def step(b, carry):
        for u in range(together):
            source(b * together + u, u)
        return carry

    lax.fori_loop(begin // together, end // together, step, 0)


SOME = 0


def painted_early():
    p, q = lax.axis_index("gx"), lax.axis_index("gy") % RING
    every = ((q == 0) & (p == 0)) | ((q == RING - 1) & (p == GX - 1))
    return jnp.where(every, GX, jnp.where((q == 0) & (p == GX - 1), SOME, 0))


def paint_early_kernel(recv_ref, out_ref, val_ref):
    paint_sources(ROWS, 2, False, None, recv_ref, out_ref, val_ref, 0, painted_early())


def paint_late_kernel(recv_ref, after_ref, acc_ref, out_ref, val_ref):
    paint_sources(ROWS, 2, False, None, recv_ref, out_ref, val_ref, painted_early())


def paint_more_kernel(handed, recv_ref, acc_ref, out_ref, val_ref):
    if handed:
        out_ref[...] = acc_ref[...]

        @pl.when((lax.axis_index("gx") == 0) | (lax.axis_index("gx") == GX - 1))
        def _():
            paint_sources(ROWS, 1, handed, acc_ref, recv_ref, out_ref, val_ref)
    else:
        paint_sources(ROWS, 1, handed, acc_ref, recv_ref, out_ref, val_ref)


def flagged(ref, row):
    flag = ref[0, row : row + 1, :]
    for i in range(1, GX):
        flag = jnp.maximum(flag, ref[i, row : row + 1, :])
    return jnp.max(jnp.where(lax.broadcasted_iota(I32, (1, 128), 1) >= 64, flag, 0.0)).astype(I32)


def paint_scratch(together):
    return [pltpu.VMEM((together, 16, 24, 128), F32)]


PAINTED = jax.ShapeDtypeStruct((GX, 2, XR, 128), F32)
PAINT_COST = pl.CostEstimate(flops=60000000, bytes_accessed=2000000, transcendentals=0)


def paint_early(recv):
    return pl.pallas_call(
        paint_early_kernel,
        out_shape=PAINTED,
        in_specs=[VM],
        out_specs=VM,
        scratch_shapes=paint_scratch(2),
        name="paint_early",
        compiler_params=ROOM,
        cost_estimate=PAINT_COST,
    )(recv)


def paint_late(recv, after, acc):
    return pl.pallas_call(
        paint_late_kernel,
        out_shape=PAINTED,
        in_specs=[VM, ANY, VM],
        out_specs=VM,
        scratch_shapes=paint_scratch(2),
        input_output_aliases={2: 0},
        name="paint_late",
        compiler_params=ROOM,
        cost_estimate=PAINT_COST,
    )(recv, after, acc)


def paint_more(recv, acc, handed=False):
    return pl.pallas_call(
        functools.partial(paint_more_kernel, handed),
        out_shape=PAINTED,
        in_specs=[VM, VM],
        out_specs=VM,
        scratch_shapes=paint_scratch(1),
        input_output_aliases={1: 0},
        name="paint_more",
        compiler_params=ROOM,
    )(recv, acc)


def paint_faces(count, cell_ref, off_ref, mass_ref, val_ref):
    slot = lax.broadcasted_iota(I32, (NROW, 128), 0) * 128 + lax.broadcasted_iota(I32, (NROW, 128), 1)
    m = jnp.where(slot < count, mass_ref[...], 0.0)
    dx, dy, dz = off_ref[0], off_ref[1], off_ref[2]
    xp, yp, zp = cells_of(cell_ref[...].astype(F32))
    up = (zp == 128.0) & (dz >= 0)
    down = (zp == 1.0) & (dz < 0)
    ax, ay = jnp.abs(dx), jnp.abs(dy)
    w = jnp.where(up | down, m * jnp.abs(dz), 0.0)
    coarse = jnp.floor(ax * 256.0) * (1.0 / 256.0)
    fine = ax - coarse
    y = yp + jnp.where(up, 24.0, 0.0)
    vals = [xp, xp + jnp.where(dx >= 0, 1.0, -1.0), 1.0 - coarse, coarse, -fine, fine]
    vals += [y, y + jnp.where(dy >= 0, 1.0, -1.0)]
    vals += [*halves(w * (1.0 - ay)), *halves(w * ay)]
    for n, v in enumerate(vals):
        val_ref[n] = v
    grid = counting(16)
    ghost = lax.broadcasted_iota(I32, (16, 128), 0)
    ghost_cell = jnp.where(ghost >= 4, 200, jnp.where((ghost & 1) == 0, 0, 129)).astype(F32).astype(BF)
    ghost_fine = (ghost >> 1).astype(F32).astype(BF) == 1.0

    def operands(r):
        def row(n):
            return jnp.broadcast_to(val_ref[n, r : r + 1, :].astype(BF), (16, 128))

        x0, x1, y0, y1 = row(0), row(1), row(6), row(7)
        weights = [row(n) for n in (2, 3, 4, 5, 8, 10, 9, 11)]
        xc, xf, high, low = [], [], [], []
        for g in range(8):
            cell = grid + float(16 * g + 1)
            first, second = cell == x0, cell == x1
            xc.append(spread(first, second, weights[0], weights[1]))
            xf.append(spread(first, second, weights[2], weights[3]))
        ends = jnp.where(ghost_cell == x1, jnp.where(ghost_fine, weights[3], weights[1]), jnp.zeros((), BF))
        for g in range(3):
            cell = grid + float(16 * g)
            first, second = cell == y0, cell == y1
            high.append(spread(first, second, weights[4], weights[5]))
            low.append(spread(first, second, weights[6], weights[7]))
        gap = [jnp.zeros((16, 128), BF)]
        return jnp.concatenate(xc + xf + [ends], axis=0), jnp.concatenate(high + gap + low + gap, axis=0)

    def step(b, total):
        for t in range(8):
            pairs = [operands(16 * b + 2 * t + u) for u in range(2)]
            x = jnp.concatenate([pair[0] for pair in pairs], axis=1)
            v = jnp.concatenate([pair[1] for pair in pairs], axis=1)
            total = total + lax.dot_general(x, v, (((1,), (1,)), ((), ())), preferred_element_type=F32)
        return total

    o = jnp.zeros((272, 128), F32)
    for b in range(NROW // 16):
        o = step(b, o)
    o = o + pltpu.roll(o, 64, 1)
    t = (o[0:128] + o[128:256]).T
    ends = o[256:264] + pltpu.roll(o[256:264], 6, 0)
    return t[0:24], t[24:48], ends[0:2]


def front_kernel(count_ref, cell_ref, off_ref, mass_ref, sorted_ref, pay_ref, hand_ref, val_ref):
    count = count_ref[0, 0, 0]
    low, high, ghosts = paint_faces(count, cell_ref, off_ref, mass_ref, val_ref)
    sort_and_pack(count, cell_ref, off_ref, mass_ref, low, high, ghosts, sorted_ref, pay_ref, hand_ref)


def front(count, cell, off, mass):
    return pl.pallas_call(
        front_kernel,
        out_shape=(
            jax.ShapeDtypeStruct((5, NROW, 128), F32),
            jax.ShapeDtypeStruct((GX, PAYROWS, 128), F32),
            pltpu.VMEM((HANDED, 128), F32),
        ),
        in_specs=[SM, VM, VM, VM],
        out_specs=(VM, VM, VM),
        scratch_shapes=[pltpu.VMEM((12, NROW, 128), F32)],
        name="front",
        compiler_params=FULL,
        cost_estimate=pl.CostEstimate(flops=40000000, bytes_accessed=1000000, transcendentals=0),
    )(count, cell, off, mass)


def forward_kernel(recv_ref, acc_ref, out_ref):
    last = lax.axis_index("gx") == GX - 1
    first = jnp.where(last, ROWS - FROWS, 0)
    row = jnp.where(last, 17.0, 0.0)
    for i in range(GX):
        parts = [recv_ref[i, pl.ds(o * ROWS + first, FROWS), :] for o in range(5)]
        for o, v in enumerate(one_row(*parts, row)):
            out_ref[i, o * FROWS : (o + 1) * FROWS, :] = v
        for n, r in enumerate((2, 5, 6, 7)):
            out_ref[i, 4 * FROWS + n : 4 * FROWS + n + 1, :] = recv_ref[i, FACE + r : FACE + r + 1, :]


def forward_pack(recv, acc):
    return pl.pallas_call(
        forward_kernel,
        out_shape=jax.ShapeDtypeStruct((GX, HANDED, 128), F32),
        in_specs=[VM, ANY],
        out_specs=VM,
        name="forward_pack",
        compiler_params=ROOM,
        cost_estimate=pl.CostEstimate(flops=500000, bytes_accessed=600000, transcendentals=0),
    )(recv, acc)


def join_kernel(one_ref, two_ref, out_ref):
    out_ref[0] = one_ref[...]
    out_ref[1] = two_ref[...]


def join(one, two):
    return pl.pallas_call(
        join_kernel,
        out_shape=jax.ShapeDtypeStruct((2, HANDED, 128), F32),
        in_specs=[VM, VM],
        out_specs=VM,
        name="join",
        compiler_params=ROOM,
    )(one, two)


def either_kernel(one_ref, two_ref, out_ref):
    out_ref[...] = one_ref[...] + two_ref[...]


def either(one, two):
    return pl.pallas_call(
        either_kernel,
        out_shape=jax.ShapeDtypeStruct((2, HANDED, 128), F32),
        in_specs=[VM, VM],
        out_specs=VM,
        name="either",
        compiler_params=ROOM,
    )(one, two)


def table_kernel(high_ref, low_ref):
    scale = 1.0 / 32.0
    j = lax.broadcasted_iota(I32, (64, 128), 1)
    k8 = 8 * lax.broadcasted_iota(I32, (64, 128), 0)
    none = jnp.zeros((64, 128), F32)

    def turns(m):
        angle = (((k8 + m) * j) & 1023).astype(F32) * (2.0 * math.pi / 1024.0)
        return jnp.cos(angle) * scale, jnp.sin(angle) * scale

    for g, (m, w) in enumerate(((1, 7), (3, 5), (2, 6), (0, 4))):
        (c, s), (e, t) = turns(m), turns(w)
        if g < 3:
            parts = ((c, s), (-s, c), (e, -t), (-t, -e))
        else:
            parts = ((c, none), (-s, none), (none, e), (none, -t))
        for n, pair in enumerate(parts):
            for h, value in enumerate(pair):
                high = value.astype(BF)
                high_ref[g, 64 * n : 64 * n + 64, 128 * h : 128 * h + 128] = high
                low_ref[g, 64 * n : 64 * n + 64, 128 * h : 128 * h + 128] = (value - high.astype(F32)).astype(BF)


def tables():
    shape = jax.ShapeDtypeStruct((4, 256, 256), BF)
    return pl.pallas_call(
        table_kernel,
        out_shape=(shape, shape),
        out_specs=(VM, VM),
        name="tables",
        compiler_params=ROOM,
        cost_estimate=pl.CostEstimate(flops=8000000, bytes_accessed=1000000, transcendentals=0),
    )()


GROUPS = ((1, 7), (3, 5), (2, 6), (0, 4))


def transform(field, th_ref, tl_ref, put):
    root = math.sqrt(0.5)

    def even(b):
        return field(b) + field(b + 4)

    def odd(b):
        return field(b) - field(b + 4)

    for g in range(4):
        if g < 2:
            d1, d3 = odd(1), odd(3)
            s, t = (d1 - d3) * root, (d1 + d3) * root
            pair = (odd(0) + s, -odd(2) - t) if g == 0 else (odd(0) - s, odd(2) - t)
        elif g == 2:
            pair = (even(0) - even(2), even(3) - even(1))
        else:
            s, t = even(0) + even(2), even(1) + even(3)
            pair = (s + t, s - t)
        value = jnp.concatenate(pair, axis=0)
        high = value.astype(BF)
        low = (value - high.astype(F32)).astype(BF)
        o = jnp.dot(th_ref[g], high, preferred_element_type=F32)
        o = o + jnp.dot(tl_ref[g], high, preferred_element_type=F32)
        put(g, o + jnp.dot(th_ref[g], low, preferred_element_type=F32))


def face_columns(i, rows, ghosts):
    before, after = (i - 1) % GX, (i + 1) % GX
    lane = lax.broadcasted_iota(I32, (1, 128), 1)
    out = []
    for side in range(2):
        v = rows[i][side] + jnp.where(lane == 127, ghosts[after][side][0:1], 0.0)
        out.append(v + jnp.where(lane == 0, ghosts[before][side][1:2], 0.0))
    return out


def pick(v, lane):
    return jnp.sum(jnp.where(lax.broadcasted_iota(I32, (2, 128), 1) == lane, v, 0.0), axis=1, keepdims=True)


def along_z_kernel(face_ref, in_ref, *refs):
    gathered, (after_ref, down_ref, up_ref, all_ref) = refs[: GX // 2], refs[GX // 2 :]
    p, q = lax.axis_index("gx"), lax.axis_index("gy") % RING
    across = ((p == 0) & (q == 0)) | ((p == GX - 1) & (q == RING - 1))
    for i in range(GX):
        n = GX - 1 - i
        mine = jnp.where(p == 0, gathered[i // 2][i % 2], gathered[n // 2][n % 2])
        all_ref[i] = jnp.where(across, mine, in_ref[i])
    for j in range(2):
        on = p == (0 if j == 0 else GX - 1)
        rows, ghosts = [], []
        for i in range(GX):
            own, handed = face_ref[i, FACE : FACE + 8, :], all_ref[i, 4 * FROWS : HANDED, :]
            rows.append([own[3 * n + j : 3 * n + j + 1] + jnp.where(on, handed[n : n + 1], 0.0) for n in range(2)])
            past = [pick(own[6:8], base + 2 * p + 1 + j) for base in (0, 24)]
            more = [pick(handed[2:4], base + (17 if j == 0 else 0)) for base in (0, 24)]
            ghosts.append([a + jnp.where(on, b, 0.0) for a, b in zip(past, more)])
        for i in range(GX):
            down, up = face_columns(i, rows, ghosts)
            down_ref[2 * i + j : 2 * i + j + 1] = down
            up_ref[2 * i + j : 2 * i + j + 1] = up


def along_z(recv, passed, gathered, after):
    shape = jax.ShapeDtypeStruct((2 * GX, 128), F32)
    return pl.pallas_call(
        along_z_kernel,
        out_shape=(shape, shape, jax.ShapeDtypeStruct((GX, HANDED, 128), F32)),
        in_specs=[VM] * (2 + GX // 2) + [ANY],
        out_specs=(VM, VM, VM),
        name="along_z",
        compiler_params=ROOM,
        cost_estimate=pl.CostEstimate(flops=500000, bytes_accessed=100000, transcendentals=0),
    )(recv, passed, *gathered, after)


def handed_kernel(in_ref, face_ref, acc_ref, out_ref, flag_ref, val_ref):
    p = lax.axis_index("gx")
    flag_ref[0] = flagged(face_ref, FACE + 6)

    @pl.when((p == 0) | (p == GX - 1))
    def _():
        flag_ref[0] = jnp.maximum(flag_ref[0], flagged(in_ref, 4 * FROWS + 2))
        paint_sources(FROWS, 4, True, acc_ref, in_ref, out_ref, val_ref)


def paint_handed(passed, recv, acc):
    return pl.pallas_call(
        handed_kernel,
        out_shape=(PAINTED, pltpu.SMEM((1,), I32)),
        in_specs=[VM, VM, VM],
        out_specs=(VM, SM),
        scratch_shapes=paint_scratch(4),
        input_output_aliases={2: 0},
        name="paint_handed",
        compiler_params=ROOM,
        cost_estimate=PAINT_COST,
    )(passed, recv, acc)


def finish_kernel(acc_ref, below_ref, above_ref, th_ref, tl_ref, dens_ref, spec_ref, x_ref):
    wide = lax.broadcasted_iota(I32, (128, 128), 1)
    for i in range(GX):
        before, after = (i - 1) % GX, (i + 1) % GX
        gap = jnp.zeros((124, 128), F32)
        t = jnp.concatenate([below_ref[2 * i : 2 * i + 2], gap, above_ref[2 * i : 2 * i + 2]], axis=0).T
        for j in range(2):
            shifted = pltpu.roll(t, 1 if j == 0 else 127, 1)
            low, high = (t, shifted) if j == 0 else (shifted, t)
            v = acc_ref[i, j, 0:128, :] + jnp.where(wide == 0, low, jnp.where(wide == 127, high, 0.0))
            cols = slice(j * 128, (j + 1) * 128)
            x_ref[i, :, cols] = v
            x_ref[i, 127:128, cols] = v[127:128] + acc_ref[after, j, 128:129, :]
            x_ref[i, 0:1, cols] = v[0:1] + acc_ref[before, j, 129:130, :]
            dens_ref[pl.ds(i * 256 + j, 128, stride=2), :] = x_ref[i, :, cols]

    def put(g, o):
        m, w = GROUPS[g]
        for n, (k, part) in enumerate(((m, 0), (m, 1), (w, 0), (w, 1))):
            for j in range(2):
                spec_ref[pl.ds(part * 1024 + 2 * k + j, 64, stride=16), :] = o[64 * n : 64 * n + 64, j * 128 : (j + 1) * 128]

    transform(lambda b: x_ref[b], th_ref, tl_ref, put)


def finish(acc, below, above, th, tl):
    shape = jax.ShapeDtypeStruct((2048, 128), F32)
    return pl.pallas_call(
        finish_kernel,
        out_shape=(shape, shape),
        in_specs=[VM] * 5,
        out_specs=(VM, VM),
        scratch_shapes=[pltpu.VMEM((GX, 128, 256), F32)],
        name="finish",
        compiler_params=ROOM,
        cost_estimate=pl.CostEstimate(flops=400000000, bytes_accessed=4000000, transcendentals=0),
    )(acc, below, above, th, tl)


def y_pairs(blocks, across):
    pairs = []
    for q in range(blocks):
        n, top = (q + 1) % blocks, (GX - 1) * blocks
        if across or q % RING != RING - 1:
            pairs += [(top + q, n), (n, top + q)]
    return pairs


def exchange(x):
    return lax.all_to_all(x, "gx", split_axis=0, concat_axis=0, tiled=False)


def hand_on(x, across=False):
    return lax.ppermute(x, ("gx", "gy"), y_pairs(lax.axis_size("gy"), across))


def beside(x, up):
    blocks, pairs = lax.axis_size("gy"), []
    for q in range(RING - 1 if up else 0, blocks, RING):
        for p in range(0, GX, 2):
            pairs.append(((p + 1) * blocks + q, p * blocks + q) if up else (p * blocks + q, (p + 1) * blocks + q))
    return lax.ppermute(x, ("gx", "gy"), pairs)


def cross(x, up):
    blocks, pairs = lax.axis_size("gy"), []
    for q in range(RING - 1, blocks, RING):
        n = (q + 1) % blocks
        for p in range(0 if up else 1, GX, 2):
            pairs.append((p * blocks + q, p * blocks + n) if up else (p * blocks + n, p * blocks + q))
    return lax.ppermute(x, ("gx", "gy"), pairs)


def gather(x, n):
    blocks, pairs = lax.axis_size("gy"), []
    for q in range(blocks):
        if q % RING == 0:
            pairs.append((n * blocks + q, q))
        elif q % RING == RING - 1:
            pairs.append(((GX - 1 - n) * blocks + q, (GX - 1) * blocks + q))
    return lax.ppermute(x, ("gx", "gy"), pairs)


def weighted(block):
    row = jnp.where(lax.axis_index("gx") == GX - 1, 17.0, 0.0)
    parts = one_row(*(block[:, o * ROWS : (o + 1) * ROWS] for o in range(5)), row)
    return jnp.concatenate([*parts, jnp.zeros((GX, PAYROWS - 4 * ROWS, 128), F32)], axis=1)


def later_window(ordered, turn):
    _, yp, _ = cells_of(ordered[0])
    live = ordered[4] != 0.0
    key = jnp.where(live, jnp.where(ordered[2] >= 0, yp, yp - 1.0), 20.0)
    space = jnp.zeros((5, NROW + 3 * ROWS, 128), F32)
    padded = jnp.concatenate([space, ordered, space], axis=1)
    base = NROW + 3 * ROWS
    blocks = []
    for p in range(GX):
        if p < GX - 1:
            begin = jnp.sum(jnp.where(key < 2 * p, 1, 0))
            w = jnp.minimum(begin // 128, NROW - ROWS) + turn * ROWS
        else:
            w = jnp.clip((jnp.sum(jnp.where(live, 1, 0)) + 127) // 128 - ROWS, 0, NROW - ROWS) - turn * ROWS
        part = lax.dynamic_slice_in_dim(padded, base + w, ROWS, axis=1).reshape(5 * ROWS, 128)
        blocks.append(jnp.concatenate([part, jnp.zeros((PAYROWS - 5 * ROWS, 128), F32)], axis=0))
    return jnp.stack(blocks)


def body(cell_index, offsets, mass, counts):
    p = lax.axis_index("gx")
    blocks = lax.axis_size("gz")
    ordered, pay, hand = front(
        counts, cell_index.reshape(NROW, 128), offsets.reshape(3, NROW, 128), mass.reshape(NROW, 128)
    )
    next_to = beside(hand, True)
    came_up = cross(join(hand, next_to), True)
    recv = exchange(pay)
    next_to = beside(hand, False)
    came_down = cross(join(hand, next_to), False)
    th, tl = tables()
    held = either(came_up, came_down)
    gathered = [held]
    for n in range(2, GX, 2):
        gathered.append(gather(held, n))
    acc = paint_early(recv)
    packed = forward_pack(recv, acc)
    passed = hand_on(packed)
    acc = paint_late(recv, packed, acc)
    down, up, passed = along_z(recv, passed, gathered, acc)
    below = lax.ppermute(up, "gz", [(i, (i + 1) % blocks) for i in range(blocks)])
    above = lax.ppermute(down, "gz", [((i + 1) % blocks, i) for i in range(blocks)])
    acc, over = paint_handed(passed, recv, acc)
    density, spectrum = finish(acc, below, above, th, tl)

    def slow(outputs):
        mine = jnp.max(recv[:, FACE + 6, 64:]) > 0
        later = lax.cond(
            mine,
            lambda: tuple(exchange(later_window(ordered, t)) for t in (1, 2, 3)),
            lambda: (jnp.zeros(recv.shape, F32),) * 3,
        )
        first = jnp.where(p == GX - 1, ROWS - FROWS, 0)
        row = lax.broadcasted_iota(I32, (PAYROWS, 128), 0) - 4 * ROWS
        sent = (row >= first) & (row < first + FROWS)
        rest = jnp.where(sent, 0.0, recv)
        acc = jnp.zeros(PAINTED.shape, F32)
        for x in (recv, *later):
            acc = paint_more(x, acc)
        for x in (rest, *later):
            acc = paint_more(hand_on(weighted(x), across=True), acc, handed=True)
        acc, _ = paint_handed(passed, recv, acc)
        return finish(acc, below, above, th, tl)

    density, spectrum = lax.cond(over[0] > 0, slow, lambda outputs: outputs, (density, spectrum))
    return density.reshape(1024, 1, 2, 128), spectrum.reshape(2, 512, 1, 2, 128)


def solution(mesh):
    placed = (
        P("gx", "gy", "gz", None),
        P("gx", "gy", "gz", None, None),
        P("gx", "gy", "gz", None),
        P("gx", "gy", "gz"),
    )
    return jax.shard_map(
        body,
        mesh=mesh,
        in_specs=placed,
        out_specs=(P(None, "gx", "gy", "gz"), P(None, None, "gx", "gy", "gz")),
        check_vma=False,
    )
```

```python
import functools
import math

import jax
import jax.numpy as jnp
from jax import lax
from jax.experimental import pallas as pl
from jax.experimental.pallas import tpu as pltpu
from jax.sharding import PartitionSpec as P


F32, I32, BF = jnp.float32, jnp.int32, jnp.bfloat16
GX = 8
RING = 4
ROWS = 17
FROWS = 7
NROW = 64
HANDED = 4 * FROWS + 4
PAYROWS = 96
FACE = 5 * ROWS
XR = 136
LANE = {6: 64, 7: 1, 8: 2, 9: 4, 10: 8, 11: 16, 12: 32}
SUB = {3: 1, 4: 2, 5: 4}
CELL = (1 << 19) - 1
FULL = pltpu.CompilerParams(vmem_limit_bytes=60 * 1024 * 1024)
ROOM = pltpu.CompilerParams(vmem_limit_bytes=12 * 1024 * 1024)
VM = pl.BlockSpec(memory_space=pltpu.VMEM)
SM = pl.BlockSpec(memory_space=pltpu.SMEM)
ANY = pl.BlockSpec(memory_space=pl.ANY)


def cells_of(flat):
    row = jnp.floor((flat + 0.5) * (1.0 / 130.0))
    xp = jnp.floor((row + 0.5) * (1.0 / 18.0))
    return xp, row - 18.0 * xp, flat - 130.0 * row


def halves(value):
    high = value.astype(BF).astype(F32)
    return high, value - high


def index_bit(bit, lane, sub, reg):
    if bit < 3:
        return bool((reg >> bit) & 1)
    if bit in SUB:
        return (sub & SUB[bit]) != 0
    return (lane & LANE[bit]) != 0


def sort_network(ops, lane, sub):
    for size in range(1, 14):
        for bit in range(size - 1, -1, -1):
            new = [[None] * 8 for _ in ops]
            if bit < 3:
                for v in range(8):
                    w = v | (1 << bit)
                    if v == w:
                        continue
                    down = False if size == 13 else index_bit(size, lane, sub, v)
                    a, c = ops[0][v], ops[0][w]
                    if down is True:
                        move = a < c
                    elif down is False:
                        move = a > c
                    else:
                        move = jnp.where(down, c, a) > jnp.where(down, a, c)
                    for o in range(len(ops)):
                        a, c = ops[o][v], ops[o][w]
                        new[o][v] = jnp.where(move, c, a)
                        new[o][w] = jnp.where(move, a, c)
            else:
                axis, step, index = (0, SUB[bit], sub) if bit in SUB else (1, LANE[bit], lane)
                upper = (index & step) != 0
                other = index ^ step

                def partner(x):
                    if 2 * step == x.shape[axis]:
                        return pltpu.roll(x, step, axis)
                    return jnp.take_along_axis(x, other, axis=axis)

                for v in range(8):
                    down = False if size == 13 else index_bit(size, lane, sub, v)
                    mine, theirs = ops[0][v], partner(ops[0][v])
                    if down is True:
                        big = ~upper
                    elif down is False:
                        big = upper
                    else:
                        big = upper ^ down
                    move = jnp.where(big, theirs, mine) > jnp.where(big, mine, theirs)
                    new[0][v] = jnp.where(move, theirs, mine)
                    for o in range(1, len(ops)):
                        new[o][v] = jnp.where(move, partner(ops[o][v]), ops[o][v])
            ops = new
    return ops


def sort_and_pack(count, cell_ref, off_ref, mass_ref, low, high, ghosts, sorted_ref, pay_ref, hand_ref):
    lane = lax.broadcasted_iota(I32, (8, 128), 1)
    sub = lax.broadcasted_iota(I32, (8, 128), 0)
    below = [jnp.zeros((8, 128), F32) for _ in range(18)]
    ops = [[] for _ in range(5)]
    for v in range(8):
        s = slice(8 * v, 8 * v + 8)
        cell, dy = cell_ref[s, :], off_ref[1, s, :]
        live = v * 1024 + sub * 128 + lane < count
        _, yp, _ = cells_of(cell.astype(F32))
        row = jnp.where(live, jnp.where(dy >= 0, yp, yp - 1.0), 20.0)
        for t in range(1, 18):
            below[t] = below[t] + jnp.where(row < t, 1.0, 0.0)
        ops[0].append((row.astype(I32) << 19) | cell)
        for o in range(3):
            ops[o + 1].append(off_ref[o, s, :])
        ops[4].append(jnp.where(live, mass_ref[s, :], 0.0))
    below = [None] + [jnp.sum(b).astype(I32) for b in below[1:]]
    ops = sort_network(ops, lane, sub)
    ops[0] = [(k & CELL).astype(F32) for k in ops[0]]
    for o in range(5):
        t = jnp.concatenate(ops[o], axis=0).T
        sorted_ref[o] = jnp.concatenate([t[:64], t[64:]], axis=1)
    over = below[1] > FROWS * 128
    starts = []
    for p in range(GX):
        if p < GX - 1:
            begin = below[2 * p] if p else jnp.int32(0)
            w = jnp.minimum(begin >> 7, NROW - ROWS)
            over = over | (below[2 * p + 3] > 128 * (w + ROWS))
        else:
            w = jnp.clip(((below[17] + 127) >> 7) - ROWS, 0, NROW - ROWS)
            over = over | (below[2 * p] < 128 * w) | (below[2 * p + 2] < 128 * (w + ROWS - FROWS))
        starts.append(w)
    ghosts = jnp.where(lax.broadcasted_iota(I32, (2, 128), 1) < 64, ghosts, jnp.where(over, 1.0, 0.0))
    for p in range(GX):
        for o in range(5):
            pay_ref[p, o * ROWS : (o + 1) * ROWS, :] = sorted_ref[o, pl.ds(starts[p], ROWS), :]
        past = 17 if p == GX - 1 else 0
        rows = []
        for v in (low, high):
            rows += [v[2 * p + 1 : 2 * p + 3], v[past : past + 1]]
        pay_ref[p, FACE : FACE + 8, :] = jnp.concatenate(rows + [ghosts], axis=0)
        pay_ref[p, FACE + 8 : PAYROWS, :] = jnp.zeros((PAYROWS - FACE - 8, 128), F32)
    last = lax.axis_index("gy") % RING == RING - 1
    first = jnp.where(last, starts[GX - 1] + ROWS - FROWS, 0)
    row = jnp.where(last, 17.0, 0.0)
    parts = [sorted_ref[o, pl.ds(first, FROWS), :] for o in range(5)]
    for o, v in enumerate(one_row(*parts, row)):
        hand_ref[o * FROWS : (o + 1) * FROWS, :] = v
    ends = [jnp.where(last, v[17:18], v[0:1]) for v in (low, high)]
    hand_ref[4 * FROWS : HANDED, :] = jnp.concatenate(ends + [ghosts], axis=0)


def one_row(cell, dx, dy, dz, m, row):
    _, yp, _ = cells_of(cell)
    ay = jnp.abs(dy)
    far = yp + jnp.where(dy >= 0, 1.0, -1.0)
    return cell, dx, dz, m * (jnp.where(yp == row, 1.0 - ay, 0.0) + jnp.where(far == row, ay, 0.0))


def spread(first, second, one, two):
    return jnp.where(first, one, jnp.where(second, two, jnp.zeros((), BF)))


def counting(height, start=0):
    return (lax.broadcasted_iota(I32, (height, 128), 0) + start).astype(F32).astype(BF)


def paint_sources(rows, together, handed, acc_ref, recv_ref, out_ref, val_ref, begin=0, end=GX):
    p = lax.axis_index("gx")
    count = 1 if handed else 2
    grid = counting(16)
    ghost = lax.broadcasted_iota(I32, (16, 128), 0)
    ghost_cell = jnp.where(ghost >= 4 * count, 200, jnp.where((ghost & 1) == 0, 0, 129)).astype(F32).astype(BF)
    ghost_row = (ghost >> 1).astype(F32).astype(BF)

    def prepare(i, slot):
        def op(k):
            return recv_ref[i, k * rows : (k + 1) * rows, :]

        xp, yp, zp = cells_of(op(0))
        if handed:
            dx, dz, weights = op(1), op(2), [op(3)]
        else:
            dx, dy, dz, m = op(1), op(2), op(3), op(4)
            y = yp - (2 * p + 1).astype(F32)
            y1 = y + jnp.where(dy >= 0, 1.0, -1.0)
            ay = jnp.abs(dy)
            weights = [m * (jnp.where(y == j, 1.0 - ay, 0.0) + jnp.where(y1 == j, ay, 0.0)) for j in range(2)]
        ax, az = jnp.abs(dx), jnp.abs(dz)
        coarse = jnp.floor(az * 256.0) * (1.0 / 256.0)
        fine = az - coarse
        vals = [xp, xp + jnp.where(dx >= 0, 1.0, -1.0), zp - 1.0, zp - 1.0 + jnp.where(dz >= 0, 1.0, -1.0)]
        vals += [1.0 - coarse, coarse, -fine, fine]
        for mj in weights:
            for w in (1.0 - ax, ax):
                vals += list(halves(mj * w))
        for n, v in enumerate(vals):
            val_ref[slot, n, 0:rows] = v

    def operands(slot, r):
        def row(n):
            return jnp.broadcast_to(val_ref[slot, n, r : r + 1, :].astype(BF), (16, 128))

        x0, x1, z0, z1 = (row(n) for n in range(4))
        near = [row(8 + 4 * (c // 2) + c % 2) for c in range(2 * count)]
        far = [row(10 + 4 * (c // 2) + c % 2) for c in range(2 * count)]
        a = [[] for _ in range(2 * count)]
        for g in range(8):
            cell = grid + float(16 * g + 1)
            first, second = cell == x0, cell == x1
            for c in range(2 * count):
                a[c].append(spread(first, second, near[c], far[c]))
        w = far[-1]
        for c in range(2 * count - 1):
            w = jnp.where(ghost_row == float(c), far[c], w)
        a = sum(a, []) + [jnp.where(ghost_cell == x1, w, jnp.zeros((), BF))]
        zc, zf = [], []
        weights = [row(n) for n in range(4, 8)]
        for g in range(8):
            cell = grid + float(16 * g)
            first, second = cell == z0, cell == z1
            zc.append(spread(first, second, weights[0], weights[1]))
            zf.append(spread(first, second, weights[2], weights[3]))
        return jnp.concatenate(a, axis=0), jnp.concatenate(zc + zf, axis=0)

    def source(i, slot):
        prepare(i, slot)
        o = None
        for t in range((rows + 1) // 2):
            pairs = [operands(slot, r) for r in range(2 * t, min(2 * t + 2, rows))]
            a = jnp.concatenate([pair[0] for pair in pairs], axis=1)
            z = jnp.concatenate([pair[1] for pair in pairs], axis=1)
            d = lax.dot_general(a, z, (((1,), (1,)), ((), ())), preferred_element_type=F32)
            o = d if o is None else o + d
        ends = o[256 * count : 256 * count + 8, :128] + o[256 * count : 256 * count + 8, 128:]
        ends = ends + pltpu.roll(ends, 6, 0)
        for j in range(count):
            at = jnp.where(p == 0, 0, 1) if handed else j
            high, low = o[256 * j : 256 * j + 128], o[256 * j + 128 : 256 * j + 256]
            total = high[:, :128] + high[:, 128:] + low[:, :128]
            end = ends if j == 0 else pltpu.roll(ends, 4, 0)
            if acc_ref is not None:
                total = total + acc_ref[i, at, 0:128]
                end = end + acc_ref[i, at, 128:136]
            out_ref[i, at, 0:128] = total
            out_ref[i, at, 128:136] = end

    def step(b, carry):
        for u in range(together):
            source(b * together + u, u)
        return carry

    lax.fori_loop(begin // together, end // together, step, 0)


SOME = 2


def painted_early():
    p, block = lax.axis_index("gx"), lax.axis_index("gy")
    q = block % RING
    every = ((q == 0) & (p == 0)) | ((q == RING - 1) & (p == GX - 1))
    return jnp.where(every, GX, jnp.where((q == 0) & (p == GX - 1) & (block > 0), SOME, 0))


def paint_early_kernel(recv_ref, out_ref, val_ref):
    paint_sources(ROWS, 2, False, None, recv_ref, out_ref, val_ref, 0, painted_early())


def paint_late_kernel(recv_ref, after_ref, acc_ref, out_ref, val_ref):
    @pl.when(painted_early() == 0)
    def _():
        paint_sources(ROWS, 4, False, None, recv_ref, out_ref, val_ref)

    @pl.when(painted_early() == SOME)
    def _():
        paint_sources(ROWS, 2, False, None, recv_ref, out_ref, val_ref, SOME)


def paint_more_kernel(handed, recv_ref, acc_ref, out_ref, val_ref):
    if handed:
        out_ref[...] = acc_ref[...]

        @pl.when((lax.axis_index("gx") == 0) | (lax.axis_index("gx") == GX - 1))
        def _():
            paint_sources(ROWS, 1, handed, acc_ref, recv_ref, out_ref, val_ref)
    else:
        paint_sources(ROWS, 1, handed, acc_ref, recv_ref, out_ref, val_ref)


def flagged(ref, row):
    flag = ref[0, row : row + 1, :]
    for i in range(1, GX):
        flag = jnp.maximum(flag, ref[i, row : row + 1, :])
    return jnp.max(jnp.where(lax.broadcasted_iota(I32, (1, 128), 1) >= 64, flag, 0.0)).astype(I32)


def paint_scratch(together):
    return [pltpu.VMEM((together, 16, 24, 128), F32)]


PAINTED = jax.ShapeDtypeStruct((GX, 2, XR, 128), F32)
PAINT_COST = pl.CostEstimate(flops=60000000, bytes_accessed=2000000, transcendentals=0)


def paint_early(recv):
    return pl.pallas_call(
        paint_early_kernel,
        out_shape=PAINTED,
        in_specs=[VM],
        out_specs=VM,
        scratch_shapes=paint_scratch(2),
        name="paint_early",
        compiler_params=ROOM,
        cost_estimate=PAINT_COST,
    )(recv)


def paint_late(recv, after, acc):
    return pl.pallas_call(
        paint_late_kernel,
        out_shape=PAINTED,
        in_specs=[VM, ANY, VM],
        out_specs=VM,
        scratch_shapes=paint_scratch(4),
        input_output_aliases={2: 0},
        name="paint_late",
        compiler_params=ROOM,
        cost_estimate=PAINT_COST,
    )(recv, after, acc)


def paint_more(recv, acc, handed=False):
    return pl.pallas_call(
        functools.partial(paint_more_kernel, handed),
        out_shape=PAINTED,
        in_specs=[VM, VM],
        out_specs=VM,
        scratch_shapes=paint_scratch(1),
        input_output_aliases={1: 0},
        name="paint_more",
        compiler_params=ROOM,
    )(recv, acc)


def paint_faces(count, cell_ref, off_ref, mass_ref, val_ref):
    slot = lax.broadcasted_iota(I32, (NROW, 128), 0) * 128 + lax.broadcasted_iota(I32, (NROW, 128), 1)
    m = jnp.where(slot < count, mass_ref[...], 0.0)
    dx, dy, dz = off_ref[0], off_ref[1], off_ref[2]
    xp, yp, zp = cells_of(cell_ref[...].astype(F32))
    up = (zp == 128.0) & (dz >= 0)
    down = (zp == 1.0) & (dz < 0)
    ax, ay = jnp.abs(dx), jnp.abs(dy)
    w = jnp.where(up | down, m * jnp.abs(dz), 0.0)
    coarse = jnp.floor(ax * 256.0) * (1.0 / 256.0)
    fine = ax - coarse
    y = yp + jnp.where(up, 24.0, 0.0)
    vals = [xp, xp + jnp.where(dx >= 0, 1.0, -1.0), 1.0 - coarse, coarse, -fine, fine]
    vals += [y, y + jnp.where(dy >= 0, 1.0, -1.0)]
    vals += [*halves(w * (1.0 - ay)), *halves(w * ay)]
    for n, v in enumerate(vals):
        val_ref[n] = v
    grid = counting(16)
    ghost = lax.broadcasted_iota(I32, (16, 128), 0)
    ghost_cell = jnp.where(ghost >= 4, 200, jnp.where((ghost & 1) == 0, 0, 129)).astype(F32).astype(BF)
    ghost_fine = (ghost >> 1).astype(F32).astype(BF) == 1.0

    def operands(r):
        def row(n):
            return jnp.broadcast_to(val_ref[n, r : r + 1, :].astype(BF), (16, 128))

        x0, x1, y0, y1 = row(0), row(1), row(6), row(7)
        weights = [row(n) for n in (2, 3, 4, 5, 8, 10, 9, 11)]
        xc, xf, high, low = [], [], [], []
        for g in range(8):
            cell = grid + float(16 * g + 1)
            first, second = cell == x0, cell == x1
            xc.append(spread(first, second, weights[0], weights[1]))
            xf.append(spread(first, second, weights[2], weights[3]))
        ends = jnp.where(ghost_cell == x1, jnp.where(ghost_fine, weights[3], weights[1]), jnp.zeros((), BF))
        for g in range(3):
            cell = grid + float(16 * g)
            first, second = cell == y0, cell == y1
            high.append(spread(first, second, weights[4], weights[5]))
            low.append(spread(first, second, weights[6], weights[7]))
        gap = [jnp.zeros((16, 128), BF)]
        return jnp.concatenate(xc + xf + [ends], axis=0), jnp.concatenate(high + gap + low + gap, axis=0)

    def step(b, total):
        for t in range(8):
            pairs = [operands(16 * b + 2 * t + u) for u in range(2)]
            x = jnp.concatenate([pair[0] for pair in pairs], axis=1)
            v = jnp.concatenate([pair[1] for pair in pairs], axis=1)
            total = total + lax.dot_general(x, v, (((1,), (1,)), ((), ())), preferred_element_type=F32)
        return total

    o = jnp.zeros((272, 128), F32)
    for b in range(NROW // 16):
        o = step(b, o)
    o = o + pltpu.roll(o, 64, 1)
    t = (o[0:128] + o[128:256]).T
    ends = o[256:264] + pltpu.roll(o[256:264], 6, 0)
    return t[0:24], t[24:48], ends[0:2]


def front_kernel(count_ref, cell_ref, off_ref, mass_ref, sorted_ref, pay_ref, hand_ref, val_ref):
    count = count_ref[0, 0, 0]
    low, high, ghosts = paint_faces(count, cell_ref, off_ref, mass_ref, val_ref)
    sort_and_pack(count, cell_ref, off_ref, mass_ref, low, high, ghosts, sorted_ref, pay_ref, hand_ref)


def front(count, cell, off, mass):
    return pl.pallas_call(
        front_kernel,
        out_shape=(
            jax.ShapeDtypeStruct((5, NROW, 128), F32),
            jax.ShapeDtypeStruct((GX, PAYROWS, 128), F32),
            pltpu.VMEM((HANDED, 128), F32),
        ),
        in_specs=[SM, VM, VM, VM],
        out_specs=(VM, VM, VM),
        scratch_shapes=[pltpu.VMEM((12, NROW, 128), F32)],
        name="front",
        compiler_params=FULL,
        cost_estimate=pl.CostEstimate(flops=40000000, bytes_accessed=1000000, transcendentals=0),
    )(count, cell, off, mass)


def forward_kernel(recv_ref, acc_ref, out_ref):
    last = lax.axis_index("gx") == GX - 1
    first = jnp.where(last, ROWS - FROWS, 0)
    row = jnp.where(last, 17.0, 0.0)
    for i in range(GX):
        parts = [recv_ref[i, pl.ds(o * ROWS + first, FROWS), :] for o in range(5)]
        for o, v in enumerate(one_row(*parts, row)):
            out_ref[i, o * FROWS : (o + 1) * FROWS, :] = v
        for n, r in enumerate((2, 5, 6, 7)):
            out_ref[i, 4 * FROWS + n : 4 * FROWS + n + 1, :] = recv_ref[i, FACE + r : FACE + r + 1, :]


def forward_pack(recv, acc):
    return pl.pallas_call(
        forward_kernel,
        out_shape=jax.ShapeDtypeStruct((GX, HANDED, 128), F32),
        in_specs=[VM, ANY],
        out_specs=VM,
        name="forward_pack",
        compiler_params=ROOM,
        cost_estimate=pl.CostEstimate(flops=500000, bytes_accessed=600000, transcendentals=0),
    )(recv, acc)


def join_kernel(one_ref, two_ref, out_ref):
    out_ref[0] = one_ref[...]
    out_ref[1] = two_ref[...]


def join(one, two):
    return pl.pallas_call(
        join_kernel,
        out_shape=jax.ShapeDtypeStruct((2, HANDED, 128), F32),
        in_specs=[VM, VM],
        out_specs=VM,
        name="join",
        compiler_params=ROOM,
    )(one, two)


def either_kernel(one_ref, two_ref, out_ref):
    out_ref[...] = one_ref[...] + two_ref[...]


def either(one, two):
    return pl.pallas_call(
        either_kernel,
        out_shape=jax.ShapeDtypeStruct((2, HANDED, 128), F32),
        in_specs=[VM, VM],
        out_specs=VM,
        name="either",
        compiler_params=ROOM,
    )(one, two)


def table_kernel(high_ref, low_ref):
    scale = 1.0 / 32.0
    j = lax.broadcasted_iota(I32, (64, 128), 1)
    k8 = 8 * lax.broadcasted_iota(I32, (64, 128), 0)
    none = jnp.zeros((64, 128), F32)

    def turns(m):
        angle = (((k8 + m) * j) & 1023).astype(F32) * (2.0 * math.pi / 1024.0)
        return jnp.cos(angle) * scale, jnp.sin(angle) * scale

    for g, (m, w) in enumerate(((1, 7), (3, 5), (2, 6), (0, 4))):
        (c, s), (e, t) = turns(m), turns(w)
        if g < 3:
            parts = ((c, s), (-s, c), (e, -t), (-t, -e))
        else:
            parts = ((c, none), (-s, none), (none, e), (none, -t))
        for n, pair in enumerate(parts):
            for h, value in enumerate(pair):
                high = value.astype(BF)
                high_ref[g, 64 * n : 64 * n + 64, 128 * h : 128 * h + 128] = high
                low_ref[g, 64 * n : 64 * n + 64, 128 * h : 128 * h + 128] = (value - high.astype(F32)).astype(BF)


def tables():
    shape = jax.ShapeDtypeStruct((4, 256, 256), BF)
    return pl.pallas_call(
        table_kernel,
        out_shape=(shape, shape),
        out_specs=(VM, VM),
        name="tables",
        compiler_params=ROOM,
        cost_estimate=pl.CostEstimate(flops=8000000, bytes_accessed=1000000, transcendentals=0),
    )()


GROUPS = ((1, 7), (3, 5), (2, 6), (0, 4))


def transform(field, th_ref, tl_ref, put):
    root = math.sqrt(0.5)

    def even(b):
        return field(b) + field(b + 4)

    def odd(b):
        return field(b) - field(b + 4)

    for g in range(4):
        if g < 2:
            d1, d3 = odd(1), odd(3)
            s, t = (d1 - d3) * root, (d1 + d3) * root
            pair = (odd(0) + s, -odd(2) - t) if g == 0 else (odd(0) - s, odd(2) - t)
        elif g == 2:
            pair = (even(0) - even(2), even(3) - even(1))
        else:
            s, t = even(0) + even(2), even(1) + even(3)
            pair = (s + t, s - t)
        value = jnp.concatenate(pair, axis=0)
        high = value.astype(BF)
        low = (value - high.astype(F32)).astype(BF)
        o = jnp.dot(th_ref[g], high, preferred_element_type=F32)
        o = o + jnp.dot(tl_ref[g], high, preferred_element_type=F32)
        put(g, o + jnp.dot(th_ref[g], low, preferred_element_type=F32))


def face_columns(i, rows, ghosts):
    before, after = (i - 1) % GX, (i + 1) % GX
    lane = lax.broadcasted_iota(I32, (1, 128), 1)
    out = []
    for side in range(2):
        v = rows[i][side] + jnp.where(lane == 127, ghosts[after][side][0:1], 0.0)
        out.append(v + jnp.where(lane == 0, ghosts[before][side][1:2], 0.0))
    return out


def pick(v, lane):
    return jnp.sum(jnp.where(lax.broadcasted_iota(I32, (2, 128), 1) == lane, v, 0.0), axis=1, keepdims=True)


def along_z_kernel(face_ref, in_ref, *refs):
    gathered, (after_ref, down_ref, up_ref, all_ref) = refs[: GX // 2], refs[GX // 2 :]
    p, q = lax.axis_index("gx"), lax.axis_index("gy") % RING
    across = ((p == 0) & (q == 0)) | ((p == GX - 1) & (q == RING - 1))
    for i in range(GX):
        n = GX - 1 - i
        mine = jnp.where(p == 0, gathered[i // 2][i % 2], gathered[n // 2][n % 2])
        all_ref[i] = jnp.where(across, mine, in_ref[i])
    for j in range(2):
        on = p == (0 if j == 0 else GX - 1)
        rows, ghosts = [], []
        for i in range(GX):
            own, handed = face_ref[i, FACE : FACE + 8, :], all_ref[i, 4 * FROWS : HANDED, :]
            rows.append([own[3 * n + j : 3 * n + j + 1] + jnp.where(on, handed[n : n + 1], 0.0) for n in range(2)])
            past = [pick(own[6:8], base + 2 * p + 1 + j) for base in (0, 24)]
            more = [pick(handed[2:4], base + (17 if j == 0 else 0)) for base in (0, 24)]
            ghosts.append([a + jnp.where(on, b, 0.0) for a, b in zip(past, more)])
        for i in range(GX):
            down, up = face_columns(i, rows, ghosts)
            down_ref[2 * i + j : 2 * i + j + 1] = down
            up_ref[2 * i + j : 2 * i + j + 1] = up


def along_z(recv, passed, gathered, after):
    shape = jax.ShapeDtypeStruct((2 * GX, 128), F32)
    return pl.pallas_call(
        along_z_kernel,
        out_shape=(shape, shape, jax.ShapeDtypeStruct((GX, HANDED, 128), F32)),
        in_specs=[VM] * (2 + GX // 2) + [ANY],
        out_specs=(VM, VM, VM),
        name="along_z",
        compiler_params=ROOM,
        cost_estimate=pl.CostEstimate(flops=500000, bytes_accessed=100000, transcendentals=0),
    )(recv, passed, *gathered, after)


def handed_kernel(in_ref, face_ref, acc_ref, out_ref, flag_ref, val_ref):
    p = lax.axis_index("gx")
    flag_ref[0] = flagged(face_ref, FACE + 6)

    @pl.when((p == 0) | (p == GX - 1))
    def _():
        flag_ref[0] = jnp.maximum(flag_ref[0], flagged(in_ref, 4 * FROWS + 2))
        paint_sources(FROWS, 4, True, acc_ref, in_ref, out_ref, val_ref)


def paint_handed(passed, recv, acc):
    return pl.pallas_call(
        handed_kernel,
        out_shape=(PAINTED, pltpu.SMEM((1,), I32)),
        in_specs=[VM, VM, VM],
        out_specs=(VM, SM),
        scratch_shapes=paint_scratch(4),
        input_output_aliases={2: 0},
        name="paint_handed",
        compiler_params=ROOM,
        cost_estimate=PAINT_COST,
    )(passed, recv, acc)


def finish_kernel(acc_ref, below_ref, above_ref, th_ref, tl_ref, dens_ref, spec_ref, x_ref):
    wide = lax.broadcasted_iota(I32, (128, 128), 1)
    for i in range(GX):
        before, after = (i - 1) % GX, (i + 1) % GX
        gap = jnp.zeros((124, 128), F32)
        t = jnp.concatenate([below_ref[2 * i : 2 * i + 2], gap, above_ref[2 * i : 2 * i + 2]], axis=0).T
        for j in range(2):
            shifted = pltpu.roll(t, 1 if j == 0 else 127, 1)
            low, high = (t, shifted) if j == 0 else (shifted, t)
            v = acc_ref[i, j, 0:128, :] + jnp.where(wide == 0, low, jnp.where(wide == 127, high, 0.0))
            cols = slice(j * 128, (j + 1) * 128)
            x_ref[i, :, cols] = v
            x_ref[i, 127:128, cols] = v[127:128] + acc_ref[after, j, 128:129, :]
            x_ref[i, 0:1, cols] = v[0:1] + acc_ref[before, j, 129:130, :]
            dens_ref[pl.ds(i * 256 + j, 128, stride=2), :] = x_ref[i, :, cols]

    def put(g, o):
        m, w = GROUPS[g]
        for n, (k, part) in enumerate(((m, 0), (m, 1), (w, 0), (w, 1))):
            for j in range(2):
                spec_ref[pl.ds(part * 1024 + 2 * k + j, 64, stride=16), :] = o[64 * n : 64 * n + 64, j * 128 : (j + 1) * 128]

    transform(lambda b: x_ref[b], th_ref, tl_ref, put)


def finish(acc, below, above, th, tl):
    shape = jax.ShapeDtypeStruct((2048, 128), F32)
    return pl.pallas_call(
        finish_kernel,
        out_shape=(shape, shape),
        in_specs=[VM] * 5,
        out_specs=(VM, VM),
        scratch_shapes=[pltpu.VMEM((GX, 128, 256), F32)],
        name="finish",
        compiler_params=ROOM,
        cost_estimate=pl.CostEstimate(flops=400000000, bytes_accessed=4000000, transcendentals=0),
    )(acc, below, above, th, tl)


def y_pairs(blocks, across):
    pairs = []
    for q in range(blocks):
        n, top = (q + 1) % blocks, (GX - 1) * blocks
        if across or q % RING != RING - 1:
            pairs += [(top + q, n), (n, top + q)]
    return pairs


def exchange(x):
    return lax.all_to_all(x, "gx", split_axis=0, concat_axis=0, tiled=False)


def hand_on(x, across=False):
    return lax.ppermute(x, ("gx", "gy"), y_pairs(lax.axis_size("gy"), across))


def beside(x, up):
    blocks, pairs = lax.axis_size("gy"), []
    for q in range(RING - 1 if up else 0, blocks, RING):
        for p in range(0, GX, 2):
            pairs.append(((p + 1) * blocks + q, p * blocks + q) if up else (p * blocks + q, (p + 1) * blocks + q))
    return lax.ppermute(x, ("gx", "gy"), pairs)


def cross(x, up):
    blocks, pairs = lax.axis_size("gy"), []
    for q in range(RING - 1, blocks, RING):
        n = (q + 1) % blocks
        for p in range(0 if up else 1, GX, 2):
            pairs.append((p * blocks + q, p * blocks + n) if up else (p * blocks + n, p * blocks + q))
    return lax.ppermute(x, ("gx", "gy"), pairs)


def gather(x, n):
    blocks, pairs = lax.axis_size("gy"), []
    for q in range(blocks):
        if q % RING == 0:
            pairs.append((n * blocks + q, q))
        elif q % RING == RING - 1:
            pairs.append(((GX - 1 - n) * blocks + q, (GX - 1) * blocks + q))
    return lax.ppermute(x, ("gx", "gy"), pairs)


def weighted(block):
    row = jnp.where(lax.axis_index("gx") == GX - 1, 17.0, 0.0)
    parts = one_row(*(block[:, o * ROWS : (o + 1) * ROWS] for o in range(5)), row)
    return jnp.concatenate([*parts, jnp.zeros((GX, PAYROWS - 4 * ROWS, 128), F32)], axis=1)


def later_window(ordered, turn):
    _, yp, _ = cells_of(ordered[0])
    live = ordered[4] != 0.0
    key = jnp.where(live, jnp.where(ordered[2] >= 0, yp, yp - 1.0), 20.0)
    space = jnp.zeros((5, NROW + 3 * ROWS, 128), F32)
    padded = jnp.concatenate([space, ordered, space], axis=1)
    base = NROW + 3 * ROWS
    blocks = []
    for p in range(GX):
        if p < GX - 1:
            begin = jnp.sum(jnp.where(key < 2 * p, 1, 0))
            w = jnp.minimum(begin // 128, NROW - ROWS) + turn * ROWS
        else:
            w = jnp.clip((jnp.sum(jnp.where(live, 1, 0)) + 127) // 128 - ROWS, 0, NROW - ROWS) - turn * ROWS
        part = lax.dynamic_slice_in_dim(padded, base + w, ROWS, axis=1).reshape(5 * ROWS, 128)
        blocks.append(jnp.concatenate([part, jnp.zeros((PAYROWS - 5 * ROWS, 128), F32)], axis=0))
    return jnp.stack(blocks)


def body(cell_index, offsets, mass, counts):
    p = lax.axis_index("gx")
    blocks = lax.axis_size("gz")
    ordered, pay, hand = front(
        counts, cell_index.reshape(NROW, 128), offsets.reshape(3, NROW, 128), mass.reshape(NROW, 128)
    )
    next_to = beside(hand, True)
    came_up = cross(join(hand, next_to), True)
    recv = exchange(pay)
    next_to = beside(hand, False)
    came_down = cross(join(hand, next_to), False)
    th, tl = tables()
    held = either(came_up, came_down)
    gathered = [held]
    for n in range(2, GX, 2):
        gathered.append(gather(held, n))
    acc = paint_early(recv)
    packed = forward_pack(recv, acc)
    passed = hand_on(packed)
    acc = paint_late(recv, packed, acc)
    down, up, passed = along_z(recv, passed, gathered, acc)
    below = lax.ppermute(up, "gz", [(i, (i + 1) % blocks) for i in range(blocks)])
    above = lax.ppermute(down, "gz", [((i + 1) % blocks, i) for i in range(blocks)])
    acc, over = paint_handed(passed, recv, acc)
    density, spectrum = finish(acc, below, above, th, tl)

    def slow(outputs):
        mine = jnp.max(recv[:, FACE + 6, 64:]) > 0
        later = lax.cond(
            mine,
            lambda: tuple(exchange(later_window(ordered, t)) for t in (1, 2, 3)),
            lambda: (jnp.zeros(recv.shape, F32),) * 3,
        )
        first = jnp.where(p == GX - 1, ROWS - FROWS, 0)
        row = lax.broadcasted_iota(I32, (PAYROWS, 128), 0) - 4 * ROWS
        sent = (row >= first) & (row < first + FROWS)
        rest = jnp.where(sent, 0.0, recv)
        acc = jnp.zeros(PAINTED.shape, F32)
        for x in (recv, *later):
            acc = paint_more(x, acc)
        for x in (rest, *later):
            acc = paint_more(hand_on(weighted(x), across=True), acc, handed=True)
        acc, _ = paint_handed(passed, recv, acc)
        return finish(acc, below, above, th, tl)

    density, spectrum = lax.cond(over[0] > 0, slow, lambda outputs: outputs, (density, spectrum))
    return density.reshape(1024, 1, 2, 128), spectrum.reshape(2, 512, 1, 2, 128)


def solution(mesh):
    placed = (
        P("gx", "gy", "gz", None),
        P("gx", "gy", "gz", None, None),
        P("gx", "gy", "gz", None),
        P("gx", "gy", "gz"),
    )
    return jax.shard_map(
        body,
        mesh=mesh,
        in_specs=placed,
        out_specs=(P(None, "gx", "gy", "gz"), P(None, None, "gx", "gy", "gz")),
        check_vma=False,
    )
```

```python
import functools
import math

import jax
import jax.numpy as jnp
from jax import lax
from jax.experimental import pallas as pl
from jax.experimental.pallas import tpu as pltpu
from jax.sharding import PartitionSpec as P


F32, I32, BF = jnp.float32, jnp.int32, jnp.bfloat16
GX = 8
RING = 4
ROWS = 17
FROWS = 7
NROW = 64
HANDED = 4 * FROWS + 4
PAYROWS = 96
FACE = 5 * ROWS
XR = 136
LANE = {6: 64, 7: 1, 8: 2, 9: 4, 10: 8, 11: 16, 12: 32}
SUB = {3: 1, 4: 2, 5: 4}
CELL = (1 << 19) - 1
FULL = pltpu.CompilerParams(vmem_limit_bytes=60 * 1024 * 1024)
ROOM = pltpu.CompilerParams(vmem_limit_bytes=12 * 1024 * 1024)
VM = pl.BlockSpec(memory_space=pltpu.VMEM)
SM = pl.BlockSpec(memory_space=pltpu.SMEM)
ANY = pl.BlockSpec(memory_space=pl.ANY)


def cells_of(flat):
    row = jnp.floor((flat + 0.5) * (1.0 / 130.0))
    xp = jnp.floor((row + 0.5) * (1.0 / 18.0))
    return xp, row - 18.0 * xp, flat - 130.0 * row


def halves(value):
    high = value.astype(BF).astype(F32)
    return high, value - high


def index_bit(bit, lane, sub, reg):
    if bit < 3:
        return bool((reg >> bit) & 1)
    if bit in SUB:
        return (sub & SUB[bit]) != 0
    return (lane & LANE[bit]) != 0


def sort_network(ops, lane, sub):
    for size in range(1, 14):
        for bit in range(size - 1, -1, -1):
            new = [[None] * 8 for _ in ops]
            if bit < 3:
                for v in range(8):
                    w = v | (1 << bit)
                    if v == w:
                        continue
                    down = False if size == 13 else index_bit(size, lane, sub, v)
                    a, c = ops[0][v], ops[0][w]
                    if down is True:
                        move = a < c
                    elif down is False:
                        move = a > c
                    else:
                        move = jnp.where(down, c, a) > jnp.where(down, a, c)
                    for o in range(len(ops)):
                        a, c = ops[o][v], ops[o][w]
                        new[o][v] = jnp.where(move, c, a)
                        new[o][w] = jnp.where(move, a, c)
            else:
                axis, step, index = (0, SUB[bit], sub) if bit in SUB else (1, LANE[bit], lane)
                upper = (index & step) != 0
                other = index ^ step

                def partner(x):
                    if 2 * step == x.shape[axis]:
                        return pltpu.roll(x, step, axis)
                    return jnp.take_along_axis(x, other, axis=axis)

                for v in range(8):
                    down = False if size == 13 else index_bit(size, lane, sub, v)
                    mine, theirs = ops[0][v], partner(ops[0][v])
                    if down is True:
                        big = ~upper
                    elif down is False:
                        big = upper
                    else:
                        big = upper ^ down
                    move = jnp.where(big, theirs, mine) > jnp.where(big, mine, theirs)
                    new[0][v] = jnp.where(move, theirs, mine)
                    for o in range(1, len(ops)):
                        new[o][v] = jnp.where(move, partner(ops[o][v]), ops[o][v])
            ops = new
    return ops


def sort_and_pack(count, cell_ref, off_ref, mass_ref, low, high, ghosts, sorted_ref, pay_ref, hand_ref):
    lane = lax.broadcasted_iota(I32, (8, 128), 1)
    sub = lax.broadcasted_iota(I32, (8, 128), 0)
    below = [jnp.zeros((8, 128), F32) for _ in range(18)]
    ops = [[] for _ in range(5)]
    for v in range(8):
        s = slice(8 * v, 8 * v + 8)
        cell, dy = cell_ref[s, :], off_ref[1, s, :]
        live = v * 1024 + sub * 128 + lane < count
        _, yp, _ = cells_of(cell.astype(F32))
        row = jnp.where(live, jnp.where(dy >= 0, yp, yp - 1.0), 20.0)
        for t in range(1, 18):
            below[t] = below[t] + jnp.where(row < t, 1.0, 0.0)
        ops[0].append((row.astype(I32) << 19) | cell)
        for o in range(3):
            ops[o + 1].append(off_ref[o, s, :])
        ops[4].append(jnp.where(live, mass_ref[s, :], 0.0))
    below = [None] + [jnp.sum(b).astype(I32) for b in below[1:]]
    ops = sort_network(ops, lane, sub)
    ops[0] = [(k & CELL).astype(F32) for k in ops[0]]
    for o in range(5):
        t = jnp.concatenate(ops[o], axis=0).T
        sorted_ref[o] = jnp.concatenate([t[:64], t[64:]], axis=1)
    over = below[1] > FROWS * 128
    starts = []
    for p in range(GX):
        if p < GX - 1:
            begin = below[2 * p] if p else jnp.int32(0)
            w = jnp.minimum(begin >> 7, NROW - ROWS)
            over = over | (below[2 * p + 3] > 128 * (w + ROWS))
        else:
            w = jnp.clip(((below[17] + 127) >> 7) - ROWS, 0, NROW - ROWS)
            over = over | (below[2 * p] < 128 * w) | (below[2 * p + 2] < 128 * (w + ROWS - FROWS))
        starts.append(w)
    ghosts = jnp.where(lax.broadcasted_iota(I32, (2, 128), 1) < 64, ghosts, jnp.where(over, 1.0, 0.0))
    for p in range(GX):
        for o in range(5):
            pay_ref[p, o * ROWS : (o + 1) * ROWS, :] = sorted_ref[o, pl.ds(starts[p], ROWS), :]
        past = 17 if p == GX - 1 else 0
        rows = []
        for v in (low, high):
            rows += [v[2 * p + 1 : 2 * p + 3], v[past : past + 1]]
        pay_ref[p, FACE : FACE + 8, :] = jnp.concatenate(rows + [ghosts], axis=0)
        pay_ref[p, FACE + 8 : PAYROWS, :] = jnp.zeros((PAYROWS - FACE - 8, 128), F32)
    last = lax.axis_index("gy") % RING == RING - 1
    first = jnp.where(last, starts[GX - 1] + ROWS - FROWS, 0)
    row = jnp.where(last, 17.0, 0.0)
    parts = [sorted_ref[o, pl.ds(first, FROWS), :] for o in range(5)]
    for o, v in enumerate(one_row(*parts, row)):
        hand_ref[o * FROWS : (o + 1) * FROWS, :] = v
    ends = [jnp.where(last, v[17:18], v[0:1]) for v in (low, high)]
    hand_ref[4 * FROWS : HANDED, :] = jnp.concatenate(ends + [ghosts], axis=0)


def one_row(cell, dx, dy, dz, m, row):
    _, yp, _ = cells_of(cell)
    ay = jnp.abs(dy)
    far = yp + jnp.where(dy >= 0, 1.0, -1.0)
    return cell, dx, dz, m * (jnp.where(yp == row, 1.0 - ay, 0.0) + jnp.where(far == row, ay, 0.0))


def spread(first, second, one, two):
    return jnp.where(first, one, jnp.where(second, two, jnp.zeros((), BF)))


def counting(height, start=0):
    return (lax.broadcasted_iota(I32, (height, 128), 0) + start).astype(F32).astype(BF)


def paint_sources(rows, together, handed, acc_ref, recv_ref, out_ref, val_ref, begin=0, end=GX):
    p = lax.axis_index("gx")
    count = 1 if handed else 2
    grid = counting(16)
    ghost = lax.broadcasted_iota(I32, (16, 128), 0)
    ghost_cell = jnp.where(ghost >= 4 * count, 200, jnp.where((ghost & 1) == 0, 0, 129)).astype(F32).astype(BF)
    ghost_row = (ghost >> 1).astype(F32).astype(BF)

    def prepare(i, slot):
        def op(k):
            return recv_ref[i, k * rows : (k + 1) * rows, :]

        xp, yp, zp = cells_of(op(0))
        if handed:
            dx, dz, weights = op(1), op(2), [op(3)]
        else:
            dx, dy, dz, m = op(1), op(2), op(3), op(4)
            y = yp - (2 * p + 1).astype(F32)
            y1 = y + jnp.where(dy >= 0, 1.0, -1.0)
            ay = jnp.abs(dy)
            weights = [m * (jnp.where(y == j, 1.0 - ay, 0.0) + jnp.where(y1 == j, ay, 0.0)) for j in range(2)]
        ax, az = jnp.abs(dx), jnp.abs(dz)
        coarse = jnp.floor(az * 256.0) * (1.0 / 256.0)
        fine = az - coarse
        vals = [xp, xp + jnp.where(dx >= 0, 1.0, -1.0), zp - 1.0, zp - 1.0 + jnp.where(dz >= 0, 1.0, -1.0)]
        vals += [1.0 - coarse, coarse, -fine, fine]
        for mj in weights:
            for w in (1.0 - ax, ax):
                vals += list(halves(mj * w))
        for n, v in enumerate(vals):
            val_ref[slot, n, 0:rows] = v

    def operands(slot, r):
        def row(n):
            return jnp.broadcast_to(val_ref[slot, n, r : r + 1, :].astype(BF), (16, 128))

        x0, x1, z0, z1 = (row(n) for n in range(4))
        near = [row(8 + 4 * (c // 2) + c % 2) for c in range(2 * count)]
        far = [row(10 + 4 * (c // 2) + c % 2) for c in range(2 * count)]
        a = [[] for _ in range(2 * count)]
        for g in range(8):
            cell = grid + float(16 * g + 1)
            first, second = cell == x0, cell == x1
            for c in range(2 * count):
                a[c].append(spread(first, second, near[c], far[c]))
        w = far[-1]
        for c in range(2 * count - 1):
            w = jnp.where(ghost_row == float(c), far[c], w)
        a = sum(a, []) + [jnp.where(ghost_cell == x1, w, jnp.zeros((), BF))]
        zc, zf = [], []
        weights = [row(n) for n in range(4, 8)]
        for g in range(8):
            cell = grid + float(16 * g)
            first, second = cell == z0, cell == z1
            zc.append(spread(first, second, weights[0], weights[1]))
            zf.append(spread(first, second, weights[2], weights[3]))
        return jnp.concatenate(a, axis=0), jnp.concatenate(zc + zf, axis=0)

    def source(i, slot):
        prepare(i, slot)
        o = None
        for t in range((rows + 1) // 2):
            pairs = [operands(slot, r) for r in range(2 * t, min(2 * t + 2, rows))]
            a = jnp.concatenate([pair[0] for pair in pairs], axis=1)
            z = jnp.concatenate([pair[1] for pair in pairs], axis=1)
            d = lax.dot_general(a, z, (((1,), (1,)), ((), ())), preferred_element_type=F32)
            o = d if o is None else o + d
        ends = o[256 * count : 256 * count + 8, :128] + o[256 * count : 256 * count + 8, 128:]
        ends = ends + pltpu.roll(ends, 6, 0)
        for j in range(count):
            at = jnp.where(p == 0, 0, 1) if handed else j
            high, low = o[256 * j : 256 * j + 128], o[256 * j + 128 : 256 * j + 256]
            total = high[:, :128] + high[:, 128:] + low[:, :128]
            end = ends if j == 0 else pltpu.roll(ends, 4, 0)
            if acc_ref is not None:
                total = total + acc_ref[i, at, 0:128]
                end = end + acc_ref[i, at, 128:136]
            out_ref[i, at, 0:128] = total
            out_ref[i, at, 128:136] = end

    def step(b, carry):
        for u in range(together):
            source(b * together + u, u)
        return carry

    lax.fori_loop(begin // together, end // together, step, 0)


SOME = 2


def painted_early():
    p, block = lax.axis_index("gx"), lax.axis_index("gy")
    q = block % RING
    every = ((q == 0) & (p == 0)) | ((q == RING - 1) & (p == GX - 1))
    return jnp.where(every, GX, jnp.where((q == 0) & (p == GX - 1) & (block > 0), SOME, 0))


def paint_early_kernel(recv_ref, out_ref, val_ref):
    paint_sources(ROWS, 2, False, None, recv_ref, out_ref, val_ref, 0, painted_early())


def paint_late_kernel(recv_ref, after_ref, acc_ref, out_ref, val_ref):
    @pl.when(painted_early() == 0)
    def _():
        paint_sources(ROWS, 4, False, None, recv_ref, out_ref, val_ref)

    @pl.when(painted_early() == SOME)
    def _():
        paint_sources(ROWS, 2, False, None, recv_ref, out_ref, val_ref, SOME)


def paint_more_kernel(handed, recv_ref, acc_ref, out_ref, val_ref):
    if handed:
        out_ref[...] = acc_ref[...]

        @pl.when((lax.axis_index("gx") == 0) | (lax.axis_index("gx") == GX - 1))
        def _():
            paint_sources(ROWS, 1, handed, acc_ref, recv_ref, out_ref, val_ref)
    else:
        paint_sources(ROWS, 1, handed, acc_ref, recv_ref, out_ref, val_ref)


def flagged(ref, row):
    flag = ref[0, row : row + 1, :]
    for i in range(1, GX):
        flag = jnp.maximum(flag, ref[i, row : row + 1, :])
    return jnp.max(jnp.where(lax.broadcasted_iota(I32, (1, 128), 1) >= 64, flag, 0.0)).astype(I32)


def paint_scratch(together):
    return [pltpu.VMEM((together, 16, 24, 128), F32)]


PAINTED = jax.ShapeDtypeStruct((GX, 2, XR, 128), F32)
PAINT_COST = pl.CostEstimate(flops=60000000, bytes_accessed=2000000, transcendentals=0)


def paint_early(recv):
    return pl.pallas_call(
        paint_early_kernel,
        out_shape=PAINTED,
        in_specs=[VM],
        out_specs=VM,
        scratch_shapes=paint_scratch(2),
        name="paint_early",
        compiler_params=ROOM,
        cost_estimate=PAINT_COST,
    )(recv)


def paint_late(recv, after, acc):
    return pl.pallas_call(
        paint_late_kernel,
        out_shape=PAINTED,
        in_specs=[VM, ANY, VM],
        out_specs=VM,
        scratch_shapes=paint_scratch(4),
        input_output_aliases={2: 0},
        name="paint_late",
        compiler_params=ROOM,
        cost_estimate=PAINT_COST,
    )(recv, after, acc)


def paint_more(recv, acc, handed=False):
    return pl.pallas_call(
        functools.partial(paint_more_kernel, handed),
        out_shape=PAINTED,
        in_specs=[VM, VM],
        out_specs=VM,
        scratch_shapes=paint_scratch(1),
        input_output_aliases={1: 0},
        name="paint_more",
        compiler_params=ROOM,
    )(recv, acc)


def paint_faces(count, cell_ref, off_ref, mass_ref, val_ref):
    slot = lax.broadcasted_iota(I32, (NROW, 128), 0) * 128 + lax.broadcasted_iota(I32, (NROW, 128), 1)
    m = jnp.where(slot < count, mass_ref[...], 0.0)
    dx, dy, dz = off_ref[0], off_ref[1], off_ref[2]
    xp, yp, zp = cells_of(cell_ref[...].astype(F32))
    up = (zp == 128.0) & (dz >= 0)
    down = (zp == 1.0) & (dz < 0)
    ax, ay = jnp.abs(dx), jnp.abs(dy)
    w = jnp.where(up | down, m * jnp.abs(dz), 0.0)
    coarse = jnp.floor(ax * 256.0) * (1.0 / 256.0)
    fine = ax - coarse
    y = yp + jnp.where(up, 24.0, 0.0)
    vals = [xp, xp + jnp.where(dx >= 0, 1.0, -1.0), 1.0 - coarse, coarse, -fine, fine]
    vals += [y, y + jnp.where(dy >= 0, 1.0, -1.0)]
    vals += [*halves(w * (1.0 - ay)), *halves(w * ay)]
    for n, v in enumerate(vals):
        val_ref[n] = v
    grid = counting(16)
    ghost = lax.broadcasted_iota(I32, (16, 128), 0)
    ghost_cell = jnp.where(ghost >= 4, 200, jnp.where((ghost & 1) == 0, 0, 129)).astype(F32).astype(BF)
    ghost_fine = (ghost >> 1).astype(F32).astype(BF) == 1.0

    def operands(r):
        def row(n):
            return jnp.broadcast_to(val_ref[n, r : r + 1, :].astype(BF), (16, 128))

        x0, x1, y0, y1 = row(0), row(1), row(6), row(7)
        weights = [row(n) for n in (2, 3, 4, 5, 8, 10, 9, 11)]
        xc, xf, high, low = [], [], [], []
        for g in range(8):
            cell = grid + float(16 * g + 1)
            first, second = cell == x0, cell == x1
            xc.append(spread(first, second, weights[0], weights[1]))
            xf.append(spread(first, second, weights[2], weights[3]))
        ends = jnp.where(ghost_cell == x1, jnp.where(ghost_fine, weights[3], weights[1]), jnp.zeros((), BF))
        for g in range(3):
            cell = grid + float(16 * g)
            first, second = cell == y0, cell == y1
            high.append(spread(first, second, weights[4], weights[5]))
            low.append(spread(first, second, weights[6], weights[7]))
        gap = [jnp.zeros((16, 128), BF)]
        return jnp.concatenate(xc + xf + [ends], axis=0), jnp.concatenate(high + gap + low + gap, axis=0)

    def step(b, total):
        for t in range(8):
            pairs = [operands(16 * b + 2 * t + u) for u in range(2)]
            x = jnp.concatenate([pair[0] for pair in pairs], axis=1)
            v = jnp.concatenate([pair[1] for pair in pairs], axis=1)
            total = total + lax.dot_general(x, v, (((1,), (1,)), ((), ())), preferred_element_type=F32)
        return total

    o = jnp.zeros((272, 128), F32)
    for b in range(NROW // 16):
        o = step(b, o)
    o = o + pltpu.roll(o, 64, 1)
    t = (o[0:128] + o[128:256]).T
    ends = o[256:264] + pltpu.roll(o[256:264], 6, 0)
    return t[0:24], t[24:48], ends[0:2]


def front_kernel(count_ref, cell_ref, off_ref, mass_ref, sorted_ref, pay_ref, hand_ref, val_ref):
    count = count_ref[0, 0, 0]
    low, high, ghosts = paint_faces(count, cell_ref, off_ref, mass_ref, val_ref)
    sort_and_pack(count, cell_ref, off_ref, mass_ref, low, high, ghosts, sorted_ref, pay_ref, hand_ref)


def front(count, cell, off, mass):
    return pl.pallas_call(
        front_kernel,
        out_shape=(
            jax.ShapeDtypeStruct((5, NROW, 128), F32),
            jax.ShapeDtypeStruct((GX, PAYROWS, 128), F32),
            pltpu.VMEM((HANDED, 128), F32),
        ),
        in_specs=[SM, VM, VM, VM],
        out_specs=(VM, VM, VM),
        scratch_shapes=[pltpu.VMEM((12, NROW, 128), F32)],
        name="front",
        compiler_params=FULL,
        cost_estimate=pl.CostEstimate(flops=40000000, bytes_accessed=1000000, transcendentals=0),
    )(count, cell, off, mass)


def forward_kernel(recv_ref, acc_ref, out_ref):
    last = lax.axis_index("gx") == GX - 1
    first = jnp.where(last, ROWS - FROWS, 0)
    row = jnp.where(last, 17.0, 0.0)
    for i in range(GX):
        parts = [recv_ref[i, pl.ds(o * ROWS + first, FROWS), :] for o in range(5)]
        for o, v in enumerate(one_row(*parts, row)):
            out_ref[i, o * FROWS : (o + 1) * FROWS, :] = v
        for n, r in enumerate((2, 5, 6, 7)):
            out_ref[i, 4 * FROWS + n : 4 * FROWS + n + 1, :] = recv_ref[i, FACE + r : FACE + r + 1, :]


def forward_pack(recv, acc):
    return pl.pallas_call(
        forward_kernel,
        out_shape=jax.ShapeDtypeStruct((GX, HANDED, 128), F32),
        in_specs=[VM, ANY],
        out_specs=VM,
        name="forward_pack",
        compiler_params=ROOM,
        cost_estimate=pl.CostEstimate(flops=500000, bytes_accessed=600000, transcendentals=0),
    )(recv, acc)


def join_kernel(one_ref, two_ref, out_ref):
    out_ref[0] = one_ref[...]
    out_ref[1] = two_ref[...]


def join(one, two):
    return pl.pallas_call(
        join_kernel,
        out_shape=jax.ShapeDtypeStruct((2, HANDED, 128), F32),
        in_specs=[VM, VM],
        out_specs=VM,
        name="join",
        compiler_params=ROOM,
    )(one, two)


def either_kernel(one_ref, two_ref, out_ref):
    out_ref[...] = one_ref[...] + two_ref[...]


def either(one, two):
    return pl.pallas_call(
        either_kernel,
        out_shape=jax.ShapeDtypeStruct((2, HANDED, 128), F32),
        in_specs=[VM, VM],
        out_specs=VM,
        name="either",
        compiler_params=ROOM,
    )(one, two)


def table_kernel(high_ref, low_ref):
    scale = 1.0 / 32.0
    none = jnp.zeros((64, 128), F32)

    def waves(height, step, size):
        j = lax.broadcasted_iota(I32, (height, 128), 1)
        k = lax.broadcasted_iota(I32, (height, 128), 0) * step
        angle = ((k * j) & 1023).astype(F32) * (2.0 * math.pi / 1024.0)
        return jnp.cos(angle) * size, jnp.sin(angle) * size

    many_c, many_s = waves(64, 8, scale)
    few_c, few_s = waves(8, 1, 1.0)

    def turns(m):
        c, s = few_c[m : m + 1], few_s[m : m + 1]
        return many_c * c - many_s * s, many_s * c + many_c * s

    for g, (m, w) in enumerate(((1, 7), (3, 5), (2, 6), (0, 4))):
        (c, s), (e, t) = turns(m), turns(w)
        if g < 3:
            parts = ((c, s), (-s, c), (e, -t), (-t, -e))
        else:
            parts = ((c, none), (-s, none), (none, e), (none, -t))
        for n, pair in enumerate(parts):
            for h, value in enumerate(pair):
                high = value.astype(BF)
                high_ref[g, 64 * n : 64 * n + 64, 128 * h : 128 * h + 128] = high
                low_ref[g, 64 * n : 64 * n + 64, 128 * h : 128 * h + 128] = (value - high.astype(F32)).astype(BF)


def tables():
    shape = jax.ShapeDtypeStruct((4, 256, 256), BF)
    return pl.pallas_call(
        table_kernel,
        out_shape=(shape, shape),
        out_specs=(VM, VM),
        name="tables",
        compiler_params=ROOM,
        cost_estimate=pl.CostEstimate(flops=8000000, bytes_accessed=1000000, transcendentals=0),
    )()


GROUPS = ((1, 7), (3, 5), (2, 6), (0, 4))


def transform(field, th_ref, tl_ref, put):
    root = math.sqrt(0.5)

    def even(b):
        return field(b) + field(b + 4)

    def odd(b):
        return field(b) - field(b + 4)

    for g in range(4):
        if g < 2:
            d1, d3 = odd(1), odd(3)
            s, t = (d1 - d3) * root, (d1 + d3) * root
            pair = (odd(0) + s, -odd(2) - t) if g == 0 else (odd(0) - s, odd(2) - t)
        elif g == 2:
            pair = (even(0) - even(2), even(3) - even(1))
        else:
            s, t = even(0) + even(2), even(1) + even(3)
            pair = (s + t, s - t)
        value = jnp.concatenate(pair, axis=0)
        high = value.astype(BF)
        low = (value - high.astype(F32)).astype(BF)
        o = jnp.dot(th_ref[g], high, preferred_element_type=F32)
        o = o + jnp.dot(tl_ref[g], high, preferred_element_type=F32)
        put(g, o + jnp.dot(th_ref[g], low, preferred_element_type=F32))


def face_columns(i, rows, ghosts):
    before, after = (i - 1) % GX, (i + 1) % GX
    lane = lax.broadcasted_iota(I32, (1, 128), 1)
    out = []
    for side in range(2):
        v = rows[i][side] + jnp.where(lane == 127, ghosts[after][side][0:1], 0.0)
        out.append(v + jnp.where(lane == 0, ghosts[before][side][1:2], 0.0))
    return out


def pick(v, lane):
    return jnp.sum(jnp.where(lax.broadcasted_iota(I32, (2, 128), 1) == lane, v, 0.0), axis=1, keepdims=True)


def along_z_kernel(face_ref, in_ref, *refs):
    gathered, (after_ref, down_ref, up_ref, all_ref) = refs[: GX // 2], refs[GX // 2 :]
    p, q = lax.axis_index("gx"), lax.axis_index("gy") % RING
    across = ((p == 0) & (q == 0)) | ((p == GX - 1) & (q == RING - 1))
    for i in range(GX):
        n = GX - 1 - i
        mine = jnp.where(p == 0, gathered[i // 2][i % 2], gathered[n // 2][n % 2])
        all_ref[i] = jnp.where(across, mine, in_ref[i])
    for j in range(2):
        on = p == (0 if j == 0 else GX - 1)
        rows, ghosts = [], []
        for i in range(GX):
            own, handed = face_ref[i, FACE : FACE + 8, :], all_ref[i, 4 * FROWS : HANDED, :]
            rows.append([own[3 * n + j : 3 * n + j + 1] + jnp.where(on, handed[n : n + 1], 0.0) for n in range(2)])
            past = [pick(own[6:8], base + 2 * p + 1 + j) for base in (0, 24)]
            more = [pick(handed[2:4], base + (17 if j == 0 else 0)) for base in (0, 24)]
            ghosts.append([a + jnp.where(on, b, 0.0) for a, b in zip(past, more)])
        for i in range(GX):
            down, up = face_columns(i, rows, ghosts)
            down_ref[2 * i + j : 2 * i + j + 1] = down
            up_ref[2 * i + j : 2 * i + j + 1] = up


def along_z(recv, passed, gathered, after):
    shape = jax.ShapeDtypeStruct((2 * GX, 128), F32)
    return pl.pallas_call(
        along_z_kernel,
        out_shape=(shape, shape, jax.ShapeDtypeStruct((GX, HANDED, 128), F32)),
        in_specs=[VM] * (2 + GX // 2) + [ANY],
        out_specs=(VM, VM, VM),
        name="along_z",
        compiler_params=ROOM,
        cost_estimate=pl.CostEstimate(flops=500000, bytes_accessed=100000, transcendentals=0),
    )(recv, passed, *gathered, after)


def handed_kernel(in_ref, face_ref, acc_ref, out_ref, flag_ref, val_ref):
    p = lax.axis_index("gx")
    flag_ref[0] = flagged(face_ref, FACE + 6)

    @pl.when((p == 0) | (p == GX - 1))
    def _():
        flag_ref[0] = jnp.maximum(flag_ref[0], flagged(in_ref, 4 * FROWS + 2))
        paint_sources(FROWS, 4, True, acc_ref, in_ref, out_ref, val_ref)


def paint_handed(passed, recv, acc):
    return pl.pallas_call(
        handed_kernel,
        out_shape=(PAINTED, pltpu.SMEM((1,), I32)),
        in_specs=[VM, VM, VM],
        out_specs=(VM, SM),
        scratch_shapes=paint_scratch(4),
        input_output_aliases={2: 0},
        name="paint_handed",
        compiler_params=ROOM,
        cost_estimate=PAINT_COST,
    )(passed, recv, acc)


def finish_kernel(acc_ref, below_ref, above_ref, th_ref, tl_ref, dens_ref, spec_ref, x_ref):
    wide = lax.broadcasted_iota(I32, (128, 128), 1)
    for i in range(GX):
        before, after = (i - 1) % GX, (i + 1) % GX
        gap = jnp.zeros((124, 128), F32)
        t = jnp.concatenate([below_ref[2 * i : 2 * i + 2], gap, above_ref[2 * i : 2 * i + 2]], axis=0).T
        for j in range(2):
            shifted = pltpu.roll(t, 1 if j == 0 else 127, 1)
            low, high = (t, shifted) if j == 0 else (shifted, t)
            v = acc_ref[i, j, 0:128, :] + jnp.where(wide == 0, low, jnp.where(wide == 127, high, 0.0))
            cols = slice(j * 128, (j + 1) * 128)
            x_ref[i, :, cols] = v
            x_ref[i, 127:128, cols] = v[127:128] + acc_ref[after, j, 128:129, :]
            x_ref[i, 0:1, cols] = v[0:1] + acc_ref[before, j, 129:130, :]
            dens_ref[pl.ds(i * 256 + j, 128, stride=2), :] = x_ref[i, :, cols]

    def put(g, o):
        m, w = GROUPS[g]
        for n, (k, part) in enumerate(((m, 0), (m, 1), (w, 0), (w, 1))):
            for j in range(2):
                spec_ref[pl.ds(part * 1024 + 2 * k + j, 64, stride=16), :] = o[64 * n : 64 * n + 64, j * 128 : (j + 1) * 128]

    transform(lambda b: x_ref[b], th_ref, tl_ref, put)


def finish(acc, below, above, th, tl):
    shape = jax.ShapeDtypeStruct((2048, 128), F32)
    return pl.pallas_call(
        finish_kernel,
        out_shape=(shape, shape),
        in_specs=[VM] * 5,
        out_specs=(VM, VM),
        scratch_shapes=[pltpu.VMEM((GX, 128, 256), F32)],
        name="finish",
        compiler_params=ROOM,
        cost_estimate=pl.CostEstimate(flops=400000000, bytes_accessed=4000000, transcendentals=0),
    )(acc, below, above, th, tl)


def y_pairs(blocks, across):
    pairs = []
    for q in range(blocks):
        n, top = (q + 1) % blocks, (GX - 1) * blocks
        if across or q % RING != RING - 1:
            pairs += [(top + q, n), (n, top + q)]
    return pairs


def exchange(x):
    return lax.all_to_all(x, "gx", split_axis=0, concat_axis=0, tiled=False)


def hand_on(x, across=False):
    return lax.ppermute(x, ("gx", "gy"), y_pairs(lax.axis_size("gy"), across))


def beside(x, up):
    blocks, pairs = lax.axis_size("gy"), []
    for q in range(RING - 1 if up else 0, blocks, RING):
        for p in range(0, GX, 2):
            pairs.append(((p + 1) * blocks + q, p * blocks + q) if up else (p * blocks + q, (p + 1) * blocks + q))
    return lax.ppermute(x, ("gx", "gy"), pairs)


def cross(x, up):
    blocks, pairs = lax.axis_size("gy"), []
    for q in range(RING - 1, blocks, RING):
        n = (q + 1) % blocks
        for p in range(0 if up else 1, GX, 2):
            pairs.append((p * blocks + q, p * blocks + n) if up else (p * blocks + n, p * blocks + q))
    return lax.ppermute(x, ("gx", "gy"), pairs)


def gather(x, n):
    blocks, pairs = lax.axis_size("gy"), []
    for q in range(blocks):
        if q % RING == 0:
            pairs.append((n * blocks + q, q))
        elif q % RING == RING - 1:
            pairs.append(((GX - 1 - n) * blocks + q, (GX - 1) * blocks + q))
    return lax.ppermute(x, ("gx", "gy"), pairs)


def weighted(block):
    row = jnp.where(lax.axis_index("gx") == GX - 1, 17.0, 0.0)
    parts = one_row(*(block[:, o * ROWS : (o + 1) * ROWS] for o in range(5)), row)
    return jnp.concatenate([*parts, jnp.zeros((GX, PAYROWS - 4 * ROWS, 128), F32)], axis=1)


def later_window(ordered, turn):
    _, yp, _ = cells_of(ordered[0])
    live = ordered[4] != 0.0
    key = jnp.where(live, jnp.where(ordered[2] >= 0, yp, yp - 1.0), 20.0)
    space = jnp.zeros((5, NROW + 3 * ROWS, 128), F32)
    padded = jnp.concatenate([space, ordered, space], axis=1)
    base = NROW + 3 * ROWS
    blocks = []
    for p in range(GX):
        if p < GX - 1:
            begin = jnp.sum(jnp.where(key < 2 * p, 1, 0))
            w = jnp.minimum(begin // 128, NROW - ROWS) + turn * ROWS
        else:
            w = jnp.clip((jnp.sum(jnp.where(live, 1, 0)) + 127) // 128 - ROWS, 0, NROW - ROWS) - turn * ROWS
        part = lax.dynamic_slice_in_dim(padded, base + w, ROWS, axis=1).reshape(5 * ROWS, 128)
        blocks.append(jnp.concatenate([part, jnp.zeros((PAYROWS - 5 * ROWS, 128), F32)], axis=0))
    return jnp.stack(blocks)


def body(cell_index, offsets, mass, counts):
    p = lax.axis_index("gx")
    blocks = lax.axis_size("gz")
    ordered, pay, hand = front(
        counts, cell_index.reshape(NROW, 128), offsets.reshape(3, NROW, 128), mass.reshape(NROW, 128)
    )
    next_to = beside(hand, True)
    came_up = cross(join(hand, next_to), True)
    recv = exchange(pay)
    next_to = beside(hand, False)
    came_down = cross(join(hand, next_to), False)
    th, tl = tables()
    held = either(came_up, came_down)
    gathered = [held]
    for n in range(2, GX, 2):
        gathered.append(gather(held, n))
    acc = paint_early(recv)
    packed = forward_pack(recv, acc)
    passed = hand_on(packed)
    acc = paint_late(recv, packed, acc)
    down, up, passed = along_z(recv, passed, gathered, acc)
    below = lax.ppermute(up, "gz", [(i, (i + 1) % blocks) for i in range(blocks)])
    above = lax.ppermute(down, "gz", [((i + 1) % blocks, i) for i in range(blocks)])
    acc, over = paint_handed(passed, recv, acc)
    density, spectrum = finish(acc, below, above, th, tl)

    def slow(outputs):
        mine = jnp.max(recv[:, FACE + 6, 64:]) > 0
        later = lax.cond(
            mine,
            lambda: tuple(exchange(later_window(ordered, t)) for t in (1, 2, 3)),
            lambda: (jnp.zeros(recv.shape, F32),) * 3,
        )
        first = jnp.where(p == GX - 1, ROWS - FROWS, 0)
        row = lax.broadcasted_iota(I32, (PAYROWS, 128), 0) - 4 * ROWS
        sent = (row >= first) & (row < first + FROWS)
        rest = jnp.where(sent, 0.0, recv)
        acc = jnp.zeros(PAINTED.shape, F32)
        for x in (recv, *later):
            acc = paint_more(x, acc)
        for x in (rest, *later):
            acc = paint_more(hand_on(weighted(x), across=True), acc, handed=True)
        acc, _ = paint_handed(passed, recv, acc)
        return finish(acc, below, above, th, tl)

    density, spectrum = lax.cond(over[0] > 0, slow, lambda outputs: outputs, (density, spectrum))
    return density.reshape(1024, 1, 2, 128), spectrum.reshape(2, 512, 1, 2, 128)


def solution(mesh):
    placed = (
        P("gx", "gy", "gz", None),
        P("gx", "gy", "gz", None, None),
        P("gx", "gy", "gz", None),
        P("gx", "gy", "gz"),
    )
    return jax.shard_map(
        body,
        mesh=mesh,
        in_specs=placed,
        out_specs=(P(None, "gx", "gy", "gz"), P(None, None, "gx", "gy", "gz")),
        check_vma=False,
    )
```
